32 devices in a mesh: row: 8 (over z, core), col: 4 (over y, x).
Axes of the slice: x: 2, y: 2, z: 4, core: 2. Of those that a mesh axis runs over, the one named last changes fastest.
Arguments:
- right_side: float32 [1, 8, 4, 1024], P(None, 'row'), may hold values from -6 to 6
- inverse_t: bfloat16 [1, 8, 1024, 1024], P(None, 'row', 'col'), as said below
- u_factor: bfloat16 [1, 8, 2, 4, 128, 1024], P(None, 'row', None, 'col'), may hold values from -0.25 to 0.25
- v_factor: bfloat16 [1, 8, 2, 4, 128, 1024], P(None, 'row', None, 'col'), may hold values from -0.1875 to 0.1875
- ranks: int32 [1, 8, 2, 4], P(None, 'row', None, 'col'), may hold values from 4 to 128, as said below
Outputs:
- whitened: float32 [1, 8, 4, 1024], P(None, 'row')
- loglik: float32 [1, 8, 4], P(None, 'row')
The draws below stay inside these ranges and needn't reach their ends.
Inputs may be any that keep to these rules, and one draw needn't show every extreme that they name: Tile (i, j) with j < i uses the first ranks of its factor rows. `inverse_t`: upper triangular with a positive diagonal.
All inputs are finite; a program needn't handle non-finite values.
Results may differ from the reference program's by a relative error of at most 0.0085.
Values sent between devices are 32-bit elements; how exact they have to be, the bound alone decides.
A program may use at most 64 MiB of HBM per device.

```python
import math
import jax
import jax.numpy as jnp

NB = 1024
RMAX = 128
NRHS = 4
CYC = 1
SLAB = 8
N_ROW = 8
N_COL = 4


def draw_inverse_t(key, part):
    key_diag, key_off = jax.random.split(jax.random.fold_in(key, 11))
    shape = (CYC, N_ROW, NB, NB)
    diagonal = jnp.exp(jax.random.uniform(key_diag, (CYC, N_ROW, NB), jnp.float32, math.log(0.3), math.log(1.2)))
    spread = jax.random.normal(key_off, shape, jnp.float32)
    upper = jnp.triu(spread * (0.3 / math.sqrt(NB)), 1)
    eye = jnp.eye(NB, dtype=jnp.float32)
    matrix = upper + eye[None, None, :, :] * diagonal[:, :, :, None]
    return matrix.astype(jnp.bfloat16)


def draw_ranks(key, part):
    slab = CYC * N_ROW
    tile_cols = slab // N_COL
    shape = (CYC, N_ROW, tile_cols, N_COL)
    row_ids = jnp.arange(CYC, dtype=jnp.int32)[:, None, None, None] * N_ROW + jnp.arange(N_ROW, dtype=jnp.int32)[None, :, None, None]
    col_ids = jnp.arange(tile_cols, dtype=jnp.int32)[None, None, :, None] * N_COL + jnp.arange(N_COL, dtype=jnp.int32)[None, None, None, :]
    distance = jnp.maximum(row_ids - col_ids, 1)
    lowest = max(RMAX // 32, 1)
    highest = jnp.maximum(RMAX // distance, lowest)
    raw = jax.random.randint(jax.random.fold_in(key, 23), shape, 0, 1 << 20)
    values = lowest + raw % (highest - lowest + 1)
    forced = (row_ids == 1) & (col_ids == 0)
    values = jnp.where(forced, RMAX, values)
    return values.astype(jnp.int32)


def levels(rng, extent, shards, least, top_value):
    def one(position, parts):
        heights = jax.random.uniform(jax.random.fold_in(jax.random.fold_in(rng, 6), position), (parts,), jnp.float32, least / len(shards), top_value / len(shards))
        return jnp.repeat(jnp.exp(heights), extent[position] // parts).reshape((-1,) + (1,) * (len(extent) - position - 1))

    level = one(*shards[0])
    for cut in shards[1:]:
        level = level * one(*cut)
    return level


def scatter_about(own_key, dims, scale, bound, cuts=(), kind=jnp.bfloat16):
    loudness = levels(own_key, dims, cuts, -0.22, 0.18) if cuts else 1.0
    drawn = jax.random.normal(own_key, dims, jnp.float32) * scale * loudness
    return jnp.minimum(jnp.maximum(drawn, -bound), bound).astype(kind)


def setup_inputs(seed: int = 0) -> dict:
    key_of = jax.random.split(jax.random.key(seed), 6)
    return {
        "right_side": scatter_about(key_of[0], (CYC, N_ROW, NRHS, NB), 1.0, 6.0, ((1, 8),), jnp.float32),
        "inverse_t": draw_inverse_t(jax.random.fold_in(key_of[5], 71), 0),
        "u_factor": scatter_about(key_of[2], (CYC, N_ROW, SLAB // N_COL, N_COL, RMAX, NB), (4 * RMAX) ** -0.5, 0.25, ((1, 8), (3, 4))),
        "v_factor": scatter_about(key_of[3], (CYC, N_ROW, SLAB // N_COL, N_COL, RMAX, NB), NB ** -0.5, 0.1875, ((1, 8), (3, 4))),
        "ranks": draw_ranks(jax.random.fold_in(key_of[5], 71), 0),
    }


def reference(right_side, inverse_t, u_factor, v_factor, ranks):
    slab = CYC * N_ROW
    sources = right_side.reshape(slab, NRHS, NB)
    inverse = inverse_t.reshape(slab, NB, NB)
    u_tiles = u_factor.reshape(slab, slab, RMAX, NB)
    v_tiles = v_factor.reshape(slab, slab, RMAX, NB)
    limits = ranks.reshape(slab, slab)
    rank_index = jnp.arange(RMAX, dtype=jnp.int32)
    tile_index = jnp.arange(slab, dtype=jnp.int32)
    solved = jnp.zeros((slab, NRHS, NB), jnp.float32)
    for row in range(slab):
        rounded = solved.astype(jnp.bfloat16).astype(jnp.float32)
        inner = jnp.einsum('jrn,jkn->jrk', v_tiles[row].astype(jnp.float32), rounded)
        keep = (rank_index[None, :] < limits[row][:, None]) & (tile_index < row)[:, None]
        inner = jnp.where(keep[:, :, None], inner, 0.0).astype(jnp.bfloat16)
        partial_value = jnp.einsum('jrk,jrn->kn', inner.astype(jnp.float32), u_tiles[row].astype(jnp.float32))
        reduced = (sources[row] - partial_value).astype(jnp.bfloat16)
        result = jnp.dot(reduced, inverse[row], preferred_element_type=jnp.float32)
        solved = solved.at[row].set(result)
    diagonal = jnp.diagonal(inverse, axis1=1, axis2=2).astype(jnp.float32)
    logdiag = jnp.mean(jnp.log(diagonal), axis=1)
    quadratic = jnp.mean(solved * solved, axis=2)
    loglik = -0.5 * quadratic + logdiag[:, None] - 0.5 * math.log(2.0 * math.pi)
    return solved.reshape(CYC, N_ROW, NRHS, NB), loglik.reshape(CYC, N_ROW, NRHS)
```

```python
import functools
import math

import jax
import jax.numpy as jnp
from jax import lax
from jax.experimental import pallas as pl
from jax.experimental.pallas import tpu as pltpu
from jax.sharding import PartitionSpec as P

MESH = pl.DeviceIdType.MESH
NT = (((1,), (1,)), ((), ()))
FIRST_SHORT = 3
NEAR = 2


def remote(src, dst, send_sem, recv_sem, device):
    return pltpu.make_async_remote_copy(
        src_ref=src,
        dst_ref=dst,
        send_sem=send_sem,
        recv_sem=recv_sem,
        device_id=device,
        device_id_type=MESH,
    )


def kernel(
    n_row, n_col,
    rhs_hbm, inv_hbm, u_hbm, v_hbm, rank_hbm,
    white_ref, lik_ref,
    rhs_ref, inv_ref, u_ref, v_ref,
    y_in, p_out, p_in, y_row, logs, base,
    v_out, v_in, u_out, u_in, fold, w_out, w_in, y_full, y_all,
    in_sem, y_send, y_recv, p_send, p_recv, o_send, o_recv, l_send, l_recv,
    v_send, v_recv, u_send, u_recv, w_send, w_recv, m_send, m_recv, f_send, e_send,
    rank_ref,
):
    row = lax.axis_index("row")
    col = lax.axis_index("col")
    per_col, rank_max, width = u_ref.shape
    nrhs = rhs_ref.shape[0]
    piece = width // n_col
    peers = [lax.rem(col + k, n_col) for k in range(1, n_col)]
    own_slot = row // n_col
    own_home = lax.rem(row, n_col)
    last = n_row - 1

    copies = [
        pltpu.make_async_copy(v_hbm.at[0, 0, :, 0], v_ref, in_sem.at[0]),
        pltpu.make_async_copy(u_hbm.at[0, 0, :, 0], u_ref, in_sem.at[1]),
        pltpu.make_async_copy(inv_hbm.at[0, 0], inv_ref, in_sem.at[2]),
        pltpu.make_async_copy(rhs_hbm.at[0, 0], rhs_ref, in_sem.at[3]),
        pltpu.make_async_copy(rank_hbm, rank_ref, in_sem.at[4]),
    ]
    for copy in copies:
        copy.start()

    short = row >= FIRST_SHORT
    feeds = (row + 1 >= FIRST_SHORT) & (row < last)
    long_count = jnp.where(short, row - 1, row)
    long_first = jnp.where(feeds, row + 2, row + 1)
    near_end = jnp.minimum(row + NEAR + 1, n_row)
    relays = col == own_home

    barrier = pltpu.get_barrier_semaphore()

    def greet(i, s):
        pl.semaphore_signal(barrier, inc=1, device_id=(i, s), device_id_type=MESH)

    for peer in peers:
        greet(row, peer)
    greeted = jnp.int32(n_col - 1)

    @pl.when(row < last)
    def _():
        for s in range(n_col):
            greet(row + 1, s)

    greeted = greeted + jnp.where(row < last, n_col, 0)

    @pl.when(row > 0)
    def _():
        for s in range(n_col):
            greet(row - 1, s)

    greeted = greeted + jnp.where(row > 0, n_col, 0)

    for d in range(2, NEAR + 1):

        @pl.when(row + d < n_row)
        def _():
            greet(row + d, own_home)

        greeted = greeted + jnp.where(row + d < n_row, 1, 0)
        fed = (row >= d) & (lax.rem(jnp.maximum(row - d, 0), n_col) == col)

        @pl.when(fed)
        def _():
            for s in range(n_col):
                greet(row - d, s)

        greeted = greeted + jnp.where(fed, n_col, 0)

    def greet_far(i, count):
        greet(i, col)
        return count + 1

    greeted = lax.fori_loop(jnp.where(relays, near_end, n_row), n_row, greet_far, greeted)
    for q in range(per_col):
        j = q * n_col + col

        @pl.when(j < row - NEAR)
        def _():
            greet(j, col)

        greeted = greeted + jnp.where(j < row - NEAR, 1, 0)

    prev_slot = jnp.maximum(row - 1, 0) // n_col
    prev_home = lax.rem(jnp.maximum(row - 1, 0), n_col)
    gives = short & (col == prev_home)
    copies[0].wait()
    copies[1].wait()
    copies[4].wait()

    @pl.when(gives)
    def _():
        v_tile = v_ref[prev_slot].astype(jnp.float32)
        keep = lax.broadcasted_iota(jnp.int32, (rank_max, width), 0) < rank_ref[prev_slot]
        u_tile = jnp.where(keep, u_ref[prev_slot].astype(jnp.float32), 0.0)
        for s in range(n_col):
            v_out[s] = v_tile[:, s * piece:(s + 1) * piece]
            u_out[s] = u_tile[:, s * piece:(s + 1) * piece]

    pl.semaphore_wait(barrier, greeted)

    def v_copy(s, i):
        part = pl.ds(s, n_col - s)
        return remote(v_out.at[part], v_in.at[part], v_send.at[s], v_recv, (i, s))

    def u_copy(k, peer):
        return remote(u_out.at[peer], u_in, u_send.at[k], u_recv, (row, peer))

    crosses = short & (lax.rem(row, 2) == 0)
    half = n_col // 2
    across = n_col - 1 - prev_home
    split = crosses & (across < prev_home)

    def by_way(s):
        return crosses & (prev_home != s) & ((across != s) | split)

    def halved(s):
        return split & (across == s)

    def way_copy(cc, s):
        return remote(v_out.at[cc], v_out.at[cc], m_send.at[s], m_recv.at[cc], (row, s))

    @pl.when(gives)
    def _():
        for s in reversed(range(n_col)):

            @pl.when(by_way(s))
            def _():
                for cc in range(s, min(s + half, n_col)):
                    way_copy(cc, s).start()

            @pl.when(by_way(s) & jnp.logical_not(halved(s)))
            def _():
                for cc in range(s + half, n_col):
                    way_copy(cc, s).start()

            @pl.when(jnp.logical_not(by_way(s)))
            def _():
                v_copy(s, row - 1).start()

        for k, peer in enumerate(peers):
            u_copy(k, peer).start()
        u_in[...] = u_out[col]

    @pl.when(by_way(col))
    def _():
        def forward(cc, carry):
            remote(v_out.at[cc], v_out.at[cc], m_send.at[0], m_recv.at[cc], (row, prev_home)).wait_recv()

            @pl.when(split & (across + 1 == col) & (cc >= across + half))
            def _():
                remote(v_out.at[cc], v_in.at[cc], e_send, v_recv, (row - 1, across)).start()

            remote(v_out.at[cc], v_in.at[cc], f_send, v_recv, (row - 1, col)).start()
            return carry

        lax.fori_loop(col, jnp.where(halved(col), across + half, n_col), forward, 0)

    copies[2].wait()
    copies[3].wait()

    for cc in range(n_col):

        @pl.when(col == cc)
        def _():
            base[...] = rhs_ref[:, cc * piece:(cc + 1) * piece]

    def log_part():
        for cc in range(n_col):

            @pl.when(col == cc)
            def _():
                block = inv_ref[:, cc * piece:(cc + 1) * piece].astype(jnp.float32)
                r_id = lax.broadcasted_iota(jnp.int32, (piece, piece), 0)
                c_id = lax.broadcasted_iota(jnp.int32, (piece, piece), 1)
                diagonal = jnp.sum(jnp.where(r_id == c_id, block, 0.0), axis=0, keepdims=True)
                total = jnp.sum(jnp.log(diagonal), axis=1, keepdims=True)
                logs[cc] = jnp.broadcast_to(total, (1, 128))

        for k, peer in enumerate(peers):
            remote(logs.at[col], logs.at[col], l_send.at[k], l_recv.at[col], (row, peer)).start()

    pl.when(row > 0)(log_part)

    for q in range(per_col):
        j = q * n_col + col

        @pl.when(j < long_count)
        def _():
            near = row - j <= NEAR
            remote(y_in.at[q, 0], y_in.at[q, 0], y_send.at[0], y_recv.at[q, 0], (j, col)).wait_recv()

            @pl.when(near)
            def _():
                for s in range(1, n_col):
                    remote(y_in.at[q, s], y_in.at[q, s], y_send.at[0], y_recv.at[q, s], (j, s)).wait_recv()
                y = y_in[q, 0]
                for s in range(1, n_col):
                    y = y + y_in[q, s]
                y_full[...] = y

            @pl.when(jnp.logical_not(near))
            def _():
                y_full[...] = y_in[q, 0]

            y = y_full[...]
            inner = lax.dot_general(y.astype(jnp.bfloat16), v_ref[q], NT, preferred_element_type=jnp.float32)
            keep = lax.broadcasted_iota(jnp.int32, (nrhs, rank_max), 1) < rank_ref[q]
            inner = jnp.where(keep, inner, 0.0).astype(jnp.bfloat16)
            p = jnp.dot(inner, u_ref[q], preferred_element_type=jnp.float32)
            for s in range(n_col):
                p_out[q, s] = p[:, s * piece:(s + 1) * piece]
            for k, peer in enumerate(peers):
                remote(p_out.at[q, peer], p_in.at[j], p_send.at[q, k], p_recv.at[j], (row, peer)).start()
            p_in[j] = p_out[q, col]

    @pl.when(feeds)
    def _():
        fold[...] = jnp.zeros_like(fold)
        for cc in range(n_col):

            @pl.when(col == cc)
            def _():
                v_copy(cc, row).wait_recv()

        for cc in range(n_col):

            @pl.when(col <= cc)
            def _():
                part = lax.dot_general(
                    inv_ref[:, cc * piece:(cc + 1) * piece],
                    v_in[cc].astype(jnp.bfloat16),
                    NT,
                    preferred_element_type=jnp.float32,
                )
                fold[...] += part

    def gather_p(j, acc):
        home = lax.rem(j, n_col)

        @pl.when(home != col)
        def _():
            remote(p_in.at[j], p_in.at[j], p_send.at[0, 0], p_recv.at[j], (row, home)).wait_recv()

        return acc - p_in[j]

    base[...] = lax.fori_loop(0, long_count, gather_p, base[...])

    @pl.when(short)
    def _():
        @pl.when(col != prev_home)
        def _():
            remote(u_in, u_in, u_send.at[0], u_recv, (row, prev_home)).wait_recv()

        u_part = u_in[...].astype(jnp.bfloat16)
        for s in range(n_col):
            remote(w_in.at[s], w_in.at[s], w_send.at[0], w_recv.at[s], (row - 1, s)).wait_recv()
        inner = w_in[0]
        for s in range(1, n_col):
            inner = inner + w_in[s]
        base[...] -= jnp.dot(inner.astype(jnp.bfloat16), u_part, preferred_element_type=jnp.float32)

    reduced = base[...].astype(jnp.bfloat16)

    @pl.when(feeds)
    def _():
        w_out[...] = jnp.dot(reduced, fold[...].astype(jnp.bfloat16), preferred_element_type=jnp.float32)
        for s in range(n_col):
            remote(w_out, w_in.at[col], w_send.at[s], w_recv.at[col], (row + 1, s)).start()

    y_row[col] = jnp.dot(reduced, inv_ref[...], preferred_element_type=jnp.float32)

    def send_y(i, carry):
        remote(y_row.at[col], y_in.at[own_slot, col], y_send.at[i], y_recv.at[own_slot, col], (i, own_home)).start()
        return carry

    lax.fori_loop(long_first, near_end, send_y, 0)
    for k, peer in enumerate(peers):
        remote(y_row.at[col], y_row.at[col], o_send.at[k], o_recv.at[col], (row, peer)).start()
    pl.when(row == 0)(log_part)
    for k, peer in enumerate(peers):
        remote(logs.at[peer], logs.at[peer], l_send.at[k], l_recv.at[peer], (row, peer)).wait_recv()
    log_sum = logs[0]
    for s in range(1, n_col):
        log_sum = log_sum + logs[s]
    log_part_of_lik = log_sum * (1.0 / width) - 0.5 * math.log(2.0 * math.pi)

    def left_y(i, carry):
        remote(y_row.at[col], y_in.at[own_slot, col], y_send.at[i], y_recv.at[own_slot, col], (i, own_home)).wait_send()
        return carry

    lax.fori_loop(long_first, near_end, left_y, 0)
    for k, peer in enumerate(peers):
        remote(logs.at[col], logs.at[col], l_send.at[k], l_recv.at[col], (row, peer)).wait_send()

    @pl.when(feeds)
    def _():
        for s in range(n_col):
            remote(w_out, w_in.at[col], w_send.at[s], w_recv.at[col], (row + 1, s)).wait_send()

    @pl.when(gives)
    def _():
        for s in range(n_col):
            part = pl.ds(s, n_col - s)
            few = pl.ds(s, min(half, n_col - s))

            @pl.when(halved(s))
            def _():
                remote(v_out.at[few], v_out.at[few], m_send.at[s], m_recv.at[0], (row, s)).wait_send()

            @pl.when(by_way(s) & jnp.logical_not(halved(s)))
            def _():
                remote(v_out.at[part], v_out.at[part], m_send.at[s], m_recv.at[0], (row, s)).wait_send()

            @pl.when(jnp.logical_not(by_way(s)))
            def _():
                v_copy(s, row - 1).wait_send()

        for k, peer in enumerate(peers):
            u_copy(k, peer).wait_send()

    for cc in range(n_col):
        part = pl.ds(cc, n_col - cc)
        few = pl.ds(cc, min(half, n_col - cc))

        @pl.when(by_way(col) & (col == cc) & jnp.logical_not(halved(cc)))
        def _():
            remote(v_out.at[part], v_in.at[part], f_send, v_recv, (row - 1, cc)).wait_send()

        @pl.when(halved(cc) & (col == cc))
        def _():
            remote(v_out.at[few], v_in.at[few], f_send, v_recv, (row - 1, cc)).wait_send()

        if cc + half < n_col:
            rest = pl.ds(cc + half, n_col - cc - half)

            @pl.when(split & (across == cc) & (col == cc + 1))
            def _():
                remote(v_out.at[rest], v_in.at[rest], e_send, v_recv, (row - 1, cc)).wait_send()

    for q in range(per_col):
        j = q * n_col + col

        @pl.when(j < long_count)
        def _():
            for k, peer in enumerate(peers):
                remote(p_out.at[q, peer], p_in.at[j], p_send.at[q, k], p_recv.at[j], (row, peer)).wait_send()

    for k, peer in enumerate(peers):
        remote(y_row.at[peer], y_row.at[peer], o_send.at[k], o_recv.at[peer], (row, peer)).wait_recv()
    y = y_row[0]
    for s in range(1, n_col):
        y = y + y_row[s]
    y_all[...] = y

    def far_copy(i):
        return remote(y_all, y_in.at[own_slot, 0], y_send.at[i], y_recv.at[own_slot, 0], (i, col))

    def send_far(i, carry):
        far_copy(i).start()
        return carry

    lax.fori_loop(jnp.where(relays, near_end, n_row), n_row, send_far, 0)
    white_ref[0, 0] = y
    quadratic = jnp.sum(y * y, axis=1, keepdims=True) * (1.0 / width)
    lik = -0.5 * quadratic + log_part_of_lik
    r_id = lax.broadcasted_iota(jnp.int32, (nrhs, 128), 0)
    c_id = lax.broadcasted_iota(jnp.int32, (nrhs, 128), 1)
    flat = jnp.sum(jnp.where(r_id == c_id, lik, 0.0), axis=0, keepdims=True)
    lik_ref[0] = flat[:, :nrhs]

    def left_far(i, carry):
        far_copy(i).wait_send()
        return carry

    lax.fori_loop(jnp.where(relays, near_end, n_row), n_row, left_far, 0)
    for k, peer in enumerate(peers):
        remote(y_row.at[col], y_row.at[col], o_send.at[k], o_recv.at[col], (row, peer)).wait_send()


def local(n_row, n_col, right_side, inverse_t, u_factor, v_factor, ranks):
    nrhs, width = right_side.shape[2:]
    per_col, _, rank_max = u_factor.shape[2:5]
    piece = width // n_col
    vmem = pl.BlockSpec(memory_space=pltpu.VMEM)
    hbm = pl.BlockSpec(memory_space=pl.ANY)
    dma = pltpu.SemaphoreType.DMA

    def f32(*shape):
        return pltpu.VMEM(shape, jnp.float32)

    def bf16(*shape):
        return pltpu.VMEM(shape, jnp.bfloat16)

    return pl.pallas_call(
        functools.partial(kernel, n_row, n_col),
        out_shape=(
            pltpu.VMEM((1, 1, nrhs, width), jnp.float32),
            pltpu.VMEM((1, 1, nrhs), jnp.float32),
        ),
        in_specs=[hbm, hbm, hbm, hbm, hbm],
        out_specs=(vmem, vmem),
        scratch_shapes=[
            f32(nrhs, width),
            bf16(piece, width),
            bf16(per_col, rank_max, width),
            bf16(per_col, rank_max, width),
            f32(per_col, n_col, nrhs, width),
            f32(per_col, n_col, nrhs, piece),
            f32(n_row, nrhs, piece),
            f32(n_col, nrhs, width),
            f32(n_col, 1, 128),
            f32(nrhs, piece),
            f32(n_col, rank_max, piece),
            f32(n_col, rank_max, piece),
            f32(n_col, rank_max, piece),
            f32(rank_max, piece),
            f32(piece, rank_max),
            f32(nrhs, rank_max),
            f32(n_col, nrhs, rank_max),
            f32(nrhs, width),
            f32(nrhs, width),
            dma((5,)),
            dma((n_row,)),
            dma((per_col, n_col)),
            dma((per_col, n_col)),
            dma((n_row,)),
            dma((n_col,)),
            dma((n_col,)),
            dma((n_col,)),
            dma((n_col,)),
            dma((n_col,)),
            dma,
            dma((n_col,)),
            dma,
            dma((n_col,)),
            dma((n_col,)),
            dma((n_col,)),
            dma((n_col,)),
            dma,
            dma,
            pltpu.SMEM((per_col,), jnp.int32),
        ],
        compiler_params=pltpu.CompilerParams(collective_id=0, has_side_effects=True),
        name="forward_solve",
    )(right_side, inverse_t, u_factor, v_factor, ranks.reshape(per_col))


def solution(mesh):
    placed = (
        P(None, "row", None, None),
        P(None, "row", "col", None),
        P(None, "row", None, "col", None, None),
        P(None, "row", None, "col", None, None),
        P(None, "row", None, "col"),
    )
    return jax.shard_map(
        functools.partial(local, mesh.shape["row"], mesh.shape["col"]),
        mesh=mesh,
        in_specs=placed,
        out_specs=(P(None, "row", None, None), P(None, "row", None)),
        check_vma=False,
    )
```

```python
import functools
import math

import jax
import jax.numpy as jnp
from jax import lax
from jax.experimental import pallas as pl
from jax.experimental.pallas import tpu as pltpu
from jax.sharding import PartitionSpec as P

MESH = pl.DeviceIdType.MESH
NT = (((1,), (1,)), ((), ()))
FIRST_SHORT = 3
NEAR = 3


def remote(src, dst, send_sem, recv_sem, device):
    return pltpu.make_async_remote_copy(
        src_ref=src,
        dst_ref=dst,
        send_sem=send_sem,
        recv_sem=recv_sem,
        device_id=device,
        device_id_type=MESH,
    )


def kernel(
    n_row, n_col,
    rhs_hbm, inv_hbm, u_hbm, v_hbm, rank_hbm,
    white_ref, lik_ref,
    rhs_ref, inv_ref, u_ref, v_ref, rank_ref,
    y_in, p_out, p_in, y_row, logs, base, y_full, y_all,
    v_out, v_in, u_out, u_in, fold, w_out, w_in,
    x_out, x_in, t_out, t_in, fold_x, wx_out, wx_in,
    d_out, d_in, d_tile, du_out, du_in, du_tile, pd_out, l_out, l_in, wl_out, wl_in, we_in,
    a_out, a_in, a_sum,
    in_sem, y_send, y_recv, p_send, p_recv, o_send, o_recv, l_send, l_recv,
    v_send, v_recv, u_send, u_recv, w_send, w_recv, m_recv, f_send, e_send, ready,
    x_recv, t_recv, k_recv, d_send, d_recv, du_send, du_recv, pd_send, wl_send, wl_recv, wp_send,
    we_send, we_recv, wx_send, wx_recv, a_send, a_recv,
):
    row = lax.axis_index("row")
    col = lax.axis_index("col")
    per_col, rank_max, width = u_ref.shape
    nrhs = rhs_ref.shape[0]
    piece = width // n_col
    half = n_col // 2
    peers = [lax.rem(col + k, n_col) for k in range(1, n_col)]
    others = pl.ds(0, n_col - 1)
    own_slot = row // n_col
    own_home = lax.rem(row, n_col)
    end = n_row - 1
    even_end = n_row - 2
    ahead = n_row - 3

    def longs_of(i):
        count = jnp.where(i >= FIRST_SHORT, i - 1, i)
        handed = (lax.rem(i, 2) == 0) & (i >= 2)
        return count - jnp.where(handed, 1, 0) - jnp.where(i >= even_end, 1, 0)

    def near_of(i):
        return NEAR + jnp.where(i >= 2, 1, 0)

    copies = [
        pltpu.make_async_copy(v_hbm.at[0, 0, :, 0], v_ref, in_sem.at[0]),
        pltpu.make_async_copy(u_hbm.at[0, 0, :, 0], u_ref, in_sem.at[1]),
        pltpu.make_async_copy(inv_hbm.at[0, 0], inv_ref, in_sem.at[2]),
        pltpu.make_async_copy(rhs_hbm.at[0, 0], rhs_ref, in_sem.at[3]),
        pltpu.make_async_copy(rank_hbm, rank_ref, in_sem.at[4]),
    ]
    for copy in copies:
        copy.start()

    even = lax.rem(row, 2) == 0
    short = row >= FIRST_SHORT
    feeds = (row + 1 >= FIRST_SHORT) & (row < end)
    is_end = row == end
    is_even_end = row == even_end
    is_ahead = row == ahead
    long_count = longs_of(row)
    near_end = jnp.minimum(row + near_of(row) + 1, n_row)
    relays = col == own_home

    barrier = pltpu.get_barrier_semaphore()

    def signal(sem, i, s):
        pl.semaphore_signal(sem, inc=1, device_id=(i, s), device_id_type=MESH)

    def row_of(i, cond, act):
        @pl.when(cond)
        def _():
            for s in range(n_col):
                act(i, s)

        return jnp.where(cond, n_col, 0)

    def above(act):
        yield row + 1, row_of(row + 1, row < end, act)
        for d in range(2, NEAR + 2):
            wide = is_ahead if d == 2 else jnp.bool_(False)
            one = (row + d < n_row) & (d <= near_of(row)) & jnp.logical_not(wide)

            @pl.when(one)
            def _():
                act(row + d, own_home)

            yield row + d, jnp.where(one, 1, 0)
            if d == 2:
                yield row + d, row_of(row + d, wide, act)

    def below(act):
        row_of(row - 1, row > 0, act)
        count = jnp.where(row > 0, n_col, 0)
        for d in range(2, NEAR + 2):
            fed = (row >= d) & (d <= near_of(row - d)) & (lax.rem(jnp.maximum(row - d, 0), n_col) == col)
            if d == 2:
                fed = fed | is_end
            count += row_of(row - d, fed, act)
        for q in range(per_col):
            j = q * n_col + col
            far = j < row - near_of(j)

            @pl.when(far)
            def _():
                act(j, col)

            count += jnp.where(far, 1, 0)
        return count

    def at_once(low, high):
        return (low == 0) & (high <= NEAR)

    for peer in peers:
        signal(barrier, row, peer)
    greeted = jnp.int32(n_col - 1)
    answers = jnp.int32(0)
    for i, count in above(lambda i, s: signal(barrier, i, s)):
        quick = at_once(row, i)
        greeted += jnp.where(quick, count, 0)
        answers += jnp.where(quick, 0, count)

    def greet_far(i, count):
        signal(barrier, i, col)
        return count + 1

    answers = lax.fori_loop(jnp.where(relays, near_end, n_row), n_row, greet_far, answers)

    def greet_quick(i, s):
        @pl.when(at_once(i, row))
        def _():
            signal(barrier, i, s)

    def answer(i, s):
        @pl.when(jnp.logical_not(at_once(i, row)))
        def _():
            signal(ready, i, s)

    greeted += below(greet_quick)

    prev = jnp.maximum(row - 1, 0)
    prev_slot = prev // n_col
    prev_home = lax.rem(prev, n_col)
    gives = short & (col == prev_home)
    crosses = short & even
    far_slot = ahead // n_col
    far_home = ahead % n_col
    gives_far = is_end & (col == far_home)
    handed = even & (row >= 2)
    mine = jnp.where(handed, long_count + jnp.where(is_even_end, 1, 0), 0)
    mine_slot = mine // n_col
    mine_home = lax.rem(mine, n_col)
    hands = handed & (col == mine_home)
    taken = (row >= 3) & jnp.logical_not(even)
    theirs = jnp.where(taken, longs_of(prev) + jnp.where(is_end, 1, 0), 0)
    their_home = lax.rem(theirs, n_col)
    takes = taken & (col == their_home)
    whole = even_end - 3
    whole_slot = whole // n_col
    whole_home = whole % n_col
    hands_whole = is_even_end & (col == whole_home)
    takes_whole = is_end & (col == whole_home)

    def masked_u(slot):
        keep = lax.broadcasted_iota(jnp.int32, (rank_max, width), 0) < rank_ref[slot]
        return jnp.where(keep, u_ref[slot].astype(jnp.float32), 0.0)

    def cut(tile, into):
        for s in range(n_col):
            into[s] = tile[:, s * piece:(s + 1) * piece]

    copies[0].wait()
    copies[1].wait()
    copies[4].wait()

    @pl.when(hands)
    def _():
        d_out[...] = v_ref[mine_slot].astype(jnp.float32)
        cut(masked_u(mine_slot), l_out)

    @pl.when(hands_whole)
    def _():
        d_out[...] = v_ref[whole_slot].astype(jnp.float32)
        du_out[...] = masked_u(whole_slot)

    @pl.when(gives)
    def _():
        cut(v_ref[prev_slot].astype(jnp.float32), v_out)
        cut(masked_u(prev_slot), u_out)

    @pl.when(gives_far)
    def _():
        cut(v_ref[far_slot].astype(jnp.float32), x_out)
        cut(masked_u(far_slot), t_out)

    pl.semaphore_wait(barrier, greeted)
    below(answer)

    def by_way(home, s, cc):
        across = n_col - 1 - home
        return (home != s) & jnp.where(across < home, (across != s) | (cc < s + half), (s > home) | (cc < s + half))

    def is_late(home, s, cc):
        across = n_col - 1 - home
        return (across == s) & (across < home) & (cc >= s + half)

    def joined(home, s):
        across = n_col - 1 - home
        return (across > home) & (across == s)

    def spread(out, into, recv, target, home, cross):
        for s in reversed(range(n_col)):
            if s > 0:

                @pl.when(cross & joined(home, s - 1))
                def _():
                    remote(out.at[s - 1], out.at[s - 1], v_send.at[s], m_recv.at[s - 1], (row, s)).start()

            for cc in range(s, n_col):
                gone = cross & joined(home, s)
                way = cross & by_way(home, s, cc)
                later = cross & is_late(home, s, cc)

                @pl.when(way & jnp.logical_not(gone))
                def _():
                    remote(out.at[cc], out.at[cc], v_send.at[s], m_recv.at[cc], (row, s)).start()

                @pl.when(jnp.logical_not(way | later | gone))
                def _():
                    remote(out.at[cc], into.at[cc], v_send.at[s], recv, (target, s)).start()

    def spread_late(out, into, recv, target, home):
        for s in range(n_col):
            for cc in range(min(s + half, n_col), n_col):

                @pl.when(is_late(home, s, cc))
                def _():
                    remote(out.at[cc], into.at[cc], v_send.at[s], recv, (target, s)).start()

    def spread_done(out, home, cross):
        for s in range(n_col):
            part = pl.ds(s, n_col - s)
            gone = cross & joined(home, s)
            more = (cross & joined(home, s - 1)) if s > 0 else jnp.bool_(False)

            @pl.when(jnp.logical_not(gone | more))
            def _():
                remote(out.at[part], out.at[part], v_send.at[s], m_recv.at[0], (row, s)).wait_send()

            if s > 0:
                part_more = pl.ds(s - 1, n_col - s + 1)

                @pl.when(more)
                def _():
                    remote(out.at[part_more], out.at[part_more], v_send.at[s], m_recv.at[0], (row, s)).wait_send()

    def relay(out, into, recv, target, home):
        across = n_col - 1 - home
        more = joined(home, col - 1)
        first = jnp.where(more, col - 1, col)
        part = jnp.where(across < home, across == col, col < home)
        stop = jnp.where(joined(home, col), col, jnp.where(part, jnp.minimum(col + half, n_col), n_col))

        def forward(cc, carry):
            remote(out.at[cc], out.at[cc], v_send.at[0], m_recv.at[cc], (row, home)).wait_recv()

            @pl.when(cc >= col)
            def _():
                remote(out.at[cc], into.at[cc], f_send, recv, (target, col)).start()

            @pl.when(more)
            def _():
                remote(out.at[cc], into.at[cc], e_send, recv, (target, across)).start()

            return carry

        lax.fori_loop(first, stop, forward, 0)

    def relay_done(out, home):
        across = n_col - 1 - home
        for cc in range(n_col):
            few = pl.ds(cc, min(half, n_col - cc))
            here = (col == cc) & jnp.logical_not(joined(home, cc))
            half_way = jnp.where(across < home, across == cc, cc < home)

            @pl.when(here & jnp.logical_not(half_way))
            def _():
                part = pl.ds(cc, n_col - cc)
                remote(out.at[part], out.at[part], f_send, v_recv, (row, home)).wait_send()

            @pl.when(here & half_way)
            def _():
                remote(out.at[few], out.at[few], f_send, v_recv, (row, home)).wait_send()

            if cc > 0:

                @pl.when((col == cc) & joined(home, cc - 1))
                def _():
                    part = pl.ds(cc - 1, n_col - cc + 1)
                    remote(out.at[part], out.at[part], e_send, v_recv, (row, home)).wait_send()

    def share(out, into, recv):
        for peer in peers:
            remote(out.at[peer], into, u_send, recv, (row, peer)).start()
        into[...] = out[col]

    def share_done(out):
        remote(out.at[others], out.at[others], u_send, u_recv, (row, peers[0])).wait_send()

    def shared_wait(into, recv, home):
        @pl.when(col != home)
        def _():
            remote(into, into, u_send, recv, (row, home)).wait_recv()

    @pl.when(hands)
    def _():
        share(l_out, l_in, k_recv)

    @pl.when(gives & is_even_end)
    def _():
        share(u_out, u_in, u_recv)

    @pl.when(gives)
    def _():
        spread(v_out, v_in, v_recv, row - 1, prev_home, crosses)

    @pl.when(gives_far)
    def _():
        spread(x_out, x_in, x_recv, row - 2, far_home, jnp.bool_(True))

    @pl.when((handed) & (answers > 0))
    def _():
        pl.semaphore_wait(ready, answers)

    @pl.when(hands | hands_whole)
    def _():
        remote(d_out, d_in, d_send, d_recv, (row + 1, col)).start()

    @pl.when(hands_whole)
    def _():
        remote(du_out, du_in, du_send, du_recv, (row + 1, col)).start()

    @pl.when(crosses & (col != prev_home))
    def _():
        relay(v_out, v_in, v_recv, row - 1, prev_home)

    copies[2].wait()
    copies[3].wait()

    for cc in range(n_col):

        @pl.when(col == cc)
        def _():
            base[...] = rhs_ref[:, cc * piece:(cc + 1) * piece]

    def log_part():
        for cc in range(n_col):

            @pl.when(col == cc)
            def _():
                block = inv_ref[:, cc * piece:(cc + 1) * piece].astype(jnp.float32)
                r_id = lax.broadcasted_iota(jnp.int32, (piece, piece), 0)
                c_id = lax.broadcasted_iota(jnp.int32, (piece, piece), 1)
                diagonal = jnp.sum(jnp.where(r_id == c_id, block, 0.0), axis=0, keepdims=True)
                total = jnp.sum(jnp.log(diagonal), axis=1, keepdims=True)
                logs[cc] = jnp.broadcast_to(total, (1, 128))

        for peer in peers:
            remote(logs.at[col], logs.at[col], l_send, l_recv, (row, peer)).start()

    pl.when(row > 0)(log_part)

    @pl.when(gives & jnp.logical_not(even))
    def _():
        spread_done(v_out, prev_home, crosses)
        share(u_out, u_in, u_recv)

    def fold_with(into, recv, target):
        target[...] = jnp.zeros_like(target)
        for cc in range(n_col):
            part = pl.ds(cc, n_col - cc)

            @pl.when(col == cc)
            def _():
                remote(into.at[part], into.at[part], f_send, recv, (row, cc)).wait_recv()

        for cc in range(n_col):

            @pl.when(col <= cc)
            def _():
                target[...] += lax.dot_general(
                    inv_ref[:, cc * piece:(cc + 1) * piece],
                    into[cc].astype(jnp.bfloat16),
                    NT,
                    preferred_element_type=jnp.float32,
                )

    def long_step(q, cond):
        j = q * n_col + col

        @pl.when((j < long_count) & cond)
        def _():
            near = row - j <= near_of(j)

            @pl.when(near)
            def _():
                remote(y_in.at[q], y_in.at[q], y_send.at[0], y_recv.at[q], (j, col)).wait_recv()
                y = y_in[q, 0]
                for s in range(1, n_col):
                    y = y + y_in[q, s]
                y_full[...] = y

            @pl.when(jnp.logical_not(near))
            def _():
                remote(y_in.at[q, 0], y_in.at[q, 0], y_send.at[0], y_recv.at[q], (j, col)).wait_recv()
                y_full[...] = y_in[q, 0]

            y = y_full[...].astype(jnp.bfloat16)

            @pl.when(takes & (j == theirs))
            def _():
                wl_out[...] = lax.dot_general(y, d_tile[...], NT, preferred_element_type=jnp.float32)
                for s in range(n_col):
                    remote(wl_out, wl_in, wl_send, wl_recv, (row - 1, s)).start()

                @pl.when(is_end)
                def _():
                    for peer in peers:
                        remote(wl_out, wl_in, wp_send, wl_recv, (row, peer)).start()
                    wl_in[...] = wl_out[...]

            @pl.when(takes_whole & (j == whole))
            def _():
                inner = lax.dot_general(y, d_tile[...], NT, preferred_element_type=jnp.float32)
                p = jnp.dot(inner.astype(jnp.bfloat16), du_tile[...], preferred_element_type=jnp.float32)
                for s in range(n_col):
                    pd_out[s] = p[:, s * piece:(s + 1) * piece]
                    remote(pd_out.at[s], p_in.at[j], pd_send, p_recv.at[j], (row - 1, s)).start()

            inner = lax.dot_general(y, v_ref[q], NT, preferred_element_type=jnp.float32)
            keep = lax.broadcasted_iota(jnp.int32, (nrhs, rank_max), 1) < rank_ref[q]
            inner = jnp.where(keep, inner, 0.0).astype(jnp.bfloat16)
            p = jnp.dot(inner, u_ref[q], preferred_element_type=jnp.float32)
            for s in range(n_col):
                p_out[q, s] = p[:, s * piece:(s + 1) * piece]
            for peer in peers:
                remote(p_out.at[q, peer], p_in.at[j], p_send.at[q], p_recv.at[j], (row, peer)).start()
            p_in[j] = p_out[q, col]

    for q in range(per_col):
        long_step(q, is_even_end & (q * n_col + col <= row - 5))

    @pl.when(is_even_end)
    def _():
        fold_with(v_in, v_recv, fold)
        factor = fold[...].astype(jnp.bfloat16)
        shared_wait(u_in, u_recv, prev_home)
        shared_wait(l_in, k_recv, mine_home)
        a_out[0] = jnp.dot(u_in[...].astype(jnp.bfloat16), factor, preferred_element_type=jnp.float32)
        a_out[1] = jnp.dot(l_in[...].astype(jnp.bfloat16), factor, preferred_element_type=jnp.float32)
        for k in range(2):
            for s in range(n_col):
                remote(a_out.at[k], a_in.at[k, col], a_send, a_recv, (row + 1, s)).start()

    @pl.when(takes | takes_whole)
    def _():
        remote(d_in, d_in, d_send, d_recv, (row - 1, col)).wait_recv()
        d_tile[...] = d_in[...].astype(jnp.bfloat16)

    @pl.when(takes_whole)
    def _():
        remote(du_in, du_in, du_send, du_recv, (row - 1, col)).wait_recv()
        du_tile[...] = du_in[...].astype(jnp.bfloat16)

    @pl.when(is_end & (col != far_home))
    def _():
        relay(x_out, x_in, x_recv, row - 2, far_home)

    for q in range(per_col):
        long_step(q, jnp.logical_not(is_even_end & (q * n_col + col <= row - 5)))

    @pl.when(feeds & jnp.logical_not(is_even_end))
    def _():
        fold_with(v_in, v_recv, fold)

    @pl.when(gives & crosses)
    def _():
        spread_late(v_out, v_in, v_recv, row - 1, prev_home)

    @pl.when(gives & crosses & jnp.logical_not(is_even_end))
    def _():
        share(u_out, u_in, u_recv)

    @pl.when(gives_far)
    def _():
        spread_late(x_out, x_in, x_recv, row - 2, far_home)
        share(t_out, t_in, t_recv)

    @pl.when(is_ahead)
    def _():
        fold_with(x_in, x_recv, fold_x)

    @pl.when(is_end)
    def _():
        remote(a_in, a_in, a_send, a_recv, (row - 1, 0)).wait_recv()
        for k in range(2):
            total = a_in[k, 0]
            for s in range(1, n_col):
                total = total + a_in[k, s]
            a_sum[k] = total.astype(jnp.bfloat16)

    def gather_p(j, acc):
        home = lax.rem(j, n_col)

        @pl.when(home != col)
        def _():
            remote(p_in.at[j], p_in.at[j], p_send.at[0], p_recv.at[j], (row, home)).wait_recv()

        return acc - p_in[j]

    base[...] = lax.fori_loop(0, long_count, gather_p, base[...])

    @pl.when(is_even_end)
    def _():
        remote(p_in.at[whole], p_in.at[whole], p_send.at[0], p_recv.at[whole], (row + 1, whole_home)).wait_recv()
        base[...] -= p_in[whole]

    def send_w(out, into, send, recv, i):
        for s in range(n_col):
            remote(out, into.at[col], send, recv, (i, s)).start()

    def wait_w(into, send, recv, i):
        remote(into, into, send, recv, (i, 0)).wait_recv()
        total = into[0]
        for s in range(1, n_col):
            total = total + into[s]
        return total

    @pl.when(is_even_end)
    def _():
        w_out[...] = jnp.dot(base[...].astype(jnp.bfloat16), fold[...].astype(jnp.bfloat16), preferred_element_type=jnp.float32)
        send_w(w_out, w_in, w_send, w_recv, row + 1)

    @pl.when(handed)
    def _():
        @pl.when(jnp.logical_not(is_even_end))
        def _():
            shared_wait(l_in, k_recv, mine_home)

        l_part = l_in[...].astype(jnp.bfloat16)
        remote(wl_in, wl_in, wl_send, wl_recv, (row + 1, mine_home)).wait_recv()
        base[...] -= jnp.dot(wl_in[...].astype(jnp.bfloat16), l_part, preferred_element_type=jnp.float32)

    @pl.when(short & jnp.logical_not(is_end))
    def _():
        @pl.when(jnp.logical_not(is_even_end))
        def _():
            shared_wait(u_in, u_recv, prev_home)

        u_part = u_in[...].astype(jnp.bfloat16)
        inner = wait_w(w_in, w_send, w_recv, row - 1)
        base[...] -= jnp.dot(inner.astype(jnp.bfloat16), u_part, preferred_element_type=jnp.float32)

    @pl.when(is_end)
    def _():
        shared_wait(u_in, u_recv, prev_home)
        shared_wait(t_in, t_recv, far_home)
        u_part = u_in[...].astype(jnp.bfloat16)
        t_part = t_in[...].astype(jnp.bfloat16)

        @pl.when(jnp.logical_not(takes))
        def _():
            remote(wl_in, wl_in, wp_send, wl_recv, (row, their_home)).wait_recv()

        inner = wait_w(w_in, w_send, w_recv, row - 1)
        inner -= jnp.dot(wl_in[...].astype(jnp.bfloat16), a_sum[1], preferred_element_type=jnp.float32)
        late = wait_w(wx_in, wx_send, wx_recv, row - 2)
        base[...] -= jnp.dot(late.astype(jnp.bfloat16), t_part, preferred_element_type=jnp.float32)
        late = wait_w(we_in, we_send, we_recv, row - 2)
        inner -= jnp.dot(late.astype(jnp.bfloat16), a_sum[0], preferred_element_type=jnp.float32)
        base[...] -= jnp.dot(inner.astype(jnp.bfloat16), u_part, preferred_element_type=jnp.float32)

    reduced = base[...].astype(jnp.bfloat16)

    @pl.when((jnp.logical_not(even)) & (answers > 0))
    def _():
        pl.semaphore_wait(ready, answers)

    @pl.when(feeds & jnp.logical_not(is_even_end))
    def _():
        w_out[...] = jnp.dot(reduced, fold[...].astype(jnp.bfloat16), preferred_element_type=jnp.float32)

        @pl.when(is_ahead)
        def _():
            send_w(w_out, we_in, we_send, we_recv, row + 2)
            wx_out[...] = jnp.dot(reduced, fold_x[...].astype(jnp.bfloat16), preferred_element_type=jnp.float32)
            send_w(wx_out, wx_in, wx_send, wx_recv, row + 2)

        send_w(w_out, w_in, w_send, w_recv, row + 1)

    y_row[col] = jnp.dot(reduced, inv_ref[...], preferred_element_type=jnp.float32)

    def near_copy(i):
        return remote(y_row.at[col], y_in.at[own_slot, col], y_send.at[i], y_recv.at[own_slot], (i, own_home))

    def send_y(i, carry):
        @pl.when(row < longs_of(i))
        def _():
            near_copy(i).start()

        return carry

    lax.fori_loop(row + 1, near_end, send_y, 0)
    for peer in peers:
        remote(y_row.at[col], y_row.at[col], o_send, o_recv, (row, peer)).start()
    pl.when(row == 0)(log_part)

    remote(logs.at[others], logs.at[others], l_send, l_recv, (row, peers[0])).wait()
    log_sum = logs[0]
    for s in range(1, n_col):
        log_sum = log_sum + logs[s]
    log_term = log_sum * (1.0 / width) - 0.5 * math.log(2.0 * math.pi)

    def left_y(i, carry):
        @pl.when(row < longs_of(i))
        def _():
            near_copy(i).wait_send()

        return carry

    lax.fori_loop(row + 1, near_end, left_y, 0)

    @pl.when(feeds)
    def _():
        remote(w_in, w_in, w_send, w_recv, (row + 1, 0)).wait_send()

    @pl.when(is_ahead)
    def _():
        remote(w_in, w_in, we_send, we_recv, (row + 2, 0)).wait_send()
        remote(w_in, w_in, wx_send, wx_recv, (row + 2, 0)).wait_send()

    @pl.when(is_even_end)
    def _():
        remote(a_in, a_in, a_send, a_recv, (row + 1, 0)).wait_send()

    @pl.when(takes)
    def _():
        remote(w_in, w_in, wl_send, wl_recv, (row - 1, 0)).wait_send()

        @pl.when(is_end)
        def _():
            remote(w_in.at[others], w_in.at[others], wp_send, wl_recv, (row, peers[0])).wait_send()

    @pl.when(hands)
    def _():
        remote(d_out, d_in, d_send, d_recv, (row + 1, col)).wait_send()
        share_done(l_out)

    @pl.when(hands_whole)
    def _():
        remote(d_out, d_in, d_send, d_recv, (row + 1, col)).wait_send()
        remote(du_out, du_in, du_send, du_recv, (row + 1, col)).wait_send()

    @pl.when(takes_whole)
    def _():
        remote(pd_out, pd_out, pd_send, p_recv.at[0], (row - 1, 0)).wait_send()

    @pl.when(gives & even)
    def _():
        spread_done(v_out, prev_home, crosses)

    @pl.when(gives)
    def _():
        share_done(u_out)

    @pl.when(gives_far)
    def _():
        spread_done(x_out, far_home, jnp.bool_(True))
        share_done(t_out)

    @pl.when(crosses & (col != prev_home))
    def _():
        relay_done(v_out, prev_home)

    @pl.when(is_end & (col != far_home))
    def _():
        relay_done(x_out, far_home)

    for q in range(per_col):

        @pl.when(q * n_col + col < long_count)
        def _():
            part = p_out.at[q, others]
            remote(part, part, p_send.at[q], p_recv.at[0], (row, peers[0])).wait_send()

    remote(y_row.at[others], y_row.at[others], o_send, o_recv, (row, peers[0])).wait_recv()
    y = y_row[0]
    for s in range(1, n_col):
        y = y + y_row[s]
    y_all[...] = y

    def far_copy(i):
        return remote(y_all, y_in.at[own_slot, 0], y_send.at[i], y_recv.at[own_slot], (i, col))

    def send_far(i, carry):
        far_copy(i).start()
        return carry

    @pl.when((row == 0) & (answers > 0))
    def _():
        pl.semaphore_wait(ready, answers)

    lax.fori_loop(jnp.where(relays, near_end, n_row), n_row, send_far, 0)
    white_ref[0, 0] = y
    quadratic = jnp.sum(y * y, axis=1, keepdims=True) * (1.0 / width)
    lik = -0.5 * quadratic + log_term
    r_id = lax.broadcasted_iota(jnp.int32, (nrhs, 128), 0)
    c_id = lax.broadcasted_iota(jnp.int32, (nrhs, 128), 1)
    flat = jnp.sum(jnp.where(r_id == c_id, lik, 0.0), axis=0, keepdims=True)
    lik_ref[0] = flat[:, :nrhs]

    def left_far(i, carry):
        far_copy(i).wait_send()
        return carry

    lax.fori_loop(jnp.where(relays, near_end, n_row), n_row, left_far, 0)
    remote(y_row.at[others], y_row.at[others], o_send, o_recv, (row, peers[0])).wait_send()


def local(n_row, n_col, right_side, inverse_t, u_factor, v_factor, ranks):
    nrhs, width = right_side.shape[2:]
    per_col, _, rank_max = u_factor.shape[2:5]
    piece = width // n_col
    vmem = pl.BlockSpec(memory_space=pltpu.VMEM)
    hbm = pl.BlockSpec(memory_space=pl.ANY)
    dma = pltpu.SemaphoreType.DMA

    def f32(*shape):
        return pltpu.VMEM(shape, jnp.float32)

    def bf16(*shape):
        return pltpu.VMEM(shape, jnp.bfloat16)

    tile_set = [
        f32(n_col, rank_max, piece),
        f32(n_col, rank_max, piece),
        f32(n_col, rank_max, piece),
        f32(rank_max, piece),
        f32(piece, rank_max),
        f32(nrhs, rank_max),
        f32(n_col, nrhs, rank_max),
    ]
    return pl.pallas_call(
        functools.partial(kernel, n_row, n_col),
        out_shape=(
            pltpu.VMEM((1, 1, nrhs, width), jnp.float32),
            pltpu.VMEM((1, 1, nrhs), jnp.float32),
        ),
        in_specs=[hbm, hbm, hbm, hbm, hbm],
        out_specs=(vmem, vmem),
        scratch_shapes=[
            f32(nrhs, width),
            bf16(piece, width),
            bf16(per_col, rank_max, width),
            bf16(per_col, rank_max, width),
            pltpu.SMEM((per_col,), jnp.int32),
            f32(per_col, n_col, nrhs, width),
            f32(per_col, n_col, nrhs, piece),
            f32(n_row, nrhs, piece),
            f32(n_col, nrhs, width),
            f32(n_col, 1, 128),
            f32(nrhs, piece),
            f32(nrhs, width),
            f32(nrhs, width),
            *tile_set,
            *tile_set,
            f32(rank_max, width),
            f32(rank_max, width),
            bf16(rank_max, width),
            f32(rank_max, width),
            f32(rank_max, width),
            bf16(rank_max, width),
            f32(n_col, nrhs, piece),
            f32(n_col, rank_max, piece),
            f32(rank_max, piece),
            f32(nrhs, rank_max),
            f32(nrhs, rank_max),
            f32(n_col, nrhs, rank_max),
            f32(2, rank_max, rank_max),
            f32(2, n_col, rank_max, rank_max),
            bf16(2, rank_max, rank_max),
            dma((5,)),
            dma((n_row,)),
            dma((per_col,)),
            dma((per_col,)),
            dma((n_row,)),
            dma, dma, dma, dma,
            dma((n_col,)),
            dma, dma, dma, dma, dma,
            dma((n_col,)),
            dma, dma,
            pltpu.SemaphoreType.REGULAR,
            dma, dma, dma, dma, dma, dma, dma, dma,
            dma, dma, dma,
            dma, dma, dma, dma, dma, dma,
        ],
        compiler_params=pltpu.CompilerParams(collective_id=0, has_side_effects=True),
        name="forward_solve",
    )(right_side, inverse_t, u_factor, v_factor, ranks.reshape(per_col))


def solution(mesh):
    placed = (
        P(None, "row", None, None),
        P(None, "row", "col", None),
        P(None, "row", None, "col", None, None),
        P(None, "row", None, "col", None, None),
        P(None, "row", None, "col"),
    )
    return jax.shard_map(
        functools.partial(local, mesh.shape["row"], mesh.shape["col"]),
        mesh=mesh,
        in_specs=placed,
        out_specs=(P(None, "row", None, None), P(None, "row", None)),
        check_vma=False,
    )
```

```python
import functools
import math

import jax
import jax.numpy as jnp
from jax import lax
from jax.experimental import pallas as pl
from jax.experimental.pallas import tpu as pltpu
from jax.sharding import PartitionSpec as P

MESH = pl.DeviceIdType.MESH
NT = (((1,), (1,)), ((), ()))
FIRST_SHORT = 3
NEAR = 3


def remote(src, dst, send_sem, recv_sem, device):
    return pltpu.make_async_remote_copy(
        src_ref=src,
        dst_ref=dst,
        send_sem=send_sem,
        recv_sem=recv_sem,
        device_id=device,
        device_id_type=MESH,
    )


def kernel(
    n_row, n_col,
    rhs_hbm, inv_hbm, u_hbm, v_hbm, rank_hbm,
    white_ref, lik_ref,
    rhs_ref, inv_ref, u_ref, v_ref, rank_ref,
    y_in, p_out, p_in, y_row, logs, base, y_full, y_all,
    v_out, v_in, u_out, u_in, fold, w_out, w_in,
    x_out, x_in, t_out, t_in, fold_x, wx_out, wx_in,
    d_out, d_in, d_tile, du_out, du_in, du_tile, pd_out, l_out, l_in, wl_out, wl_in, we_in,
    a_out, a_in, a_sum,
    in_sem, y_send, y_recv, p_send, p_recv, o_send, o_recv, l_send, l_recv,
    v_send, v_recv, u_send, u_recv, w_send, w_recv, m_recv, f_send, e_send, ready,
    x_recv, t_recv, k_recv, d_send, d_recv, du_send, du_recv, pd_send, wl_send, wl_recv, wp_send,
    we_send, we_recv, wx_send, wx_recv, a_send, a_recv,
):
    row = lax.axis_index("row")
    col = lax.axis_index("col")
    per_col, rank_max, width = u_ref.shape
    nrhs = rhs_ref.shape[0]
    piece = width // n_col
    half = n_col // 2
    peers = [lax.rem(col + k, n_col) for k in range(1, n_col)]
    others = pl.ds(0, n_col - 1)
    own_slot = row // n_col
    own_home = lax.rem(row, n_col)
    end = n_row - 1
    even_end = n_row - 2
    ahead = n_row - 3

    def longs_of(i):
        count = jnp.where(i >= FIRST_SHORT, i - 1, i)
        handed = (lax.rem(i, 2) == 0) & (i >= 2)
        return count - jnp.where(handed, 1, 0) - jnp.where(i >= even_end, 1, 0)

    def near_of(i):
        return NEAR + jnp.where(i >= 2, 1, 0)

    copies = [
        pltpu.make_async_copy(v_hbm.at[0, 0, :, 0], v_ref, in_sem.at[0]),
        pltpu.make_async_copy(u_hbm.at[0, 0, :, 0], u_ref, in_sem.at[1]),
        pltpu.make_async_copy(inv_hbm.at[0, 0], inv_ref, in_sem.at[2]),
        pltpu.make_async_copy(rhs_hbm.at[0, 0], rhs_ref, in_sem.at[3]),
        pltpu.make_async_copy(rank_hbm, rank_ref, in_sem.at[4]),
    ]
    @pl.when(lax.axis_index("row") > 0)
    def _():
        copies[0].start()
        copies[1].start()

    for copy in copies[2:]:
        copy.start()

    even = lax.rem(row, 2) == 0
    short = row >= FIRST_SHORT
    feeds = (row + 1 >= FIRST_SHORT) & (row < end)
    is_end = row == end
    is_even_end = row == even_end
    is_ahead = row == ahead
    long_count = longs_of(row)
    near_end = jnp.minimum(row + near_of(row) + 1, n_row)
    relays = col == own_home

    barrier = pltpu.get_barrier_semaphore()

    def signal(sem, i, s):
        pl.semaphore_signal(sem, inc=1, device_id=(i, s), device_id_type=MESH)

    def row_of(i, cond, act):
        @pl.when(cond)
        def _():
            for s in range(n_col):
                act(i, s)

        return jnp.where(cond, n_col, 0)

    def above(act):
        yield row + 1, row_of(row + 1, row < end, act)
        for d in range(2, NEAR + 2):
            wide = is_ahead if d == 2 else jnp.bool_(False)
            one = (row + d < n_row) & (d <= near_of(row)) & jnp.logical_not(wide)

            @pl.when(one)
            def _():
                act(row + d, own_home)

            yield row + d, jnp.where(one, 1, 0)
            if d == 2:
                yield row + d, row_of(row + d, wide, act)

    def below(act):
        row_of(row - 1, row > 0, act)
        count = jnp.where(row > 0, n_col, 0)
        for d in range(2, NEAR + 2):
            fed = (row >= d) & (d <= near_of(row - d)) & (lax.rem(jnp.maximum(row - d, 0), n_col) == col)
            if d == 2:
                fed = fed | is_end
            count += row_of(row - d, fed, act)
        for q in range(per_col):
            j = q * n_col + col
            far = j < row - near_of(j)

            @pl.when(far)
            def _():
                act(j, col)

            count += jnp.where(far, 1, 0)
        return count

    def at_once(low, high):
        return (low == 0) & (high == 1)

    for peer in peers:
        signal(barrier, row, peer)
    greeted = jnp.int32(n_col - 1)
    answers = jnp.int32(0)
    for i, count in above(lambda i, s: signal(barrier, i, s)):
        quick = at_once(row, i)
        greeted += jnp.where(quick, count, 0)
        answers += jnp.where(quick, 0, count)

    def greet_far(i, count):
        signal(barrier, i, col)
        return count + 1

    answers = lax.fori_loop(jnp.where(relays, near_end, n_row), n_row, greet_far, answers)

    def greet_quick(i, s):
        @pl.when(at_once(i, row))
        def _():
            signal(barrier, i, s)

    def answer(i, s):
        @pl.when(jnp.logical_not(at_once(i, row)))
        def _():
            signal(ready, i, s)

    greeted += below(greet_quick)

    prev = jnp.maximum(row - 1, 0)
    prev_slot = prev // n_col
    prev_home = lax.rem(prev, n_col)
    gives = short & (col == prev_home)
    crosses = short & even
    far_slot = ahead // n_col
    far_home = ahead % n_col
    gives_far = is_end & (col == far_home)
    handed = even & (row >= 2)
    mine = jnp.where(handed, long_count + jnp.where(is_even_end, 1, 0), 0)
    mine_slot = mine // n_col
    mine_home = lax.rem(mine, n_col)
    hands = handed & (col == mine_home)
    taken = (row >= 3) & jnp.logical_not(even)
    theirs = jnp.where(taken, longs_of(prev) + jnp.where(is_end, 1, 0), 0)
    their_home = lax.rem(theirs, n_col)
    takes = taken & (col == their_home)
    whole = even_end - 3
    whole_slot = whole // n_col
    whole_home = whole % n_col
    hands_whole = is_even_end & (col == whole_home)
    takes_whole = is_end & (col == whole_home)

    def masked_u(slot):
        keep = lax.broadcasted_iota(jnp.int32, (rank_max, width), 0) < rank_ref[slot]
        return jnp.where(keep, u_ref[slot].astype(jnp.float32), 0.0)

    def cut(tile, into):
        for s in range(n_col):
            into[s] = tile[:, s * piece:(s + 1) * piece]

    @pl.when(row > 0)
    def _():
        copies[0].wait()
        copies[1].wait()

    copies[4].wait()

    @pl.when(hands)
    def _():
        d_out[...] = v_ref[mine_slot].astype(jnp.float32)
        cut(masked_u(mine_slot), l_out)

    @pl.when(hands_whole)
    def _():
        d_out[...] = v_ref[whole_slot].astype(jnp.float32)
        du_out[...] = masked_u(whole_slot)

    @pl.when(gives)
    def _():
        cut(v_ref[prev_slot].astype(jnp.float32), v_out)
        cut(masked_u(prev_slot), u_out)

    @pl.when(gives_far)
    def _():
        cut(v_ref[far_slot].astype(jnp.float32), x_out)
        cut(masked_u(far_slot), t_out)

    pl.semaphore_wait(barrier, greeted)
    below(answer)

    def by_way(home, s, cc):
        across = n_col - 1 - home
        return (home != s) & jnp.where(across < home, (across != s) | (cc < s + half), (s > home) | (cc < s + half))

    def is_late(home, s, cc):
        across = n_col - 1 - home
        return (across == s) & (across < home) & (cc >= s + half)

    def is_split(home, s):
        across = n_col - 1 - home
        return (across == s) & (across < home)

    def joined(home, s):
        across = n_col - 1 - home
        return (across > home) & (across == s)

    def spread(out, into, recv, target, home, cross):
        for s in range(n_col):
            if s > 0:

                @pl.when(cross & joined(home, s - 1))
                def _():
                    remote(out.at[s - 1], out.at[s - 1], v_send.at[s], m_recv.at[s - 1], (row, s)).start()

            for cc in range(s, n_col):
                gone = cross & (joined(home, s) | is_split(home, s))
                way = cross & by_way(home, s, cc)
                later = cross & is_late(home, s, cc)

                @pl.when(way & jnp.logical_not(gone))
                def _():
                    remote(out.at[cc], out.at[cc], v_send.at[s], m_recv.at[cc], (row, s)).start()

                @pl.when(jnp.logical_not(way | later | gone))
                def _():
                    remote(out.at[cc], into.at[cc], v_send.at[s], recv, (target, s)).start()

        for s in range(n_col):
            for cc in range(s, min(s + half, n_col)):

                @pl.when(cross & is_split(home, s))
                def _():
                    remote(out.at[cc], out.at[cc], v_send.at[s], m_recv.at[cc], (row, s)).start()

    def spread_late(out, into, recv, target, home):
        for s in range(1, n_col):

            @pl.when(is_split(home, s - 1))
            def _():
                part = pl.ds(s, n_col - s)
                remote(out.at[part], out.at[part], v_send.at[s], m_recv.at[0], (row, s)).wait_send()

        for s in range(n_col):
            for cc in range(min(s + half, n_col), n_col):

                @pl.when(is_late(home, s, cc))
                def _():
                    remote(out.at[cc], into.at[cc], v_send.at[s], recv, (target, s)).start()

    def spread_done(out, home, cross):
        for s in range(n_col):
            part = pl.ds(s, n_col - s)
            gone = cross & joined(home, s)
            if s > 0:
                gone = gone | (cross & is_split(home, s - 1))
            more = (cross & joined(home, s - 1)) if s > 0 else jnp.bool_(False)

            @pl.when(jnp.logical_not(gone | more))
            def _():
                remote(out.at[part], out.at[part], v_send.at[s], m_recv.at[0], (row, s)).wait_send()

            if s > 0:
                part_more = pl.ds(s - 1, n_col - s + 1)

                @pl.when(more)
                def _():
                    remote(out.at[part_more], out.at[part_more], v_send.at[s], m_recv.at[0], (row, s)).wait_send()

    def relay(out, into, recv, target, home):
        across = n_col - 1 - home
        more = joined(home, col - 1)
        first = jnp.where(more, col - 1, col)
        part = jnp.where(across < home, across == col, col < home)
        stop = jnp.where(part, jnp.minimum(col + half, n_col), n_col)

        def forward(cc, carry):
            remote(out.at[cc], out.at[cc], v_send.at[0], m_recv.at[cc], (row, home)).wait_recv()

            @pl.when(cc >= col)
            def _():
                remote(out.at[cc], into.at[cc], f_send, recv, (target, col)).start()

            @pl.when(more)
            def _():
                remote(out.at[cc], out.at[cc], e_send, m_recv.at[cc], (row, across)).start()

            return carry

        lax.fori_loop(first, stop, forward, 0)

    def relay_done(out, home):
        across = n_col - 1 - home
        for cc in range(n_col):
            few = pl.ds(cc, min(half, n_col - cc))
            here = col == cc
            half_way = jnp.where(across < home, across == cc, cc < home)

            @pl.when(here & jnp.logical_not(half_way))
            def _():
                part = pl.ds(cc, n_col - cc)
                remote(out.at[part], out.at[part], f_send, v_recv, (row, home)).wait_send()

            @pl.when(here & half_way)
            def _():
                remote(out.at[few], out.at[few], f_send, v_recv, (row, home)).wait_send()

            if cc > 0:

                @pl.when((col == cc) & joined(home, cc - 1))
                def _():
                    part = pl.ds(cc - 1, n_col - cc + 1)
                    remote(out.at[part], out.at[part], e_send, v_recv, (row, home)).wait_send()

    def share(out, into, recv):
        for peer in peers:
            remote(out.at[peer], into, u_send, recv, (row, peer)).start()
        into[...] = out[col]

    def share_done(out):
        remote(out.at[others], out.at[others], u_send, u_recv, (row, peers[0])).wait_send()

    def shared_wait(into, recv, home):
        @pl.when(col != home)
        def _():
            remote(into, into, u_send, recv, (row, home)).wait_recv()

    early_l = (row < FIRST_SHORT) | is_even_end

    @pl.when(hands & early_l)
    def _():
        share(l_out, l_in, k_recv)

    @pl.when(gives)
    def _():
        spread(v_out, v_in, v_recv, row - 1, prev_home, crosses)

    @pl.when(gives & is_even_end)
    def _():
        share(u_out, u_in, u_recv)

    @pl.when(gives_far)
    def _():
        spread(x_out, x_in, x_recv, row - 2, far_home, jnp.bool_(True))

    @pl.when((handed) & (answers > 0))
    def _():
        pl.semaphore_wait(ready, answers)

    @pl.when(hands | hands_whole)
    def _():
        remote(d_out, d_in, d_send, d_recv, (row + 1, col)).start()

    @pl.when(hands_whole)
    def _():
        remote(du_out, du_in, du_send, du_recv, (row + 1, col)).start()

    @pl.when(crosses & (col != prev_home))
    def _():
        relay(v_out, v_in, v_recv, row - 1, prev_home)

    copies[2].wait()
    copies[3].wait()

    for cc in range(n_col):

        @pl.when(col == cc)
        def _():
            base[...] = rhs_ref[:, cc * piece:(cc + 1) * piece]

    def log_part():
        for cc in range(n_col):

            @pl.when(col == cc)
            def _():
                block = inv_ref[:, cc * piece:(cc + 1) * piece].astype(jnp.float32)
                r_id = lax.broadcasted_iota(jnp.int32, (piece, piece), 0)
                c_id = lax.broadcasted_iota(jnp.int32, (piece, piece), 1)
                diagonal = jnp.sum(jnp.where(r_id == c_id, block, 0.0), axis=0, keepdims=True)
                total = jnp.sum(jnp.log(diagonal), axis=1, keepdims=True)
                logs[cc] = jnp.broadcast_to(total, (1, 128))

        for peer in peers:
            remote(logs.at[col], logs.at[col], l_send, l_recv, (row, peer)).start()

    pl.when(row > 0)(log_part)

    @pl.when(gives & crosses)
    def _():
        spread_late(v_out, v_in, v_recv, row - 1, prev_home)

    @pl.when(gives & jnp.logical_not(even))
    def _():
        spread_done(v_out, prev_home, crosses)
        share(u_out, u_in, u_recv)

    def fold_with(into, recv, target):
        target[...] = jnp.zeros_like(target)
        for cc in range(n_col):
            part = pl.ds(cc, n_col - cc)

            @pl.when(col == cc)
            def _():
                remote(into.at[part], into.at[part], f_send, recv, (row, cc)).wait_recv()

        for cc in range(n_col):

            @pl.when(col <= cc)
            def _():
                target[...] += lax.dot_general(
                    inv_ref[:, cc * piece:(cc + 1) * piece],
                    into[cc].astype(jnp.bfloat16),
                    NT,
                    preferred_element_type=jnp.float32,
                )

    def long_step(q):
        j = q * n_col + col

        @pl.when(j < long_count)
        def _():
            near = row - j <= near_of(j)

            @pl.when(near)
            def _():
                remote(y_in.at[q], y_in.at[q], y_send.at[0], y_recv.at[q], (j, col)).wait_recv()
                y = y_in[q, 0]
                for s in range(1, n_col):
                    y = y + y_in[q, s]
                y_full[...] = y

            @pl.when(jnp.logical_not(near))
            def _():
                remote(y_in.at[q, 0], y_in.at[q, 0], y_send.at[0], y_recv.at[q], (j, col)).wait_recv()
                y_full[...] = y_in[q, 0]

            y = y_full[...].astype(jnp.bfloat16)

            @pl.when(takes & (j == theirs))
            def _():
                wl_out[...] = lax.dot_general(y, d_tile[...], NT, preferred_element_type=jnp.float32)
                for s in range(n_col):
                    remote(wl_out, wl_in, wl_send, wl_recv, (row - 1, s)).start()

                @pl.when(is_end)
                def _():
                    for peer in peers:
                        remote(wl_out, wl_in, wp_send, wl_recv, (row, peer)).start()
                    wl_in[...] = wl_out[...]

            @pl.when(takes_whole & (j == whole))
            def _():
                inner = lax.dot_general(y, d_tile[...], NT, preferred_element_type=jnp.float32)
                p = jnp.dot(inner.astype(jnp.bfloat16), du_tile[...], preferred_element_type=jnp.float32)
                for s in range(n_col):
                    pd_out[s] = p[:, s * piece:(s + 1) * piece]
                    remote(pd_out.at[s], p_in.at[j], pd_send, p_recv.at[j], (row - 1, s)).start()

            inner = lax.dot_general(y, v_ref[q], NT, preferred_element_type=jnp.float32)
            keep = lax.broadcasted_iota(jnp.int32, (nrhs, rank_max), 1) < rank_ref[q]
            inner = jnp.where(keep, inner, 0.0).astype(jnp.bfloat16)
            p = jnp.dot(inner, u_ref[q], preferred_element_type=jnp.float32)
            for s in range(n_col):
                p_out[q, s] = p[:, s * piece:(s + 1) * piece]
            for peer in peers:
                remote(p_out.at[q, peer], p_in.at[j], p_send.at[q], p_recv.at[j], (row, peer)).start()
            p_in[j] = p_out[q, col]

    @pl.when(takes | takes_whole)
    def _():
        remote(d_in, d_in, d_send, d_recv, (row - 1, col)).wait_recv()
        d_tile[...] = d_in[...].astype(jnp.bfloat16)

    @pl.when(takes_whole)
    def _():
        remote(du_in, du_in, du_send, du_recv, (row - 1, col)).wait_recv()
        du_tile[...] = du_in[...].astype(jnp.bfloat16)

    @pl.when(is_end & (col != far_home))
    def _():
        relay(x_out, x_in, x_recv, row - 2, far_home)

    for q in range(per_col):
        long_step(q)

    @pl.when(is_even_end)
    def _():
        fold_with(v_in, v_recv, fold)
        factor = fold[...].astype(jnp.bfloat16)
        shared_wait(u_in, u_recv, prev_home)
        shared_wait(l_in, k_recv, mine_home)
        a_out[0] = jnp.dot(u_in[...].astype(jnp.bfloat16), factor, preferred_element_type=jnp.float32)
        a_out[1] = jnp.dot(l_in[...].astype(jnp.bfloat16), factor, preferred_element_type=jnp.float32)
        for k in range(2):
            for s in range(n_col):
                remote(a_out.at[k], a_in.at[k, col], a_send, a_recv, (row + 1, s)).start()

    @pl.when(feeds & jnp.logical_not(is_even_end))
    def _():
        fold_with(v_in, v_recv, fold)

    @pl.when(gives & crosses & jnp.logical_not(is_even_end))
    def _():
        share(u_out, u_in, u_recv)

    @pl.when(hands & jnp.logical_not(early_l))
    def _():
        share(l_out, l_in, k_recv)

    @pl.when(gives_far)
    def _():
        spread_late(x_out, x_in, x_recv, row - 2, far_home)
        share(t_out, t_in, t_recv)

    @pl.when(is_ahead)
    def _():
        fold_with(x_in, x_recv, fold_x)

    @pl.when(is_end)
    def _():
        remote(a_in, a_in, a_send, a_recv, (row - 1, 0)).wait_recv()
        for k in range(2):
            total = a_in[k, 0]
            for s in range(1, n_col):
                total = total + a_in[k, s]
            a_sum[k] = total.astype(jnp.bfloat16)

    def gather_p(j, acc):
        home = lax.rem(j, n_col)

        @pl.when(home != col)
        def _():
            remote(p_in.at[j], p_in.at[j], p_send.at[0], p_recv.at[j], (row, home)).wait_recv()

        return acc - p_in[j]

    base[...] = lax.fori_loop(0, long_count, gather_p, base[...])

    @pl.when(is_even_end)
    def _():
        remote(p_in.at[whole], p_in.at[whole], p_send.at[0], p_recv.at[whole], (row + 1, whole_home)).wait_recv()
        base[...] -= p_in[whole]

    def send_w(out, into, send, recv, i):
        for s in range(n_col):
            remote(out, into.at[col], send, recv, (i, s)).start()

    def wait_w(into, send, recv, i):
        remote(into, into, send, recv, (i, 0)).wait_recv()
        total = into[0]
        for s in range(1, n_col):
            total = total + into[s]
        return total

    @pl.when(is_even_end)
    def _():
        w_out[...] = jnp.dot(base[...].astype(jnp.bfloat16), fold[...].astype(jnp.bfloat16), preferred_element_type=jnp.float32)
        send_w(w_out, w_in, w_send, w_recv, row + 1)

    @pl.when(handed)
    def _():
        @pl.when(jnp.logical_not(is_even_end))
        def _():
            shared_wait(l_in, k_recv, mine_home)

        l_part = l_in[...].astype(jnp.bfloat16)
        remote(wl_in, wl_in, wl_send, wl_recv, (row + 1, mine_home)).wait_recv()
        base[...] -= jnp.dot(wl_in[...].astype(jnp.bfloat16), l_part, preferred_element_type=jnp.float32)

    @pl.when(short & jnp.logical_not(is_end))
    def _():
        @pl.when(jnp.logical_not(is_even_end))
        def _():
            shared_wait(u_in, u_recv, prev_home)

        u_part = u_in[...].astype(jnp.bfloat16)
        inner = wait_w(w_in, w_send, w_recv, row - 1)
        base[...] -= jnp.dot(inner.astype(jnp.bfloat16), u_part, preferred_element_type=jnp.float32)

    @pl.when(is_end)
    def _():
        shared_wait(u_in, u_recv, prev_home)
        shared_wait(t_in, t_recv, far_home)
        u_part = u_in[...].astype(jnp.bfloat16)
        t_part = t_in[...].astype(jnp.bfloat16)

        @pl.when(jnp.logical_not(takes))
        def _():
            remote(wl_in, wl_in, wp_send, wl_recv, (row, their_home)).wait_recv()

        inner = wait_w(w_in, w_send, w_recv, row - 1)
        inner -= jnp.dot(wl_in[...].astype(jnp.bfloat16), a_sum[1], preferred_element_type=jnp.float32)
        late = wait_w(wx_in, wx_send, wx_recv, row - 2)
        base[...] -= jnp.dot(late.astype(jnp.bfloat16), t_part, preferred_element_type=jnp.float32)
        late = wait_w(we_in, we_send, we_recv, row - 2)
        inner -= jnp.dot(late.astype(jnp.bfloat16), a_sum[0], preferred_element_type=jnp.float32)
        base[...] -= jnp.dot(inner.astype(jnp.bfloat16), u_part, preferred_element_type=jnp.float32)

    reduced = base[...].astype(jnp.bfloat16)

    @pl.when((jnp.logical_not(even)) & (answers > 0))
    def _():
        pl.semaphore_wait(ready, answers)

    @pl.when(feeds & jnp.logical_not(is_even_end))
    def _():
        w_out[...] = jnp.dot(reduced, fold[...].astype(jnp.bfloat16), preferred_element_type=jnp.float32)

        @pl.when(is_ahead)
        def _():
            send_w(w_out, we_in, we_send, we_recv, row + 2)
            wx_out[...] = jnp.dot(reduced, fold_x[...].astype(jnp.bfloat16), preferred_element_type=jnp.float32)
            send_w(wx_out, wx_in, wx_send, wx_recv, row + 2)

        send_w(w_out, w_in, w_send, w_recv, row + 1)

    y_row[col] = jnp.dot(reduced, inv_ref[...], preferred_element_type=jnp.float32)

    def near_copy(i):
        return remote(y_row.at[col], y_in.at[own_slot, col], y_send.at[i], y_recv.at[own_slot], (i, own_home))

    def send_y(i, carry):
        @pl.when(row < longs_of(i))
        def _():
            near_copy(i).start()

        return carry

    first = row == 0
    lax.fori_loop(row + 1, jnp.where(first, 2, near_end), send_y, 0)
    for peer in peers:
        remote(y_row.at[col], y_row.at[col], o_send, o_recv, (row, peer)).start()

    @pl.when(first)
    def _():
        log_part()
        pl.semaphore_wait(ready, answers)
        lax.fori_loop(2, near_end, send_y, 0)

    remote(logs.at[others], logs.at[others], l_send, l_recv, (row, peers[0])).wait()
    log_sum = logs[0]
    for s in range(1, n_col):
        log_sum = log_sum + logs[s]
    log_term = log_sum * (1.0 / width) - 0.5 * math.log(2.0 * math.pi)

    def left_y(i, carry):
        @pl.when(row < longs_of(i))
        def _():
            near_copy(i).wait_send()

        return carry

    lax.fori_loop(row + 1, near_end, left_y, 0)

    @pl.when(feeds)
    def _():
        remote(w_in, w_in, w_send, w_recv, (row + 1, 0)).wait_send()

    @pl.when(is_ahead)
    def _():
        remote(w_in, w_in, we_send, we_recv, (row + 2, 0)).wait_send()
        remote(w_in, w_in, wx_send, wx_recv, (row + 2, 0)).wait_send()

    @pl.when(is_even_end)
    def _():
        remote(a_in, a_in, a_send, a_recv, (row + 1, 0)).wait_send()

    @pl.when(takes)
    def _():
        remote(w_in, w_in, wl_send, wl_recv, (row - 1, 0)).wait_send()

        @pl.when(is_end)
        def _():
            remote(w_in.at[others], w_in.at[others], wp_send, wl_recv, (row, peers[0])).wait_send()

    @pl.when(hands)
    def _():
        remote(d_out, d_in, d_send, d_recv, (row + 1, col)).wait_send()
        share_done(l_out)

    @pl.when(hands_whole)
    def _():
        remote(d_out, d_in, d_send, d_recv, (row + 1, col)).wait_send()
        remote(du_out, du_in, du_send, du_recv, (row + 1, col)).wait_send()

    @pl.when(takes_whole)
    def _():
        remote(pd_out, pd_out, pd_send, p_recv.at[0], (row - 1, 0)).wait_send()

    @pl.when(gives & even)
    def _():
        spread_done(v_out, prev_home, crosses)

    @pl.when(gives)
    def _():
        share_done(u_out)

    @pl.when(gives_far)
    def _():
        spread_done(x_out, far_home, jnp.bool_(True))
        share_done(t_out)

    @pl.when(crosses & (col != prev_home))
    def _():
        relay_done(v_out, prev_home)

    @pl.when(is_end & (col != far_home))
    def _():
        relay_done(x_out, far_home)

    for q in range(per_col):

        @pl.when(q * n_col + col < long_count)
        def _():
            part = p_out.at[q, others]
            remote(part, part, p_send.at[q], p_recv.at[0], (row, peers[0])).wait_send()

    remote(y_row.at[others], y_row.at[others], o_send, o_recv, (row, peers[0])).wait_recv()
    y = y_row[0]
    for s in range(1, n_col):
        y = y + y_row[s]
    y_all[...] = y

    def far_copy(i):
        return remote(y_all, y_in.at[own_slot, 0], y_send.at[i], y_recv.at[own_slot], (i, col))

    def send_far(i, carry):
        far_copy(i).start()
        return carry

    lax.fori_loop(jnp.where(relays, near_end, n_row), n_row, send_far, 0)
    white_ref[0, 0] = y
    quadratic = jnp.sum(y * y, axis=1, keepdims=True) * (1.0 / width)
    lik = -0.5 * quadratic + log_term
    r_id = lax.broadcasted_iota(jnp.int32, (nrhs, 128), 0)
    c_id = lax.broadcasted_iota(jnp.int32, (nrhs, 128), 1)
    flat = jnp.sum(jnp.where(r_id == c_id, lik, 0.0), axis=0, keepdims=True)
    lik_ref[0] = flat[:, :nrhs]

    def left_far(i, carry):
        far_copy(i).wait_send()
        return carry

    lax.fori_loop(jnp.where(relays, near_end, n_row), n_row, left_far, 0)
    remote(y_row.at[others], y_row.at[others], o_send, o_recv, (row, peers[0])).wait_send()


def local(n_row, n_col, right_side, inverse_t, u_factor, v_factor, ranks):
    nrhs, width = right_side.shape[2:]
    per_col, _, rank_max = u_factor.shape[2:5]
    piece = width // n_col
    vmem = pl.BlockSpec(memory_space=pltpu.VMEM)
    hbm = pl.BlockSpec(memory_space=pl.ANY)
    dma = pltpu.SemaphoreType.DMA

    def f32(*shape):
        return pltpu.VMEM(shape, jnp.float32)

    def bf16(*shape):
        return pltpu.VMEM(shape, jnp.bfloat16)

    tile_set = [
        f32(n_col, rank_max, piece),
        f32(n_col, rank_max, piece),
        f32(n_col, rank_max, piece),
        f32(rank_max, piece),
        f32(piece, rank_max),
        f32(nrhs, rank_max),
        f32(n_col, nrhs, rank_max),
    ]
    return pl.pallas_call(
        functools.partial(kernel, n_row, n_col),
        out_shape=(
            pltpu.VMEM((1, 1, nrhs, width), jnp.float32),
            pltpu.VMEM((1, 1, nrhs), jnp.float32),
        ),
        in_specs=[hbm, hbm, hbm, hbm, hbm],
        out_specs=(vmem, vmem),
        scratch_shapes=[
            f32(nrhs, width),
            bf16(piece, width),
            bf16(per_col, rank_max, width),
            bf16(per_col, rank_max, width),
            pltpu.SMEM((per_col,), jnp.int32),
            f32(per_col, n_col, nrhs, width),
            f32(per_col, n_col, nrhs, piece),
            f32(n_row, nrhs, piece),
            f32(n_col, nrhs, width),
            f32(n_col, 1, 128),
            f32(nrhs, piece),
            f32(nrhs, width),
            f32(nrhs, width),
            *tile_set,
            *tile_set,
            f32(rank_max, width),
            f32(rank_max, width),
            bf16(rank_max, width),
            f32(rank_max, width),
            f32(rank_max, width),
            bf16(rank_max, width),
            f32(n_col, nrhs, piece),
            f32(n_col, rank_max, piece),
            f32(rank_max, piece),
            f32(nrhs, rank_max),
            f32(nrhs, rank_max),
            f32(n_col, nrhs, rank_max),
            f32(2, rank_max, rank_max),
            f32(2, n_col, rank_max, rank_max),
            bf16(2, rank_max, rank_max),
            dma((5,)),
            dma((n_row,)),
            dma((per_col,)),
            dma((per_col,)),
            dma((n_row,)),
            dma, dma, dma, dma,
            dma((n_col,)),
            dma, dma, dma, dma, dma,
            dma((n_col,)),
            dma, dma,
            pltpu.SemaphoreType.REGULAR,
            dma, dma, dma, dma, dma, dma, dma, dma,
            dma, dma, dma,
            dma, dma, dma, dma, dma, dma,
        ],
        compiler_params=pltpu.CompilerParams(collective_id=0, has_side_effects=True),
        name="forward_solve",
    )(right_side, inverse_t, u_factor, v_factor, ranks.reshape(per_col))


def solution(mesh):
    placed = (
        P(None, "row", None, None),
        P(None, "row", "col", None),
        P(None, "row", None, "col", None, None),
        P(None, "row", None, "col", None, None),
        P(None, "row", None, "col"),
    )
    return jax.shard_map(
        functools.partial(local, mesh.shape["row"], mesh.shape["col"]),
        mesh=mesh,
        in_specs=placed,
        out_specs=(P(None, "row", None, None), P(None, "row", None)),
        check_vma=False,
    )
```

```python
import functools
import math

import jax
import jax.numpy as jnp
from jax import lax
from jax.experimental import pallas as pl
from jax.experimental.pallas import tpu as pltpu
from jax.sharding import PartitionSpec as P

MESH = pl.DeviceIdType.MESH
NT = (((1,), (1,)), ((), ()))
FIRST_SHORT = 3
NEAR = 3


def remote(src, dst, send_sem, recv_sem, device):
    return pltpu.make_async_remote_copy(
        src_ref=src,
        dst_ref=dst,
        send_sem=send_sem,
        recv_sem=recv_sem,
        device_id=device,
        device_id_type=MESH,
    )


def kernel(
    n_row, n_col,
    rhs_hbm, inv_hbm, u_hbm, v_hbm, rank_hbm,
    white_ref, lik_ref,
    rhs_ref, inv_ref, u_ref, v_ref, rank_ref,
    y_in, p_out, p_in, y_row, logs, base, y_full, y_all,
    v_out, v_in, u_out, u_in, fold, w_out, w_in,
    x_out, x_in, t_out, t_in, fold_x, wx_out, wx_in,
    d_out, d_in, d_tile, du_out, du_in, du_tile, pd_out, l_out, l_in, wl_out, wl_in, we_in,
    a_out, a_in, a_sum,
    in_sem, y_send, y_recv, p_send, p_recv, o_send, o_recv, l_send, l_recv,
    v_send, v_recv, u_send, u_recv, w_send, w_recv, m_recv, f_send, e_send, ready,
    x_recv, t_recv, k_recv, d_send, d_recv, du_send, du_recv, pd_send, wl_send, wl_recv, wp_send,
    we_send, we_recv, wx_send, wx_recv, a_send, a_recv,
):
    row = lax.axis_index("row")
    col = lax.axis_index("col")
    per_col, rank_max, width = u_ref.shape
    nrhs = rhs_ref.shape[0]
    piece = width // n_col
    half = n_col // 2
    some = max(n_col // 4, 1)
    peers = [lax.rem(col + k, n_col) for k in range(1, n_col)]
    others = pl.ds(0, n_col - 1)
    own_slot = row // n_col
    own_home = lax.rem(row, n_col)
    end = n_row - 1
    even_end = n_row - 2
    ahead = n_row - 3

    def longs_of(i):
        count = jnp.where(i >= FIRST_SHORT, i - 1, i)
        handed = (lax.rem(i, 2) == 0) & (i >= 2)
        return count - jnp.where(handed, 1, 0) - jnp.where(i >= even_end, 1, 0)

    def near_of(i):
        return NEAR + jnp.where(i >= 2, 1, 0)

    copies = [
        pltpu.make_async_copy(v_hbm.at[0, 0, :, 0], v_ref, in_sem.at[0]),
        pltpu.make_async_copy(u_hbm.at[0, 0, :, 0], u_ref, in_sem.at[1]),
        None,
        pltpu.make_async_copy(rhs_hbm.at[0, 0], rhs_ref, in_sem.at[3]),
        pltpu.make_async_copy(rank_hbm, rank_ref, in_sem.at[4]),
    ]
    @pl.when(lax.axis_index("row") > 0)
    def _():
        copies[0].start()
        copies[1].start()

    def tail_of(c):
        start = c * piece // 128 * 128
        return pl.ds(start, width - start)

    def inverse_copy(c):
        return pltpu.make_async_copy(inv_hbm.at[0, 0, :, tail_of(c)], inv_ref.at[:, tail_of(c)], in_sem.at[2])

    def by_col(act):
        for c in range(n_col):
            pl.when(col == c)(functools.partial(act, c))

    by_col(lambda c: inverse_copy(c).start())
    for copy in copies[3:]:
        copy.start()

    for s in range(1, n_col):
        start = s * piece // 128 * 128
        if start:
            y_row[s, :, :start] = jnp.zeros((nrhs, start), jnp.float32)
            for q in range(per_col):
                y_in[q, s, :, :start] = jnp.zeros((nrhs, start), jnp.float32)

    even = lax.rem(row, 2) == 0
    short = row >= FIRST_SHORT
    feeds = (row + 1 >= FIRST_SHORT) & (row < end)
    is_end = row == end
    is_even_end = row == even_end
    is_ahead = row == ahead
    long_count = longs_of(row)
    near_end = jnp.minimum(row + near_of(row) + 1, n_row)
    relays = col == own_home

    barrier = pltpu.get_barrier_semaphore()

    def signal(sem, i, s):
        pl.semaphore_signal(sem, inc=1, device_id=(i, s), device_id_type=MESH)

    def row_of(i, cond, act):
        @pl.when(cond)
        def _():
            for s in range(n_col):
                act(i, s)

        return jnp.where(cond, n_col, 0)

    def above(act):
        yield row + 1, row_of(row + 1, row < end, act)
        for d in range(2, NEAR + 2):
            wide = is_ahead if d == 2 else jnp.bool_(False)
            one = (row + d < n_row) & (d <= near_of(row)) & jnp.logical_not(wide)

            @pl.when(one)
            def _():
                act(row + d, own_home)

            yield row + d, jnp.where(one, 1, 0)
            if d == 2:
                yield row + d, row_of(row + d, wide, act)

    def below(act):
        row_of(row - 1, row > 0, act)
        count = jnp.where(row > 0, n_col, 0)
        for d in range(2, NEAR + 2):
            fed = (row >= d) & (d <= near_of(row - d)) & (lax.rem(jnp.maximum(row - d, 0), n_col) == col)
            if d == 2:
                fed = fed | is_end
            count += row_of(row - d, fed, act)
        for q in range(per_col):
            j = q * n_col + col
            far = j < row - near_of(j)

            @pl.when(far)
            def _():
                act(j, col)

            count += jnp.where(far, 1, 0)
        return count

    def at_once(low, high):
        return (low == 0) & (high == 1)

    for peer in peers:
        signal(barrier, row, peer)
    greeted = jnp.int32(n_col - 1)
    answers = jnp.int32(0)
    for i, count in above(lambda i, s: signal(barrier, i, s)):
        quick = at_once(row, i)
        greeted += jnp.where(quick, count, 0)
        answers += jnp.where(quick, 0, count)

    def greet_far(i, count):
        signal(barrier, i, col)
        return count + 1

    answers = lax.fori_loop(jnp.where(relays, near_end, n_row), n_row, greet_far, answers)

    def greet_quick(i, s):
        @pl.when(at_once(i, row))
        def _():
            signal(barrier, i, s)

    def answer(i, s):
        @pl.when(jnp.logical_not(at_once(i, row)))
        def _():
            signal(ready, i, s)

    greeted += below(greet_quick)

    prev = jnp.maximum(row - 1, 0)
    prev_slot = prev // n_col
    prev_home = lax.rem(prev, n_col)
    gives = short & (col == prev_home)
    crosses = short & even
    far_slot = ahead // n_col
    far_home = ahead % n_col
    gives_far = is_end & (col == far_home)
    handed = even & (row >= 2)
    mine = jnp.where(handed, long_count + jnp.where(is_even_end, 1, 0), 0)
    mine_slot = mine // n_col
    mine_home = lax.rem(mine, n_col)
    hands = handed & (col == mine_home)
    taken = (row >= 3) & jnp.logical_not(even)
    theirs = jnp.where(taken, longs_of(prev) + jnp.where(is_end, 1, 0), 0)
    their_home = lax.rem(theirs, n_col)
    takes = taken & (col == their_home)
    whole = even_end - 3
    whole_slot = whole // n_col
    whole_home = whole % n_col
    hands_whole = is_even_end & (col == whole_home)
    takes_whole = is_end & (col == whole_home)

    def masked_u(slot):
        keep = lax.broadcasted_iota(jnp.int32, (rank_max, width), 0) < rank_ref[slot]
        return jnp.where(keep, u_ref[slot].astype(jnp.float32), 0.0)

    def cut(tile, into):
        for s in range(n_col):
            into[s] = tile[:, s * piece:(s + 1) * piece]

    @pl.when(row > 0)
    def _():
        copies[0].wait()
        copies[1].wait()

    copies[4].wait()

    @pl.when(hands)
    def _():
        d_out[...] = v_ref[mine_slot].astype(jnp.float32)
        cut(masked_u(mine_slot), l_out)

    @pl.when(hands_whole)
    def _():
        d_out[...] = v_ref[whole_slot].astype(jnp.float32)
        du_out[...] = masked_u(whole_slot)

    @pl.when(gives)
    def _():
        cut(v_ref[prev_slot].astype(jnp.float32), v_out)
        cut(masked_u(prev_slot), u_out)

    @pl.when(gives_far)
    def _():
        cut(v_ref[far_slot].astype(jnp.float32), x_out)
        cut(masked_u(far_slot), t_out)

    pl.semaphore_wait(barrier, greeted)
    below(answer)

    def by_way(home, s, cc):
        across = n_col - 1 - home
        return (home != s) & jnp.where(across < home, (across != s) | (cc < s + some), (s > home) | (cc < s + half))

    def is_late(home, s, cc):
        across = n_col - 1 - home
        return (across == s) & (across < home) & (cc >= s + some)

    def split_row(home):
        return n_col - 1 - home < home

    def is_split(home, s):
        across = n_col - 1 - home
        return (across == s) & (across < home)

    def joined(home, s):
        across = n_col - 1 - home
        return (across > home) & (across == s)

    def spread(out, into, recv, target, home, cross):
        for s in range(n_col):
            if s > 0:

                @pl.when(cross & joined(home, s - 1))
                def _():
                    remote(out.at[s - 1], out.at[s - 1], v_send.at[s], m_recv.at[s - 1], (row, s)).start()

            for cc in range(s, n_col):
                gone = cross & (joined(home, s) | is_split(home, s))
                way = cross & by_way(home, s, cc)
                later = cross & is_late(home, s, cc)

                @pl.when(way & jnp.logical_not(gone))
                def _():
                    remote(out.at[cc], out.at[cc], v_send.at[s], m_recv.at[cc], (row, s)).start()

                @pl.when(jnp.logical_not(way | later | gone))
                def _():
                    remote(out.at[cc], into.at[cc], v_send.at[s], recv, (target, s)).start()

        for s in range(n_col):
            for cc in range(s, min(s + some, n_col)):

                @pl.when(cross & is_split(home, s))
                def _():
                    remote(out.at[cc], out.at[cc], v_send.at[s], m_recv.at[cc], (row, s)).start()

    def spread_late(out, into, recv, target, home):
        for s in range(n_col - 1):

            @pl.when(split_row(home) & (home == s + 1))
            def _():
                part = pl.ds(s, n_col - s)
                remote(out.at[part], out.at[part], v_send.at[s], m_recv.at[0], (row, s)).wait_send()

        for s in range(n_col):
            for cc in range(min(s + some, n_col), n_col):

                @pl.when(is_late(home, s, cc))
                def _():
                    remote(out.at[cc], into.at[cc], v_send.at[s], recv, (target, s)).start()

    def spread_done(out, home, cross):
        for s in range(n_col):
            part = pl.ds(s, n_col - s)
            gone = cross & joined(home, s)
            gone = gone | (cross & split_row(home) & (home == s + 1))
            more = (cross & joined(home, s - 1)) if s > 0 else jnp.bool_(False)

            @pl.when(jnp.logical_not(gone | more))
            def _():
                remote(out.at[part], out.at[part], v_send.at[s], m_recv.at[0], (row, s)).wait_send()

            if s > 0:
                part_more = pl.ds(s - 1, n_col - s + 1)

                @pl.when(more)
                def _():
                    remote(out.at[part_more], out.at[part_more], v_send.at[s], m_recv.at[0], (row, s)).wait_send()

    def relay(out, into, recv, target, home):
        across = n_col - 1 - home
        more = joined(home, col - 1)
        first = jnp.where(more, col - 1, col)
        part = jnp.where(across < home, across == col, col < home)
        share_of = jnp.where(across < home, some, half)
        stop = jnp.where(part, jnp.minimum(col + share_of, n_col), n_col)

        def forward(cc, carry):
            remote(out.at[cc], out.at[cc], v_send.at[0], m_recv.at[cc], (row, home)).wait_recv()

            @pl.when(cc >= col)
            def _():
                remote(out.at[cc], into.at[cc], f_send, recv, (target, col)).start()

            @pl.when(more)
            def _():
                remote(out.at[cc], out.at[cc], e_send, m_recv.at[cc], (row, across)).start()

            return carry

        lax.fori_loop(first, stop, forward, 0)

    def relay_done(out, home):
        across = n_col - 1 - home
        for cc in range(n_col):
            here = col == cc
            half_way = jnp.where(across < home, across == cc, cc < home)

            @pl.when(here & jnp.logical_not(half_way))
            def _():
                part = pl.ds(cc, n_col - cc)
                remote(out.at[part], out.at[part], f_send, v_recv, (row, home)).wait_send()

            for count, cond in ((some, across < home), (half, across > home)):
                few = pl.ds(cc, min(count, n_col - cc))

                @pl.when(here & half_way & cond)
                def _():
                    remote(out.at[few], out.at[few], f_send, v_recv, (row, home)).wait_send()

            if cc > 0:

                @pl.when((col == cc) & joined(home, cc - 1))
                def _():
                    part = pl.ds(cc - 1, n_col - cc + 1)
                    remote(out.at[part], out.at[part], e_send, v_recv, (row, home)).wait_send()

    def share(out, into, recv):
        for peer in peers:
            remote(out.at[peer], into, u_send, recv, (row, peer)).start()
        into[...] = out[col]

    def share_done(out):
        remote(out.at[others], out.at[others], u_send, u_recv, (row, peers[0])).wait_send()

    def shared_wait(into, recv, home):
        @pl.when(col != home)
        def _():
            remote(into, into, u_send, recv, (row, home)).wait_recv()

    early_l = (row < FIRST_SHORT) | is_even_end

    @pl.when(hands & early_l)
    def _():
        share(l_out, l_in, k_recv)

    @pl.when(gives)
    def _():
        spread(v_out, v_in, v_recv, row - 1, prev_home, crosses)

    @pl.when(gives & is_even_end)
    def _():
        share(u_out, u_in, u_recv)

    @pl.when(gives_far)
    def _():
        spread(x_out, x_in, x_recv, row - 2, far_home, jnp.bool_(True))

    @pl.when((handed) & (answers > 0))
    def _():
        pl.semaphore_wait(ready, answers)

    @pl.when(hands | hands_whole)
    def _():
        remote(d_out, d_in, d_send, d_recv, (row + 1, col)).start()

    @pl.when(hands_whole)
    def _():
        remote(du_out, du_in, du_send, du_recv, (row + 1, col)).start()

    @pl.when(crosses & (col != prev_home))
    def _():
        relay(v_out, v_in, v_recv, row - 1, prev_home)

    by_col(lambda c: inverse_copy(c).wait())
    copies[3].wait()

    for cc in range(n_col):

        @pl.when(col == cc)
        def _():
            base[...] = rhs_ref[:, cc * piece:(cc + 1) * piece]

    def log_part():
        for cc in range(n_col):

            @pl.when(col == cc)
            def _():
                block = inv_ref[:, cc * piece:(cc + 1) * piece].astype(jnp.float32)
                r_id = lax.broadcasted_iota(jnp.int32, (piece, piece), 0)
                c_id = lax.broadcasted_iota(jnp.int32, (piece, piece), 1)
                diagonal = jnp.sum(jnp.where(r_id == c_id, block, 0.0), axis=0, keepdims=True)
                total = jnp.sum(jnp.log(diagonal), axis=1, keepdims=True)
                logs[cc] = jnp.broadcast_to(total, (1, 128))

        for peer in peers:
            remote(logs.at[col], logs.at[col], l_send, l_recv, (row, peer)).start()

    pl.when(row > 0)(log_part)

    @pl.when(gives & crosses)
    def _():
        spread_late(v_out, v_in, v_recv, row - 1, prev_home)

    @pl.when(gives & jnp.logical_not(even))
    def _():
        spread_done(v_out, prev_home, crosses)
        share(u_out, u_in, u_recv)

    def fold_with(into, recv, target):
        target[...] = jnp.zeros_like(target)
        for cc in range(n_col):
            part = pl.ds(cc, n_col - cc)

            @pl.when(col == cc)
            def _():
                remote(into.at[part], into.at[part], f_send, recv, (row, cc)).wait_recv()

        for cc in range(n_col):

            @pl.when(col <= cc)
            def _():
                target[...] += lax.dot_general(
                    inv_ref[:, cc * piece:(cc + 1) * piece],
                    into[cc].astype(jnp.bfloat16),
                    NT,
                    preferred_element_type=jnp.float32,
                )

    def long_step(q):
        j = q * n_col + col

        @pl.when(j < long_count)
        def _():
            near = row - j <= near_of(j)

            @pl.when(near)
            def _():
                for s in range(n_col):
                    part = y_in.at[q, s, :, tail_of(s)]
                    remote(part, part, y_send.at[0], y_recv.at[q, s], (j, col)).wait_recv()
                y = y_in[q, 0]
                for s in range(1, n_col):
                    y = y + y_in[q, s]
                y_full[...] = y

            @pl.when(jnp.logical_not(near))
            def _():
                remote(y_in.at[q, 0], y_in.at[q, 0], y_send.at[0], y_recv.at[q, 0], (j, col)).wait_recv()
                y_full[...] = y_in[q, 0]

            y = y_full[...].astype(jnp.bfloat16)

            @pl.when(takes & (j == theirs))
            def _():
                wl_out[...] = lax.dot_general(y, d_tile[...], NT, preferred_element_type=jnp.float32)
                for s in range(n_col):
                    remote(wl_out, wl_in, wl_send, wl_recv, (row - 1, s)).start()

                @pl.when(is_end)
                def _():
                    for peer in peers:
                        remote(wl_out, wl_in, wp_send, wl_recv, (row, peer)).start()
                    wl_in[...] = wl_out[...]

            @pl.when(takes_whole & (j == whole))
            def _():
                inner = lax.dot_general(y, d_tile[...], NT, preferred_element_type=jnp.float32)
                p = jnp.dot(inner.astype(jnp.bfloat16), du_tile[...], preferred_element_type=jnp.float32)
                for s in range(n_col):
                    pd_out[s] = p[:, s * piece:(s + 1) * piece]
                    remote(pd_out.at[s], p_in.at[j], pd_send, p_recv.at[j], (row - 1, s)).start()

            inner = lax.dot_general(y, v_ref[q], NT, preferred_element_type=jnp.float32)
            keep = lax.broadcasted_iota(jnp.int32, (nrhs, rank_max), 1) < rank_ref[q]
            inner = jnp.where(keep, inner, 0.0).astype(jnp.bfloat16)
            p = jnp.dot(inner, u_ref[q], preferred_element_type=jnp.float32)
            for s in range(n_col):
                p_out[q, s] = p[:, s * piece:(s + 1) * piece]
            for peer in peers:
                remote(p_out.at[q, peer], p_in.at[j], p_send.at[q], p_recv.at[j], (row, peer)).start()
            p_in[j] = p_out[q, col]

    @pl.when(takes | takes_whole)
    def _():
        remote(d_in, d_in, d_send, d_recv, (row - 1, col)).wait_recv()
        d_tile[...] = d_in[...].astype(jnp.bfloat16)

    @pl.when(takes_whole)
    def _():
        remote(du_in, du_in, du_send, du_recv, (row - 1, col)).wait_recv()
        du_tile[...] = du_in[...].astype(jnp.bfloat16)

    @pl.when(is_end & (col != far_home))
    def _():
        relay(x_out, x_in, x_recv, row - 2, far_home)

    for q in range(per_col):
        long_step(q)

    @pl.when(is_even_end)
    def _():
        fold_with(v_in, v_recv, fold)
        factor = fold[...].astype(jnp.bfloat16)
        shared_wait(u_in, u_recv, prev_home)
        shared_wait(l_in, k_recv, mine_home)
        a_out[0] = jnp.dot(u_in[...].astype(jnp.bfloat16), factor, preferred_element_type=jnp.float32)
        a_out[1] = jnp.dot(l_in[...].astype(jnp.bfloat16), factor, preferred_element_type=jnp.float32)
        for k in range(2):
            for s in range(n_col):
                remote(a_out.at[k], a_in.at[k, col], a_send, a_recv, (row + 1, s)).start()

    @pl.when(feeds & jnp.logical_not(is_even_end))
    def _():
        fold_with(v_in, v_recv, fold)

    @pl.when(gives & crosses & jnp.logical_not(is_even_end))
    def _():
        share(u_out, u_in, u_recv)

    @pl.when(hands & jnp.logical_not(early_l))
    def _():
        share(l_out, l_in, k_recv)

    @pl.when(gives_far)
    def _():
        spread_late(x_out, x_in, x_recv, row - 2, far_home)
        share(t_out, t_in, t_recv)

    @pl.when(is_ahead)
    def _():
        fold_with(x_in, x_recv, fold_x)

    @pl.when(is_end)
    def _():
        remote(a_in, a_in, a_send, a_recv, (row - 1, 0)).wait_recv()
        for k in range(2):
            total = a_in[k, 0]
            for s in range(1, n_col):
                total = total + a_in[k, s]
            a_sum[k] = total.astype(jnp.bfloat16)

    def gather_p(j, acc):
        home = lax.rem(j, n_col)

        @pl.when(home != col)
        def _():
            remote(p_in.at[j], p_in.at[j], p_send.at[0], p_recv.at[j], (row, home)).wait_recv()

        return acc - p_in[j]

    base[...] = lax.fori_loop(0, long_count, gather_p, base[...])

    @pl.when(is_even_end)
    def _():
        remote(p_in.at[whole], p_in.at[whole], p_send.at[0], p_recv.at[whole], (row + 1, whole_home)).wait_recv()
        base[...] -= p_in[whole]

    def send_w(out, into, send, recv, i):
        for s in range(n_col):
            remote(out, into.at[col], send, recv, (i, s)).start()

    def wait_w(into, send, recv, i):
        remote(into, into, send, recv, (i, 0)).wait_recv()
        total = into[0]
        for s in range(1, n_col):
            total = total + into[s]
        return total

    @pl.when(is_even_end)
    def _():
        w_out[...] = jnp.dot(base[...].astype(jnp.bfloat16), fold[...].astype(jnp.bfloat16), preferred_element_type=jnp.float32)
        send_w(w_out, w_in, w_send, w_recv, row + 1)

    @pl.when(handed)
    def _():
        @pl.when(jnp.logical_not(is_even_end))
        def _():
            shared_wait(l_in, k_recv, mine_home)

        l_part = l_in[...].astype(jnp.bfloat16)
        remote(wl_in, wl_in, wl_send, wl_recv, (row + 1, mine_home)).wait_recv()
        base[...] -= jnp.dot(wl_in[...].astype(jnp.bfloat16), l_part, preferred_element_type=jnp.float32)

    @pl.when(short & jnp.logical_not(is_end))
    def _():
        @pl.when(jnp.logical_not(is_even_end))
        def _():
            shared_wait(u_in, u_recv, prev_home)

        u_part = u_in[...].astype(jnp.bfloat16)
        inner = wait_w(w_in, w_send, w_recv, row - 1)
        base[...] -= jnp.dot(inner.astype(jnp.bfloat16), u_part, preferred_element_type=jnp.float32)

    @pl.when(is_end)
    def _():
        shared_wait(u_in, u_recv, prev_home)
        shared_wait(t_in, t_recv, far_home)
        u_part = u_in[...].astype(jnp.bfloat16)
        t_part = t_in[...].astype(jnp.bfloat16)

        @pl.when(jnp.logical_not(takes))
        def _():
            remote(wl_in, wl_in, wp_send, wl_recv, (row, their_home)).wait_recv()

        inner = wait_w(w_in, w_send, w_recv, row - 1)
        inner -= jnp.dot(wl_in[...].astype(jnp.bfloat16), a_sum[1], preferred_element_type=jnp.float32)
        late = wait_w(wx_in, wx_send, wx_recv, row - 2)
        base[...] -= jnp.dot(late.astype(jnp.bfloat16), t_part, preferred_element_type=jnp.float32)
        late = wait_w(we_in, we_send, we_recv, row - 2)
        inner -= jnp.dot(late.astype(jnp.bfloat16), a_sum[0], preferred_element_type=jnp.float32)
        base[...] -= jnp.dot(inner.astype(jnp.bfloat16), u_part, preferred_element_type=jnp.float32)

    reduced = base[...].astype(jnp.bfloat16)

    @pl.when((jnp.logical_not(even)) & (answers > 0))
    def _():
        pl.semaphore_wait(ready, answers)

    @pl.when(feeds & jnp.logical_not(is_even_end))
    def _():
        w_out[...] = jnp.dot(reduced, fold[...].astype(jnp.bfloat16), preferred_element_type=jnp.float32)

        @pl.when(is_ahead)
        def _():
            send_w(w_out, we_in, we_send, we_recv, row + 2)
            wx_out[...] = jnp.dot(reduced, fold_x[...].astype(jnp.bfloat16), preferred_element_type=jnp.float32)
            send_w(wx_out, wx_in, wx_send, wx_recv, row + 2)

        send_w(w_out, w_in, w_send, w_recv, row + 1)

    def own_part(c):
        tail = tail_of(c)
        y_row[c, :, tail] = jnp.dot(reduced, inv_ref[:, tail], preferred_element_type=jnp.float32)

    by_col(own_part)

    def near_copy(i, c):
        tail = tail_of(c)
        return remote(
            y_row.at[c, :, tail], y_in.at[own_slot, c, :, tail], y_send.at[i], y_recv.at[own_slot, c], (i, own_home)
        )

    def send_y(i, carry):
        @pl.when(row < longs_of(i))
        def _():
            by_col(lambda c: near_copy(i, c).start())

        return carry

    def own_copy(c, peer):
        part = y_row.at[c, :, tail_of(c)]
        return remote(part, part, o_send, o_recv.at[c], (row, peer))

    first = row == 0
    lax.fori_loop(row + 1, jnp.where(first, 2, near_end), send_y, 0)
    for peer in peers:
        by_col(lambda c: own_copy(c, peer).start())

    @pl.when(first)
    def _():
        log_part()
        pl.semaphore_wait(ready, answers)
        lax.fori_loop(2, near_end, send_y, 0)

    remote(logs.at[others], logs.at[others], l_send, l_recv, (row, peers[0])).wait()
    log_sum = logs[0]
    for s in range(1, n_col):
        log_sum = log_sum + logs[s]
    log_term = log_sum * (1.0 / width) - 0.5 * math.log(2.0 * math.pi)

    def left_y(i, carry):
        @pl.when(row < longs_of(i))
        def _():
            by_col(lambda c: near_copy(i, c).wait_send())

        return carry

    lax.fori_loop(row + 1, near_end, left_y, 0)

    @pl.when(feeds)
    def _():
        remote(w_in, w_in, w_send, w_recv, (row + 1, 0)).wait_send()

    @pl.when(is_ahead)
    def _():
        remote(w_in, w_in, we_send, we_recv, (row + 2, 0)).wait_send()
        remote(w_in, w_in, wx_send, wx_recv, (row + 2, 0)).wait_send()

    @pl.when(is_even_end)
    def _():
        remote(a_in, a_in, a_send, a_recv, (row + 1, 0)).wait_send()

    @pl.when(takes)
    def _():
        remote(w_in, w_in, wl_send, wl_recv, (row - 1, 0)).wait_send()

        @pl.when(is_end)
        def _():
            remote(w_in.at[others], w_in.at[others], wp_send, wl_recv, (row, peers[0])).wait_send()

    @pl.when(hands)
    def _():
        remote(d_out, d_in, d_send, d_recv, (row + 1, col)).wait_send()
        share_done(l_out)

    @pl.when(hands_whole)
    def _():
        remote(d_out, d_in, d_send, d_recv, (row + 1, col)).wait_send()
        remote(du_out, du_in, du_send, du_recv, (row + 1, col)).wait_send()

    @pl.when(takes_whole)
    def _():
        remote(pd_out, pd_out, pd_send, p_recv.at[0], (row - 1, 0)).wait_send()

    @pl.when(gives & even)
    def _():
        spread_done(v_out, prev_home, crosses)

    @pl.when(gives)
    def _():
        share_done(u_out)

    @pl.when(gives_far)
    def _():
        spread_done(x_out, far_home, jnp.bool_(True))
        share_done(t_out)

    @pl.when(crosses & (col != prev_home))
    def _():
        relay_done(v_out, prev_home)

    @pl.when(is_end & (col != far_home))
    def _():
        relay_done(x_out, far_home)

    for q in range(per_col):

        @pl.when(q * n_col + col < long_count)
        def _():
            part = p_out.at[q, others]
            remote(part, part, p_send.at[q], p_recv.at[0], (row, peers[0])).wait_send()

    for s in range(n_col):

        @pl.when(col != s)
        def _():
            own_copy(s, peers[0]).wait_recv()

    y = y_row[0]
    for s in range(1, n_col):
        y = y + y_row[s]
    y_all[...] = y

    def far_copy(i):
        return remote(y_all, y_in.at[own_slot, 0], y_send.at[i], y_recv.at[own_slot, 0], (i, col))

    def send_far(i, carry):
        far_copy(i).start()
        return carry

    lax.fori_loop(jnp.where(relays, near_end, n_row), n_row, send_far, 0)
    white_ref[0, 0] = y
    quadratic = jnp.sum(y * y, axis=1, keepdims=True) * (1.0 / width)
    lik = -0.5 * quadratic + log_term
    r_id = lax.broadcasted_iota(jnp.int32, (nrhs, 128), 0)
    c_id = lax.broadcasted_iota(jnp.int32, (nrhs, 128), 1)
    flat = jnp.sum(jnp.where(r_id == c_id, lik, 0.0), axis=0, keepdims=True)
    lik_ref[0] = flat[:, :nrhs]

    def left_far(i, carry):
        far_copy(i).wait_send()
        return carry

    lax.fori_loop(jnp.where(relays, near_end, n_row), n_row, left_far, 0)

    def own_left(c):
        part = y_row.at[others, :, tail_of(c)]
        remote(part, part, o_send, o_recv.at[c], (row, peers[0])).wait_send()

    by_col(own_left)


def local(n_row, n_col, right_side, inverse_t, u_factor, v_factor, ranks):
    nrhs, width = right_side.shape[2:]
    per_col, _, rank_max = u_factor.shape[2:5]
    piece = width // n_col
    vmem = pl.BlockSpec(memory_space=pltpu.VMEM)
    hbm = pl.BlockSpec(memory_space=pl.ANY)
    dma = pltpu.SemaphoreType.DMA

    def f32(*shape):
        return pltpu.VMEM(shape, jnp.float32)

    def bf16(*shape):
        return pltpu.VMEM(shape, jnp.bfloat16)

    tile_set = [
        f32(n_col, rank_max, piece),
        f32(n_col, rank_max, piece),
        f32(n_col, rank_max, piece),
        f32(rank_max, piece),
        f32(piece, rank_max),
        f32(nrhs, rank_max),
        f32(n_col, nrhs, rank_max),
    ]
    return pl.pallas_call(
        functools.partial(kernel, n_row, n_col),
        out_shape=(
            pltpu.VMEM((1, 1, nrhs, width), jnp.float32),
            pltpu.VMEM((1, 1, nrhs), jnp.float32),
        ),
        in_specs=[hbm, hbm, hbm, hbm, hbm],
        out_specs=(vmem, vmem),
        scratch_shapes=[
            f32(nrhs, width),
            bf16(piece, width),
            bf16(per_col, rank_max, width),
            bf16(per_col, rank_max, width),
            pltpu.SMEM((per_col,), jnp.int32),
            f32(per_col, n_col, nrhs, width),
            f32(per_col, n_col, nrhs, piece),
            f32(n_row, nrhs, piece),
            f32(n_col, nrhs, width),
            f32(n_col, 1, 128),
            f32(nrhs, piece),
            f32(nrhs, width),
            f32(nrhs, width),
            *tile_set,
            *tile_set,
            f32(rank_max, width),
            f32(rank_max, width),
            bf16(rank_max, width),
            f32(rank_max, width),
            f32(rank_max, width),
            bf16(rank_max, width),
            f32(n_col, nrhs, piece),
            f32(n_col, rank_max, piece),
            f32(rank_max, piece),
            f32(nrhs, rank_max),
            f32(nrhs, rank_max),
            f32(n_col, nrhs, rank_max),
            f32(2, rank_max, rank_max),
            f32(2, n_col, rank_max, rank_max),
            bf16(2, rank_max, rank_max),
            dma((5,)),
            dma((n_row,)),
            dma((per_col, n_col)),
            dma((per_col,)),
            dma((n_row,)),
            dma, dma((n_col,)), dma, dma,
            dma((n_col,)),
            dma, dma, dma, dma, dma,
            dma((n_col,)),
            dma, dma,
            pltpu.SemaphoreType.REGULAR,
            dma, dma, dma, dma, dma, dma, dma, dma,
            dma, dma, dma,
            dma, dma, dma, dma, dma, dma,
        ],
        compiler_params=pltpu.CompilerParams(collective_id=0, has_side_effects=True),
        name="forward_solve",
    )(right_side, inverse_t, u_factor, v_factor, ranks.reshape(per_col))


def solution(mesh):
    placed = (
        P(None, "row", None, None),
        P(None, "row", "col", None),
        P(None, "row", None, "col", None, None),
        P(None, "row", None, "col", None, None),
        P(None, "row", None, "col"),
    )
    return jax.shard_map(
        functools.partial(local, mesh.shape["row"], mesh.shape["col"]),
        mesh=mesh,
        in_specs=placed,
        out_specs=(P(None, "row", None, None), P(None, "row", None)),
        check_vma=False,
    )
```

```python
import functools
import math

import jax
import jax.numpy as jnp
from jax import lax
from jax.experimental import pallas as pl
from jax.experimental.pallas import tpu as pltpu
from jax.sharding import PartitionSpec as P

MESH = pl.DeviceIdType.MESH
NT = (((1,), (1,)), ((), ()))
FIRST_SHORT = 3
NEAR = 3


def remote(src, dst, send_sem, recv_sem, device):
    return pltpu.make_async_remote_copy(
        src_ref=src,
        dst_ref=dst,
        send_sem=send_sem,
        recv_sem=recv_sem,
        device_id=device,
        device_id_type=MESH,
    )


def kernel(
    n_row, n_col,
    rhs_hbm, inv_hbm, u_hbm, v_hbm, rank_hbm,
    white_ref, lik_ref,
    rhs_ref, inv_ref, u_ref, v_ref, rank_ref,
    y_in, p_out, p_in, y_row, logs, base, y_full, y_all,
    v_out, v_in, u_out, u_in, fold, w_out, w_in,
    x_out, x_in, t_out, t_in, fold_x, wx_out, wx_in,
    d_out, d_in, d_tile, du_out, du_in, du_tile, pd_out, l_out, l_in, wl_out, wl_in, we_in,
    a_out, a_in, a_sum,
    hl_in, hu_in, hf_in, hv_out, hv_in, hv_tile, hb_out, hb_in, hz_out, hz_in, hw_out, hw_in, hy_out,
    in_sem, y_send, y_recv, p_send, p_recv, o_send, o_recv, l_send, l_recv,
    v_send, v_recv, u_send, u_recv, w_send, w_recv, m_recv, f_send, e_send, ready,
    x_recv, t_recv, k_recv, d_send, d_recv, du_send, du_recv, pd_send, wl_send, wl_recv, wp_send,
    we_send, we_recv, wx_send, wx_recv, a_send, a_recv,
):
    row = lax.axis_index("row")
    col = lax.axis_index("col")
    per_col, rank_max, width = u_ref.shape
    nrhs = rhs_ref.shape[0]
    piece = width // n_col
    half = n_col // 2
    some = max(n_col // 4, 1)
    peers = [lax.rem(col + k, n_col) for k in range(1, n_col)]
    others = pl.ds(0, n_col - 1)
    own_slot = row // n_col
    own_home = lax.rem(row, n_col)
    end = n_row - 1
    even_end = n_row - 2
    ahead = n_row - 3

    def longs_of(i):
        count = jnp.where(i >= FIRST_SHORT, i - 1, i)
        handed = (lax.rem(i, 2) == 0) & (i >= 2)
        return count - jnp.where(handed, 1, 0) - jnp.where(i >= even_end, 1, 0)

    def near_of(i):
        return NEAR + jnp.where(i >= 2, 1, 0)

    copies = [
        pltpu.make_async_copy(v_hbm.at[0, 0, :, 0], v_ref, in_sem.at[0]),
        pltpu.make_async_copy(u_hbm.at[0, 0, :, 0], u_ref, in_sem.at[1]),
        None,
        pltpu.make_async_copy(rhs_hbm.at[0, 0], rhs_ref, in_sem.at[3]),
        pltpu.make_async_copy(rank_hbm, rank_ref, in_sem.at[4]),
    ]
    @pl.when(lax.axis_index("row") > 0)
    def _():
        copies[0].start()
        copies[1].start()

    def tail_of(c):
        start = c * piece // 128 * 128
        return pl.ds(start, width - start)

    def inverse_copy(c):
        return pltpu.make_async_copy(inv_hbm.at[0, 0, :, tail_of(c)], inv_ref.at[:, tail_of(c)], in_sem.at[2])

    def by_col(act):
        for c in range(n_col):
            pl.when(col == c)(functools.partial(act, c))

    by_col(lambda c: inverse_copy(c).start())
    for copy in copies[3:]:
        copy.start()

    for s in range(1, n_col):
        start = s * piece // 128 * 128
        if start:
            y_row[s, :, :start] = jnp.zeros((nrhs, start), jnp.float32)
            for q in range(per_col):
                y_in[q, s, :, :start] = jnp.zeros((nrhs, start), jnp.float32)

    even = lax.rem(row, 2) == 0
    short = row >= FIRST_SHORT
    feeds = (row + 1 >= FIRST_SHORT) & (row < end)
    is_end = row == end
    is_even_end = row == even_end
    is_ahead = row == ahead
    lent = row == ahead - 1
    before = row == ahead - 2
    long_count = longs_of(row)
    near_end = jnp.minimum(row + near_of(row) + 1, n_row)
    relays = col == own_home

    barrier = pltpu.get_barrier_semaphore()

    def signal(sem, i, s):
        pl.semaphore_signal(sem, inc=1, device_id=(i, s), device_id_type=MESH)

    def row_of(i, cond, act):
        @pl.when(cond)
        def _():
            for s in range(n_col):
                act(i, s)

        return jnp.where(cond, n_col, 0)

    def above(act):
        yield row + 1, row_of(row + 1, row < end, act)
        for d in range(2, NEAR + 2):
            wide = (is_ahead | before) if d == 2 else jnp.bool_(False)
            one = (row + d < n_row) & (d <= near_of(row)) & jnp.logical_not(wide)

            @pl.when(one)
            def _():
                act(row + d, own_home)

            yield row + d, jnp.where(one, 1, 0)
            if d == 2:
                yield row + d, row_of(row + d, wide, act)

    def below(act):
        row_of(row - 1, row > 0, act)
        count = jnp.where(row > 0, n_col, 0)
        for d in range(2, NEAR + 2):
            fed = (row >= d) & (d <= near_of(row - d)) & (lax.rem(jnp.maximum(row - d, 0), n_col) == col)
            if d == 2:
                fed = fed | is_end | is_ahead
            count += row_of(row - d, fed, act)
        for q in range(per_col):
            j = q * n_col + col
            far = j < row - near_of(j)

            @pl.when(far)
            def _():
                act(j, col)

            count += jnp.where(far, 1, 0)
        return count

    def at_once(low, high):
        return (low == 0) & (high == 1)

    for peer in peers:
        signal(barrier, row, peer)
    greeted = jnp.int32(n_col - 1)
    answers = jnp.int32(0)
    for i, count in above(lambda i, s: signal(barrier, i, s)):
        quick = at_once(row, i)
        greeted += jnp.where(quick, count, 0)
        answers += jnp.where(quick, 0, count)

    def greet_far(i, count):
        signal(barrier, i, col)
        return count + 1

    answers = lax.fori_loop(jnp.where(relays, near_end, n_row), n_row, greet_far, answers)

    def greet_quick(i, s):
        @pl.when(at_once(i, row))
        def _():
            signal(barrier, i, s)

    def answer(i, s):
        @pl.when(jnp.logical_not(at_once(i, row)))
        def _():
            signal(ready, i, s)

    greeted += below(greet_quick)

    prev = jnp.maximum(row - 1, 0)
    prev_slot = prev // n_col
    prev_home = lax.rem(prev, n_col)
    gives = short & (col == prev_home)
    crosses = short & even
    far_slot = ahead // n_col
    far_home = ahead % n_col
    gives_far = is_end & (col == far_home)
    handed = even & (row >= 2)
    mine = jnp.where(handed, long_count + jnp.where(is_even_end, 1, 0), 0)
    mine_slot = mine // n_col
    mine_home = lax.rem(mine, n_col)
    hands = handed & (col == mine_home)
    taken = (row >= 3) & jnp.logical_not(even)
    theirs = jnp.where(taken, longs_of(prev) + jnp.where(is_end, 1, 0), 0)
    their_home = lax.rem(theirs, n_col)
    takes = taken & (col == their_home)
    whole = even_end - 3
    whole_slot = whole // n_col
    whole_home = whole % n_col
    hands_whole = is_even_end & (col == whole_home)
    takes_whole = is_end & (col == whole_home)

    def masked_u(slot):
        keep = lax.broadcasted_iota(jnp.int32, (rank_max, width), 0) < rank_ref[slot]
        return jnp.where(keep, u_ref[slot].astype(jnp.float32), 0.0)

    def cut(tile, into):
        for s in range(n_col):
            into[s] = tile[:, s * piece:(s + 1) * piece]

    @pl.when(row > 0)
    def _():
        copies[0].wait()
        copies[1].wait()

    copies[4].wait()

    @pl.when(hands)
    def _():
        d_out[...] = v_ref[mine_slot].astype(jnp.float32)
        cut(masked_u(mine_slot), l_out)

    @pl.when(hands_whole)
    def _():
        d_out[...] = v_ref[whole_slot].astype(jnp.float32)
        du_out[...] = masked_u(whole_slot)

    @pl.when(gives)
    def _():
        cut(v_ref[prev_slot].astype(jnp.float32), v_out)
        cut(masked_u(prev_slot), u_out)

    @pl.when(gives_far)
    def _():
        cut(v_ref[far_slot].astype(jnp.float32), x_out)
        cut(masked_u(far_slot), t_out)

    pl.semaphore_wait(barrier, greeted)
    below(answer)

    def by_way(home, s, cc):
        across = n_col - 1 - home
        return (home != s) & jnp.where(across < home, (across != s) | (cc < s + some), (s > home) | (cc < s + half))

    def is_late(home, s, cc):
        across = n_col - 1 - home
        return (across == s) & (across < home) & (cc >= s + some)

    def split_row(home):
        return n_col - 1 - home < home

    def is_split(home, s):
        across = n_col - 1 - home
        return (across == s) & (across < home)

    def joined(home, s):
        across = n_col - 1 - home
        return (across > home) & (across == s)

    def spread(out, into, recv, target, home, cross):
        for s in range(n_col):
            if s > 0:

                @pl.when(cross & joined(home, s - 1))
                def _():
                    remote(out.at[s - 1], out.at[s - 1], v_send.at[s], m_recv.at[s - 1], (row, s)).start()

            for cc in range(s, n_col):
                gone = cross & (joined(home, s) | is_split(home, s))
                way = cross & by_way(home, s, cc)
                later = cross & is_late(home, s, cc)

                @pl.when(way & jnp.logical_not(gone))
                def _():
                    remote(out.at[cc], out.at[cc], v_send.at[s], m_recv.at[cc], (row, s)).start()

                @pl.when(jnp.logical_not(way | later | gone))
                def _():
                    remote(out.at[cc], into.at[cc], v_send.at[s], recv, (target, s)).start()

        for s in range(n_col):
            for cc in range(s, min(s + some, n_col)):

                @pl.when(cross & is_split(home, s))
                def _():
                    remote(out.at[cc], out.at[cc], v_send.at[s], m_recv.at[cc], (row, s)).start()

    def spread_late(out, into, recv, target, home):
        for s in range(n_col - 1):

            @pl.when(split_row(home) & (home == s + 1))
            def _():
                part = pl.ds(s, n_col - s)
                remote(out.at[part], out.at[part], v_send.at[s], m_recv.at[0], (row, s)).wait_send()

        for s in range(n_col):
            for cc in range(min(s + some, n_col), n_col):

                @pl.when(is_late(home, s, cc))
                def _():
                    remote(out.at[cc], into.at[cc], v_send.at[s], recv, (target, s)).start()

    def spread_done(out, home, cross):
        for s in range(n_col):
            part = pl.ds(s, n_col - s)
            gone = cross & joined(home, s)
            gone = gone | (cross & split_row(home) & (home == s + 1))
            more = (cross & joined(home, s - 1)) if s > 0 else jnp.bool_(False)

            @pl.when(jnp.logical_not(gone | more))
            def _():
                remote(out.at[part], out.at[part], v_send.at[s], m_recv.at[0], (row, s)).wait_send()

            if s > 0:
                part_more = pl.ds(s - 1, n_col - s + 1)

                @pl.when(more)
                def _():
                    remote(out.at[part_more], out.at[part_more], v_send.at[s], m_recv.at[0], (row, s)).wait_send()

    def relay(out, into, recv, target, home):
        across = n_col - 1 - home
        more = joined(home, col - 1)
        first = jnp.where(more, col - 1, col)
        part = jnp.where(across < home, across == col, col < home)
        share_of = jnp.where(across < home, some, half)
        stop = jnp.where(part, jnp.minimum(col + share_of, n_col), n_col)

        def forward(cc, carry):
            remote(out.at[cc], out.at[cc], v_send.at[0], m_recv.at[cc], (row, home)).wait_recv()

            @pl.when(cc >= col)
            def _():
                remote(out.at[cc], into.at[cc], f_send, recv, (target, col)).start()

            @pl.when(more)
            def _():
                remote(out.at[cc], out.at[cc], e_send, m_recv.at[cc], (row, across)).start()

            return carry

        lax.fori_loop(first, stop, forward, 0)

    def relay_done(out, home):
        across = n_col - 1 - home
        for cc in range(n_col):
            here = col == cc
            half_way = jnp.where(across < home, across == cc, cc < home)

            @pl.when(here & jnp.logical_not(half_way))
            def _():
                part = pl.ds(cc, n_col - cc)
                remote(out.at[part], out.at[part], f_send, v_recv, (row, home)).wait_send()

            for count, cond in ((some, across < home), (half, across > home)):
                few = pl.ds(cc, min(count, n_col - cc))

                @pl.when(here & half_way & cond)
                def _():
                    remote(out.at[few], out.at[few], f_send, v_recv, (row, home)).wait_send()

            if cc > 0:

                @pl.when((col == cc) & joined(home, cc - 1))
                def _():
                    part = pl.ds(cc - 1, n_col - cc + 1)
                    remote(out.at[part], out.at[part], e_send, v_recv, (row, home)).wait_send()

    def share(out, into, recv):
        for peer in peers:
            remote(out.at[peer], into, u_send, recv, (row, peer)).start()
        into[...] = out[col]

    def share_done(out):
        remote(out.at[others], out.at[others], u_send, u_recv, (row, peers[0])).wait_send()

    def shared_wait(into, recv, home):
        @pl.when(col != home)
        def _():
            remote(into, into, u_send, recv, (row, home)).wait_recv()

    early_l = (row < FIRST_SHORT) | is_even_end

    @pl.when(hands & early_l)
    def _():
        share(l_out, l_in, k_recv)

    @pl.when(gives)
    def _():
        spread(v_out, v_in, v_recv, row - 1, prev_home, crosses)

    @pl.when(gives & (is_even_end | jnp.logical_not(even)))
    def _():
        share(u_out, u_in, u_recv)

    @pl.when(gives_far)
    def _():
        spread(x_out, x_in, x_recv, row - 2, far_home, jnp.bool_(True))

    @pl.when((handed) & (answers > 0))
    def _():
        pl.semaphore_wait(ready, answers)

    @pl.when(hands | hands_whole)
    def _():
        remote(d_out, d_in, d_send, d_recv, (row + 1, col)).start()

    @pl.when(hands_whole)
    def _():
        remote(du_out, du_in, du_send, du_recv, (row + 1, col)).start()

    @pl.when(crosses & (col != prev_home))
    def _():
        relay(v_out, v_in, v_recv, row - 1, prev_home)

    by_col(lambda c: inverse_copy(c).wait())
    copies[3].wait()

    def lend(src, dst, send, recv):
        return remote(src, dst, send, recv, (row + 1, col))

    def lend_inverse(c):
        return lend(hv_out.at[:, tail_of(c)], hv_in.at[:, tail_of(c)], wl_send, wx_recv)

    def lend_tail(c):
        hv_out[:, tail_of(c)] = inv_ref[:, tail_of(c)].astype(jnp.float32)
        lend_inverse(c).start()

    pl.when(lent)(functools.partial(by_col, lend_tail))

    for cc in range(n_col):

        @pl.when(col == cc)
        def _():
            base[...] = rhs_ref[:, cc * piece:(cc + 1) * piece]

    def log_part():
        for cc in range(n_col):

            @pl.when(col == cc)
            def _():
                block = inv_ref[:, cc * piece:(cc + 1) * piece].astype(jnp.float32)
                r_id = lax.broadcasted_iota(jnp.int32, (piece, piece), 0)
                c_id = lax.broadcasted_iota(jnp.int32, (piece, piece), 1)
                diagonal = jnp.sum(jnp.where(r_id == c_id, block, 0.0), axis=0, keepdims=True)
                total = jnp.sum(jnp.log(diagonal), axis=1, keepdims=True)
                logs[cc] = jnp.broadcast_to(total, (1, 128))

        for peer in peers:
            remote(logs.at[col], logs.at[col], l_send, l_recv, (row, peer)).start()

    pl.when(row > 0)(log_part)

    @pl.when(gives & crosses)
    def _():
        spread_late(v_out, v_in, v_recv, row - 1, prev_home)

    def fold_with(into, recv, target):
        target[...] = jnp.zeros_like(target)
        for cc in range(n_col):
            part = pl.ds(cc, n_col - cc)

            @pl.when(col == cc)
            def _():
                remote(into.at[part], into.at[part], f_send, recv, (row, cc)).wait_recv()

        for cc in range(n_col):

            @pl.when(col <= cc)
            def _():
                target[...] += lax.dot_general(
                    inv_ref[:, cc * piece:(cc + 1) * piece],
                    into[cc].astype(jnp.bfloat16),
                    NT,
                    preferred_element_type=jnp.float32,
                )

    def long_step(q, cond):
        j = q * n_col + col

        @pl.when((j < long_count) & cond)
        def _():
            near = row - j <= near_of(j)

            @pl.when(near)
            def _():
                for s in range(n_col):
                    part = y_in.at[q, s, :, tail_of(s)]
                    remote(part, part, y_send.at[0], y_recv.at[q, s], (j, col)).wait_recv()
                y = y_in[q, 0]
                for s in range(1, n_col):
                    y = y + y_in[q, s]
                y_full[...] = y

            @pl.when(jnp.logical_not(near))
            def _():
                remote(y_in.at[q, 0], y_in.at[q, 0], y_send.at[0], y_recv.at[q, 0], (j, col)).wait_recv()
                y_full[...] = y_in[q, 0]

            y = y_full[...].astype(jnp.bfloat16)

            @pl.when(takes & (j == theirs))
            def _():
                wl_out[...] = lax.dot_general(y, d_tile[...], NT, preferred_element_type=jnp.float32)
                @pl.when(jnp.logical_not(is_ahead))
                def _():
                    for s in range(n_col):
                        remote(wl_out, wl_in, wl_send, wl_recv, (row - 1, s)).start()

                @pl.when(is_end | is_ahead)
                def _():
                    for peer in peers:
                        remote(wl_out, wl_in, wp_send, wl_recv, (row, peer)).start()
                    wl_in[...] = wl_out[...]

            @pl.when(takes_whole & (j == whole))
            def _():
                inner = lax.dot_general(y, d_tile[...], NT, preferred_element_type=jnp.float32)
                p = jnp.dot(inner.astype(jnp.bfloat16), du_tile[...], preferred_element_type=jnp.float32)
                for s in range(n_col):
                    pd_out[s] = p[:, s * piece:(s + 1) * piece]
                    remote(pd_out.at[s], p_in.at[j], pd_send, p_recv.at[j], (row - 1, s)).start()

            inner = lax.dot_general(y, v_ref[q], NT, preferred_element_type=jnp.float32)
            keep = lax.broadcasted_iota(jnp.int32, (nrhs, rank_max), 1) < rank_ref[q]
            inner = jnp.where(keep, inner, 0.0).astype(jnp.bfloat16)
            p = jnp.dot(inner, u_ref[q], preferred_element_type=jnp.float32)
            for s in range(n_col):
                p_out[q, s] = p[:, s * piece:(s + 1) * piece]
            for peer in peers:
                remote(p_out.at[q, peer], p_in.at[j], p_send.at[q], p_recv.at[j], (row, peer)).start()
            p_in[j] = p_out[q, col]

    @pl.when(takes | takes_whole)
    def _():
        remote(d_in, d_in, d_send, d_recv, (row - 1, col)).wait_recv()
        d_tile[...] = d_in[...].astype(jnp.bfloat16)

    @pl.when(takes_whole)
    def _():
        remote(du_in, du_in, du_send, du_recv, (row - 1, col)).wait_recv()
        du_tile[...] = du_in[...].astype(jnp.bfloat16)

    @pl.when(is_end & (col != far_home))
    def _():
        relay(x_out, x_in, x_recv, row - 2, far_home)

    for q in range(per_col):
        long_step(q, jnp.logical_not(is_ahead & (q * n_col + col == row - 2)))

    def send_w(out, into, send, recv, i):
        for s in range(n_col):
            remote(out, into.at[col], send, recv, (i, s)).start()

    def wait_w(into, send, recv, i):
        remote(into, into, send, recv, (i, 0)).wait_recv()
        total = into[0]
        for s in range(1, n_col):
            total = total + into[s]
        return total

    def borrowed_y(c):
        tail = tail_of(c)
        slot = (ahead - 1) // n_col
        home = (ahead - 1) % n_col
        return remote(hy_out.at[:, tail], y_in.at[slot, c, :, tail], y_send.at[end], y_recv.at[slot, c], (end, home))

    @pl.when(is_ahead)
    def _():
        back = (row - 1, col)
        by_col(lambda c: remote(hv_in.at[:, tail_of(c)], hv_in.at[:, tail_of(c)], wl_send, wx_recv, back).wait_recv())
        by_col(lambda c: hv_tile.__setitem__((slice(None), tail_of(c)), hv_in[:, tail_of(c)].astype(jnp.bfloat16)))
        remote(hl_in, hl_in, a_send, k_recv, back).wait_recv()
        remote(hu_in, hu_in, we_send, a_recv, back).wait_recv()
        remote(hf_in, hf_in, wx_send, we_recv, back).wait_recv()
        remote(hb_in, hb_in, wp_send, t_recv, back).wait_recv()
        l_part = hl_in[...].astype(jnp.bfloat16)
        u_part = hu_in[...].astype(jnp.bfloat16)
        factor = hf_in[...].astype(jnp.bfloat16)

        @pl.when(answers > 0)
        def _():
            pl.semaphore_wait(ready, answers)

        @pl.when(jnp.logical_not(takes))
        def _():
            remote(wl_in, wl_in, wp_send, wl_recv, (row, their_home)).wait_recv()

        part = hb_in[...] - jnp.dot(wl_in[...].astype(jnp.bfloat16), l_part, preferred_element_type=jnp.float32)
        inner = wait_w(hw_in, w_send, du_recv, row - 2)
        part -= jnp.dot(inner.astype(jnp.bfloat16), u_part, preferred_element_type=jnp.float32)
        part = part.astype(jnp.bfloat16)
        hw_out[...] = jnp.dot(part, factor, preferred_element_type=jnp.float32)
        for peer in peers:
            remote(hw_out, w_in.at[col], a_send, w_recv, (row, peer)).start()
        w_in[col] = hw_out[...]

        def borrowed_part(c):
            tail = tail_of(c)
            hy_out[:, tail] = jnp.dot(part, hv_tile[:, tail], preferred_element_type=jnp.float32)
            borrowed_y(c).start()

        by_col(borrowed_part)
        hz_out[...] = part.astype(jnp.float32)
        remote(hz_out, hz_in, pd_send, du_recv, back).start()

    for q in range(per_col):
        long_step(q, is_ahead & (q * n_col + col == row - 2))

    @pl.when(is_even_end)
    def _():
        fold_with(v_in, v_recv, fold)
        factor = fold[...].astype(jnp.bfloat16)
        shared_wait(u_in, u_recv, prev_home)
        shared_wait(l_in, k_recv, mine_home)
        a_out[0] = jnp.dot(u_in[...].astype(jnp.bfloat16), factor, preferred_element_type=jnp.float32)
        a_out[1] = jnp.dot(l_in[...].astype(jnp.bfloat16), factor, preferred_element_type=jnp.float32)
        for k in range(2):
            for s in range(n_col):
                remote(a_out.at[k], a_in.at[k, col], a_send, a_recv, (row + 1, s)).start()

    @pl.when(feeds & jnp.logical_not(is_even_end))
    def _():
        fold_with(v_in, v_recv, fold)

        @pl.when(lent)
        def _():
            lend(fold, hf_in, wx_send, we_recv).start()

    @pl.when(gives & crosses & jnp.logical_not(is_even_end))
    def _():
        share(u_out, u_in, u_recv)

    @pl.when(hands & jnp.logical_not(early_l))
    def _():
        share(l_out, l_in, k_recv)

    @pl.when(gives_far)
    def _():
        spread_late(x_out, x_in, x_recv, row - 2, far_home)
        share(t_out, t_in, t_recv)

    @pl.when(is_ahead)
    def _():
        fold_with(x_in, x_recv, fold_x)

    @pl.when(is_end)
    def _():
        remote(a_in, a_in, a_send, a_recv, (row - 1, 0)).wait_recv()
        for k in range(2):
            total = a_in[k, 0]
            for s in range(1, n_col):
                total = total + a_in[k, s]
            a_sum[k] = total.astype(jnp.bfloat16)

    def gather_p(j, acc):
        home = lax.rem(j, n_col)

        @pl.when(home != col)
        def _():
            remote(p_in.at[j], p_in.at[j], p_send.at[0], p_recv.at[j], (row, home)).wait_recv()

        return acc - p_in[j]

    base[...] = lax.fori_loop(0, long_count, gather_p, base[...])

    @pl.when(lent)
    def _():
        hb_out[...] = base[...]
        lend(hb_out, hb_in, wp_send, t_recv).start()
        shared_wait(l_in, k_recv, mine_home)
        lend(l_in, hl_in, a_send, k_recv).start()
        shared_wait(u_in, u_recv, prev_home)
        lend(u_in, hu_in, we_send, a_recv).start()
        remote(hz_in, hz_in, pd_send, du_recv, (row + 1, col)).wait_recv()
        base[...] = hz_in[...]

    @pl.when(is_even_end)
    def _():
        remote(p_in.at[whole], p_in.at[whole], p_send.at[0], p_recv.at[whole], (row + 1, whole_home)).wait_recv()
        base[...] -= p_in[whole]

    @pl.when(is_even_end)
    def _():
        w_out[...] = jnp.dot(base[...].astype(jnp.bfloat16), fold[...].astype(jnp.bfloat16), preferred_element_type=jnp.float32)
        send_w(w_out, w_in, w_send, w_recv, row + 1)

    @pl.when(handed & jnp.logical_not(lent))
    def _():
        @pl.when(jnp.logical_not(is_even_end))
        def _():
            shared_wait(l_in, k_recv, mine_home)

        l_part = l_in[...].astype(jnp.bfloat16)
        remote(wl_in, wl_in, wl_send, wl_recv, (row + 1, mine_home)).wait_recv()
        base[...] -= jnp.dot(wl_in[...].astype(jnp.bfloat16), l_part, preferred_element_type=jnp.float32)

    @pl.when(is_ahead)
    def _():
        shared_wait(u_in, u_recv, prev_home)
        u_part = u_in[...].astype(jnp.bfloat16)
        part = w_in.at[others]
        remote(part, part, a_send, w_recv, (row, peers[0])).wait_recv()
        inner = w_in[0]
        for s in range(1, n_col):
            inner = inner + w_in[s]
        base[...] -= jnp.dot(inner.astype(jnp.bfloat16), u_part, preferred_element_type=jnp.float32)

    @pl.when(short & jnp.logical_not(is_end | is_ahead | lent))
    def _():
        @pl.when(jnp.logical_not(is_even_end))
        def _():
            shared_wait(u_in, u_recv, prev_home)

        u_part = u_in[...].astype(jnp.bfloat16)
        inner = wait_w(w_in, w_send, w_recv, row - 1)
        base[...] -= jnp.dot(inner.astype(jnp.bfloat16), u_part, preferred_element_type=jnp.float32)

    @pl.when(is_end)
    def _():
        shared_wait(u_in, u_recv, prev_home)
        shared_wait(t_in, t_recv, far_home)
        u_part = u_in[...].astype(jnp.bfloat16)
        t_part = t_in[...].astype(jnp.bfloat16)

        @pl.when(jnp.logical_not(takes))
        def _():
            remote(wl_in, wl_in, wp_send, wl_recv, (row, their_home)).wait_recv()

        inner = wait_w(w_in, w_send, w_recv, row - 1)
        inner -= jnp.dot(wl_in[...].astype(jnp.bfloat16), a_sum[1], preferred_element_type=jnp.float32)
        late = wait_w(wx_in, wx_send, wx_recv, row - 2)
        base[...] -= jnp.dot(late.astype(jnp.bfloat16), t_part, preferred_element_type=jnp.float32)
        late = wait_w(we_in, we_send, we_recv, row - 2)
        inner -= jnp.dot(late.astype(jnp.bfloat16), a_sum[0], preferred_element_type=jnp.float32)
        base[...] -= jnp.dot(inner.astype(jnp.bfloat16), u_part, preferred_element_type=jnp.float32)

    reduced = base[...].astype(jnp.bfloat16)

    @pl.when(jnp.logical_not(even | is_ahead) & (answers > 0))
    def _():
        pl.semaphore_wait(ready, answers)

    @pl.when(feeds & jnp.logical_not(is_even_end | lent))
    def _():
        w_out[...] = jnp.dot(reduced, fold[...].astype(jnp.bfloat16), preferred_element_type=jnp.float32)

        @pl.when(is_ahead)
        def _():
            send_w(w_out, we_in, we_send, we_recv, row + 2)
            wx_out[...] = jnp.dot(reduced, fold_x[...].astype(jnp.bfloat16), preferred_element_type=jnp.float32)
            send_w(wx_out, wx_in, wx_send, wx_recv, row + 2)

        @pl.when(before)
        def _():
            send_w(w_out, hw_in, w_send, du_recv, row + 2)

        @pl.when(jnp.logical_not(before))
        def _():
            send_w(w_out, w_in, w_send, w_recv, row + 1)

    def own_part(c):
        tail = tail_of(c)
        y_row[c, :, tail] = jnp.dot(reduced, inv_ref[:, tail], preferred_element_type=jnp.float32)

    by_col(own_part)

    def near_copy(i, c):
        tail = tail_of(c)
        return remote(
            y_row.at[c, :, tail], y_in.at[own_slot, c, :, tail], y_send.at[i], y_recv.at[own_slot, c], (i, own_home)
        )

    def send_y(i, carry):
        @pl.when((row < longs_of(i)) & jnp.logical_not(lent))
        def _():
            by_col(lambda c: near_copy(i, c).start())

        return carry

    def own_copy(c, peer):
        part = y_row.at[c, :, tail_of(c)]
        return remote(part, part, o_send, o_recv.at[c], (row, peer))

    first = row == 0
    lax.fori_loop(row + 1, jnp.where(first, 2, near_end), send_y, 0)
    for peer in peers:
        by_col(lambda c: own_copy(c, peer).start())

    @pl.when(first)
    def _():
        log_part()
        pl.semaphore_wait(ready, answers)
        lax.fori_loop(2, near_end, send_y, 0)

    remote(logs.at[others], logs.at[others], l_send, l_recv, (row, peers[0])).wait()
    log_sum = logs[0]
    for s in range(1, n_col):
        log_sum = log_sum + logs[s]
    log_term = log_sum * (1.0 / width) - 0.5 * math.log(2.0 * math.pi)

    def left_y(i, carry):
        @pl.when((row < longs_of(i)) & jnp.logical_not(lent))
        def _():
            by_col(lambda c: near_copy(i, c).wait_send())

        return carry

    lax.fori_loop(row + 1, near_end, left_y, 0)

    @pl.when(feeds & jnp.logical_not(lent))
    def _():
        remote(w_in, w_in, w_send, w_recv, (row + 1, 0)).wait_send()

    @pl.when(lent)
    def _():
        by_col(lambda c: lend_inverse(c).wait_send())
        lend(fold, hf_in, wx_send, we_recv).wait_send()
        lend(hb_out, hb_in, wp_send, t_recv).wait_send()
        lend(l_in, hl_in, a_send, k_recv).wait_send()
        lend(u_in, hu_in, we_send, a_recv).wait_send()

    @pl.when(is_ahead)
    def _():
        part = w_in.at[others]
        remote(part, part, a_send, w_recv, (row, peers[0])).wait_send()
        by_col(lambda c: borrowed_y(c).wait_send())
        remote(hz_out, hz_in, pd_send, du_recv, (row - 1, col)).wait_send()
        remote(w_in, w_in, we_send, we_recv, (row + 2, 0)).wait_send()
        remote(w_in, w_in, wx_send, wx_recv, (row + 2, 0)).wait_send()

    @pl.when(is_even_end)
    def _():
        remote(a_in, a_in, a_send, a_recv, (row + 1, 0)).wait_send()

    @pl.when(takes)
    def _():
        @pl.when(jnp.logical_not(is_ahead))
        def _():
            remote(w_in, w_in, wl_send, wl_recv, (row - 1, 0)).wait_send()

        @pl.when(is_end | is_ahead)
        def _():
            remote(w_in.at[others], w_in.at[others], wp_send, wl_recv, (row, peers[0])).wait_send()

    @pl.when(hands)
    def _():
        remote(d_out, d_in, d_send, d_recv, (row + 1, col)).wait_send()
        share_done(l_out)

    @pl.when(hands_whole)
    def _():
        remote(d_out, d_in, d_send, d_recv, (row + 1, col)).wait_send()
        remote(du_out, du_in, du_send, du_recv, (row + 1, col)).wait_send()

    @pl.when(takes_whole)
    def _():
        remote(pd_out, pd_out, pd_send, p_recv.at[0], (row - 1, 0)).wait_send()

    @pl.when(gives)
    def _():
        spread_done(v_out, prev_home, crosses)
        share_done(u_out)

    @pl.when(gives_far)
    def _():
        spread_done(x_out, far_home, jnp.bool_(True))
        share_done(t_out)

    @pl.when(crosses & (col != prev_home))
    def _():
        relay_done(v_out, prev_home)

    @pl.when(is_end & (col != far_home))
    def _():
        relay_done(x_out, far_home)

    for q in range(per_col):

        @pl.when(q * n_col + col < long_count)
        def _():
            part = p_out.at[q, others]
            remote(part, part, p_send.at[q], p_recv.at[0], (row, peers[0])).wait_send()

    for s in range(n_col):

        @pl.when(col != s)
        def _():
            own_copy(s, peers[0]).wait_recv()

    y = y_row[0]
    for s in range(1, n_col):
        y = y + y_row[s]
    y_all[...] = y

    def far_copy(i):
        return remote(y_all, y_in.at[own_slot, 0], y_send.at[i], y_recv.at[own_slot, 0], (i, col))

    def send_far(i, carry):
        far_copy(i).start()
        return carry

    lax.fori_loop(jnp.where(relays, near_end, n_row), n_row, send_far, 0)
    white_ref[0, 0] = y
    quadratic = jnp.sum(y * y, axis=1, keepdims=True) * (1.0 / width)
    lik = -0.5 * quadratic + log_term
    r_id = lax.broadcasted_iota(jnp.int32, (nrhs, 128), 0)
    c_id = lax.broadcasted_iota(jnp.int32, (nrhs, 128), 1)
    flat = jnp.sum(jnp.where(r_id == c_id, lik, 0.0), axis=0, keepdims=True)
    lik_ref[0] = flat[:, :nrhs]

    def left_far(i, carry):
        far_copy(i).wait_send()
        return carry

    lax.fori_loop(jnp.where(relays, near_end, n_row), n_row, left_far, 0)

    def own_left(c):
        part = y_row.at[others, :, tail_of(c)]
        remote(part, part, o_send, o_recv.at[c], (row, peers[0])).wait_send()

    by_col(own_left)


def local(n_row, n_col, right_side, inverse_t, u_factor, v_factor, ranks):
    nrhs, width = right_side.shape[2:]
    per_col, _, rank_max = u_factor.shape[2:5]
    piece = width // n_col
    vmem = pl.BlockSpec(memory_space=pltpu.VMEM)
    hbm = pl.BlockSpec(memory_space=pl.ANY)
    dma = pltpu.SemaphoreType.DMA

    def f32(*shape):
        return pltpu.VMEM(shape, jnp.float32)

    def bf16(*shape):
        return pltpu.VMEM(shape, jnp.bfloat16)

    tile_set = [
        f32(n_col, rank_max, piece),
        f32(n_col, rank_max, piece),
        f32(n_col, rank_max, piece),
        f32(rank_max, piece),
        f32(piece, rank_max),
        f32(nrhs, rank_max),
        f32(n_col, nrhs, rank_max),
    ]
    return pl.pallas_call(
        functools.partial(kernel, n_row, n_col),
        out_shape=(
            pltpu.VMEM((1, 1, nrhs, width), jnp.float32),
            pltpu.VMEM((1, 1, nrhs), jnp.float32),
        ),
        in_specs=[hbm, hbm, hbm, hbm, hbm],
        out_specs=(vmem, vmem),
        scratch_shapes=[
            f32(nrhs, width),
            bf16(piece, width),
            bf16(per_col, rank_max, width),
            bf16(per_col, rank_max, width),
            pltpu.SMEM((per_col,), jnp.int32),
            f32(per_col, n_col, nrhs, width),
            f32(per_col, n_col, nrhs, piece),
            f32(n_row, nrhs, piece),
            f32(n_col, nrhs, width),
            f32(n_col, 1, 128),
            f32(nrhs, piece),
            f32(nrhs, width),
            f32(nrhs, width),
            *tile_set,
            *tile_set,
            f32(rank_max, width),
            f32(rank_max, width),
            bf16(rank_max, width),
            f32(rank_max, width),
            f32(rank_max, width),
            bf16(rank_max, width),
            f32(n_col, nrhs, piece),
            f32(n_col, rank_max, piece),
            f32(rank_max, piece),
            f32(nrhs, rank_max),
            f32(nrhs, rank_max),
            f32(n_col, nrhs, rank_max),
            f32(2, rank_max, rank_max),
            f32(2, n_col, rank_max, rank_max),
            bf16(2, rank_max, rank_max),
            f32(rank_max, piece),
            f32(rank_max, piece),
            f32(piece, rank_max),
            f32(piece, width),
            f32(piece, width),
            bf16(piece, width),
            f32(nrhs, piece),
            f32(nrhs, piece),
            f32(nrhs, piece),
            f32(nrhs, piece),
            f32(nrhs, rank_max),
            f32(n_col, nrhs, rank_max),
            f32(nrhs, width),
            dma((5,)),
            dma((n_row,)),
            dma((per_col, n_col)),
            dma((per_col,)),
            dma((n_row,)),
            dma, dma((n_col,)), dma, dma,
            dma((n_col,)),
            dma, dma, dma, dma, dma,
            dma((n_col,)),
            dma, dma,
            pltpu.SemaphoreType.REGULAR,
            dma, dma, dma, dma, dma, dma, dma, dma,
            dma, dma, dma,
            dma, dma, dma, dma, dma, dma,
        ],
        compiler_params=pltpu.CompilerParams(collective_id=0, has_side_effects=True),
        name="forward_solve",
    )(right_side, inverse_t, u_factor, v_factor, ranks.reshape(per_col))


def solution(mesh):
    placed = (
        P(None, "row", None, None),
        P(None, "row", "col", None),
        P(None, "row", None, "col", None, None),
        P(None, "row", None, "col", None, None),
        P(None, "row", None, "col"),
    )
    return jax.shard_map(
        functools.partial(local, mesh.shape["row"], mesh.shape["col"]),
        mesh=mesh,
        in_specs=placed,
        out_specs=(P(None, "row", None, None), P(None, "row", None)),
        check_vma=False,
    )
```

```python
import functools
import math

import jax
import jax.numpy as jnp
from jax import lax
from jax.experimental import pallas as pl
from jax.experimental.pallas import tpu as pltpu
from jax.sharding import PartitionSpec as P

MESH = pl.DeviceIdType.MESH
NT = (((1,), (1,)), ((), ()))
FIRST_SHORT = 3
NEAR = 3


def remote(src, dst, send_sem, recv_sem, device):
    return pltpu.make_async_remote_copy(
        src_ref=src,
        dst_ref=dst,
        send_sem=send_sem,
        recv_sem=recv_sem,
        device_id=device,
        device_id_type=MESH,
    )


def kernel(
    n_row, n_col,
    rhs_hbm, inv_hbm, u_hbm, v_hbm, rank_hbm,
    white_ref, lik_ref,
    rhs_ref, inv_ref, u_ref, v_ref, rank_ref,
    y_in, p_out, p_in, y_row, logs, base, y_full, y_all,
    v_out, v_in, u_out, u_in, fold, w_out, w_in,
    x_out, x_in, t_out, t_in, fold_x, wx_out, wx_in,
    d_out, d_in, d_tile, vt_ref, l2_in, w2_out, w2_in, l_out, l_in, wl_out, wl_in, we_in,
    a_out, a_in, a_sum,
    hl_in, hu_in, hf_in, hv_out, hv_in, hv_tile, hb_out, hb_in, hz_out, hz_in, hw_out, hw_in, hy_out,
    in_sem, y_send, y_recv, p_send, p_recv, o_send, o_recv, l_send, l_recv,
    v_send, v_recv, u_send, u_recv, w_send, w_recv, m_recv, f_send, e_send, ready,
    x_recv, t_recv, k_recv, d_send, d_recv, du_send, du_recv, pd_send, wl_send, wl_recv, wp_send,
    we_send, we_recv, wx_send, wx_recv, a_send, a_recv,
):
    row = lax.axis_index("row")
    col = lax.axis_index("col")
    per_col, rank_max, width = u_ref.shape
    nrhs = rhs_ref.shape[0]
    piece = width // n_col
    half = n_col // 2
    y_sends = y_send.shape[0]
    some = max(n_col // 4, 1)
    peers = [lax.rem(col + k, n_col) for k in range(1, n_col)]
    others = pl.ds(0, n_col - 1)
    own_slot = row // n_col
    own_home = lax.rem(row, n_col)
    end = n_row - 1
    even_end = n_row - 2
    ahead = n_row - 3

    def longs_of(i):
        count = jnp.where(i >= FIRST_SHORT, i - 1, i)
        handed = (lax.rem(i, 2) == 0) & (i >= 2)
        return count - jnp.where(handed, 1, 0) - jnp.where(i >= even_end, 1, 0)

    def near_of(i):
        return NEAR + jnp.where(i >= 2, 1, 0)

    copies = [
        pltpu.make_async_copy(v_hbm.at[0, 0, :, 0], v_ref, in_sem.at[0]),
        pltpu.make_async_copy(u_hbm.at[0, 0, :, 0], u_ref, in_sem.at[1]),
        None,
        pltpu.make_async_copy(rhs_hbm.at[0, 0], rhs_ref, in_sem.at[3]),
        pltpu.make_async_copy(rank_hbm, rank_ref, in_sem.at[4]),
    ]
    @pl.when(lax.axis_index("row") > 0)
    def _():
        copies[0].start()
        copies[1].start()

    def tail_of(c):
        start = c * piece // 128 * 128
        return pl.ds(start, width - start)

    def inverse_copy(c):
        return pltpu.make_async_copy(inv_hbm.at[0, 0, :, tail_of(c)], inv_ref.at[:, tail_of(c)], in_sem.at[2])

    def by_col(act):
        for c in range(n_col):
            pl.when(col == c)(functools.partial(act, c))

    by_col(lambda c: inverse_copy(c).start())
    for copy in copies[3:]:
        copy.start()

    for s in range(1, n_col):
        start = s * piece // 128 * 128
        if start:
            y_row[s, :, :start] = jnp.zeros((nrhs, start), jnp.float32)
            for q in range(per_col):
                y_in[q, s, :, :start] = jnp.zeros((nrhs, start), jnp.float32)

    even = lax.rem(row, 2) == 0
    short = row >= FIRST_SHORT
    feeds = (row + 1 >= FIRST_SHORT) & (row < end)
    is_end = row == end
    is_even_end = row == even_end
    is_ahead = row == ahead
    lent = row == ahead - 1
    before = row == ahead - 2
    long_count = longs_of(row)
    near_end = jnp.minimum(row + near_of(row) + 1, n_row)
    relays = col == own_home

    barrier = pltpu.get_barrier_semaphore()

    def signal(sem, i, s):
        pl.semaphore_signal(sem, inc=1, device_id=(i, s), device_id_type=MESH)

    def row_of(i, cond, act):
        @pl.when(cond)
        def _():
            for s in range(n_col):
                act(i, s)

        return jnp.where(cond, n_col, 0)

    def above(act):
        yield row + 1, row_of(row + 1, row < end, act)
        for d in range(2, NEAR + 2):
            wide = (is_ahead | before) if d == 2 else jnp.bool_(False)
            one = (row + d < n_row) & (d <= near_of(row)) & jnp.logical_not(wide)

            @pl.when(one)
            def _():
                act(row + d, own_home)

            yield row + d, jnp.where(one, 1, 0)
            if d == 2:
                yield row + d, row_of(row + d, wide, act)

    def below(act):
        row_of(row - 1, row > 0, act)
        count = jnp.where(row > 0, n_col, 0)
        for d in range(2, NEAR + 2):
            fed = (row >= d) & (d <= near_of(row - d)) & (lax.rem(jnp.maximum(row - d, 0), n_col) == col)
            if d == 2:
                fed = fed | is_end | is_ahead
            count += row_of(row - d, fed, act)
        for q in range(per_col):
            j = q * n_col + col
            far = j < row - near_of(j)

            @pl.when(far)
            def _():
                act(j, col)

            count += jnp.where(far, 1, 0)
        return count

    def at_once(low, high):
        return (low == 0) & (high == 1)

    for peer in peers:
        signal(barrier, row, peer)
    greeted = jnp.int32(n_col - 1)
    answers = jnp.int32(0)
    for i, count in above(lambda i, s: signal(barrier, i, s)):
        quick = at_once(row, i)
        greeted += jnp.where(quick, count, 0)
        answers += jnp.where(quick, 0, count)

    def greet_far(i, count):
        signal(barrier, i, col)
        return count + 1

    answers = lax.fori_loop(jnp.where(relays, near_end, n_row), n_row, greet_far, answers)

    def greet_quick(i, s):
        @pl.when(at_once(i, row))
        def _():
            signal(barrier, i, s)

    def answer(i, s):
        @pl.when(jnp.logical_not(at_once(i, row)))
        def _():
            signal(ready, i, s)

    greeted += below(greet_quick)

    prev = jnp.maximum(row - 1, 0)
    prev_slot = prev // n_col
    prev_home = lax.rem(prev, n_col)
    gives = short & (col == prev_home)
    crosses = short & even
    far_slot = ahead // n_col
    far_home = ahead % n_col
    gives_far = is_end & (col == far_home)
    handed = even & (row >= 2)
    mine = jnp.where(handed, long_count + jnp.where(is_even_end, 1, 0), 0)
    mine_slot = mine // n_col
    mine_home = lax.rem(mine, n_col)
    hands = handed & (col == mine_home)
    taken = (row >= 3) & jnp.logical_not(even)
    theirs = jnp.where(taken, longs_of(prev) + jnp.where(is_end, 1, 0), 0)
    their_home = lax.rem(theirs, n_col)
    takes = taken & (col == their_home)
    whole = even_end - 3
    whole_slot = whole // n_col
    whole_home = whole % n_col
    hands_whole = is_even_end & (col == whole_home)
    takes_whole = is_end & (col == whole_home)

    def masked_u(slot):
        keep = lax.broadcasted_iota(jnp.int32, (rank_max, width), 0) < rank_ref[slot]
        return jnp.where(keep, u_ref[slot].astype(jnp.float32), 0.0)

    def cut(tile, into):
        for s in range(n_col):
            into[s] = tile[:, s * piece:(s + 1) * piece]

    @pl.when(row > 0)
    def _():
        copies[0].wait()
        copies[1].wait()

    copies[4].wait()

    @pl.when(hands)
    def _():
        d_out[...] = v_ref[mine_slot].astype(jnp.float32)
        cut(masked_u(mine_slot), l_out)

    @pl.when(hands_whole)
    def _():
        d_out[...] = v_ref[whole_slot].astype(jnp.float32)
        cut(masked_u(whole_slot), l_out)

    @pl.when(gives)
    def _():
        cut(v_ref[prev_slot].astype(jnp.float32), v_out)
        cut(masked_u(prev_slot), u_out)

    @pl.when(gives_far)
    def _():
        cut(v_ref[far_slot].astype(jnp.float32), x_out)
        cut(masked_u(far_slot), t_out)

    pl.semaphore_wait(barrier, greeted)
    below(answer)

    def by_way(home, s, cc):
        across = n_col - 1 - home
        return (home != s) & jnp.where(across < home, (across != s) | (cc < s + some), (s > home) | (cc < s + half))

    def is_late(home, s, cc):
        across = n_col - 1 - home
        return (across == s) & (across < home) & (cc >= s + some)

    def split_row(home):
        return n_col - 1 - home < home

    def is_split(home, s):
        across = n_col - 1 - home
        return (across == s) & (across < home)

    def joined(home, s):
        across = n_col - 1 - home
        return (across > home) & (across == s)

    def spread(out, into, recv, target, home, cross):
        for s in range(n_col):
            if s > 0:

                @pl.when(cross & joined(home, s - 1))
                def _():
                    remote(out.at[s - 1], out.at[s - 1], v_send.at[s], m_recv.at[s - 1], (row, s)).start()

            for cc in range(s, n_col):
                gone = cross & (joined(home, s) | is_split(home, s))
                way = cross & by_way(home, s, cc)
                later = cross & is_late(home, s, cc)

                @pl.when(way & jnp.logical_not(gone))
                def _():
                    remote(out.at[cc], out.at[cc], v_send.at[s], m_recv.at[cc], (row, s)).start()

                @pl.when(jnp.logical_not(way | later | gone))
                def _():
                    remote(out.at[cc], into.at[cc], v_send.at[s], recv, (target, s)).start()

        for s in range(n_col):
            for cc in range(s, min(s + some, n_col)):

                @pl.when(cross & is_split(home, s))
                def _():
                    remote(out.at[cc], out.at[cc], v_send.at[s], m_recv.at[cc], (row, s)).start()

    def spread_late(out, into, recv, target, home):
        for s in range(n_col - 1):

            @pl.when(split_row(home) & (home == s + 1))
            def _():
                part = pl.ds(s, n_col - s)
                remote(out.at[part], out.at[part], v_send.at[s], m_recv.at[0], (row, s)).wait_send()

        for s in range(n_col):
            for cc in range(min(s + some, n_col), n_col):

                @pl.when(is_late(home, s, cc))
                def _():
                    remote(out.at[cc], into.at[cc], v_send.at[s], recv, (target, s)).start()

    def spread_done(out, home, cross):
        for s in range(n_col):
            part = pl.ds(s, n_col - s)
            gone = cross & joined(home, s)
            gone = gone | (cross & split_row(home) & (home == s + 1))
            more = (cross & joined(home, s - 1)) if s > 0 else jnp.bool_(False)

            @pl.when(jnp.logical_not(gone | more))
            def _():
                remote(out.at[part], out.at[part], v_send.at[s], m_recv.at[0], (row, s)).wait_send()

            if s > 0:
                part_more = pl.ds(s - 1, n_col - s + 1)

                @pl.when(more)
                def _():
                    remote(out.at[part_more], out.at[part_more], v_send.at[s], m_recv.at[0], (row, s)).wait_send()

    def relay(out, into, recv, target, home):
        across = n_col - 1 - home
        more = joined(home, col - 1)
        first = jnp.where(more, col - 1, col)
        part = jnp.where(across < home, across == col, col < home)
        share_of = jnp.where(across < home, some, half)
        stop = jnp.where(part, jnp.minimum(col + share_of, n_col), n_col)

        def forward(cc, carry):
            remote(out.at[cc], out.at[cc], v_send.at[0], m_recv.at[cc], (row, home)).wait_recv()

            @pl.when(cc >= col)
            def _():
                remote(out.at[cc], into.at[cc], f_send, recv, (target, col)).start()

            @pl.when(more)
            def _():
                remote(out.at[cc], out.at[cc], e_send, m_recv.at[cc], (row, across)).start()

            return carry

        lax.fori_loop(first, stop, forward, 0)

    def relay_done(out, home):
        across = n_col - 1 - home
        for cc in range(n_col):
            here = col == cc
            half_way = jnp.where(across < home, across == cc, cc < home)

            @pl.when(here & jnp.logical_not(half_way))
            def _():
                part = pl.ds(cc, n_col - cc)
                remote(out.at[part], out.at[part], f_send, v_recv, (row, home)).wait_send()

            for count, cond in ((some, across < home), (half, across > home)):
                few = pl.ds(cc, min(count, n_col - cc))

                @pl.when(here & half_way & cond)
                def _():
                    remote(out.at[few], out.at[few], f_send, v_recv, (row, home)).wait_send()

            if cc > 0:

                @pl.when((col == cc) & joined(home, cc - 1))
                def _():
                    part = pl.ds(cc - 1, n_col - cc + 1)
                    remote(out.at[part], out.at[part], e_send, v_recv, (row, home)).wait_send()

    def share(out, into, recv):
        for peer in peers:
            remote(out.at[peer], into, u_send, recv, (row, peer)).start()
        into[...] = out[col]

    def share_done(out):
        remote(out.at[others], out.at[others], u_send, u_recv, (row, peers[0])).wait_send()

    def shared_wait(into, recv, home):
        @pl.when(col != home)
        def _():
            remote(into, into, u_send, recv, (row, home)).wait_recv()

    early_l = (row < FIRST_SHORT) | is_even_end

    @pl.when(hands & early_l)
    def _():
        share(l_out, l_in, k_recv)

    @pl.when(hands_whole)
    def _():
        share(l_out, l2_in, du_recv)

    @pl.when(gives)
    def _():
        spread(v_out, v_in, v_recv, row - 1, prev_home, crosses)

    @pl.when(gives & (is_even_end | jnp.logical_not(even)))
    def _():
        share(u_out, u_in, u_recv)

    @pl.when(gives_far)
    def _():
        spread(x_out, x_in, x_recv, row - 2, far_home, jnp.bool_(True))

    @pl.when((handed) & (answers > 0))
    def _():
        pl.semaphore_wait(ready, answers)

    @pl.when(hands | hands_whole)
    def _():
        remote(d_out, d_in, d_send, d_recv, (row + 1, col)).start()

    relays_late = is_even_end & joined(prev_home, col)

    @pl.when(crosses & (col != prev_home) & jnp.logical_not(relays_late))
    def _():
        relay(v_out, v_in, v_recv, row - 1, prev_home)

    by_col(lambda c: inverse_copy(c).wait())
    copies[3].wait()

    def lend(src, dst, send, recv):
        return remote(src, dst, send, recv, (row + 1, col))

    def lend_inverse(c):
        return lend(hv_out.at[:, tail_of(c)], hv_in.at[:, tail_of(c)], wl_send, wx_recv)

    def lend_tail(c):
        hv_out[:, tail_of(c)] = inv_ref[:, tail_of(c)].astype(jnp.float32)
        lend_inverse(c).start()

    pl.when(lent)(functools.partial(by_col, lend_tail))

    for cc in range(n_col):

        @pl.when(col == cc)
        def _():
            base[...] = rhs_ref[:, cc * piece:(cc + 1) * piece]

    def log_part():
        for cc in range(n_col):

            @pl.when(col == cc)
            def _():
                block = inv_ref[:, cc * piece:(cc + 1) * piece].astype(jnp.float32)
                r_id = lax.broadcasted_iota(jnp.int32, (piece, piece), 0)
                c_id = lax.broadcasted_iota(jnp.int32, (piece, piece), 1)
                diagonal = jnp.sum(jnp.where(r_id == c_id, block, 0.0), axis=0, keepdims=True)
                total = jnp.sum(jnp.log(diagonal), axis=1, keepdims=True)
                logs[cc] = jnp.broadcast_to(total, (1, 128))

        for peer in peers:
            remote(logs.at[col], logs.at[col], l_send, l_recv, (row, peer)).start()

    pl.when(row > 0)(log_part)

    for q in range(per_col):

        @pl.when(q * n_col + col < long_count)
        def _():
            vt_ref[q] = v_ref[q].astype(jnp.float32).T.astype(jnp.bfloat16)

    @pl.when(gives & crosses)
    def _():
        spread_late(v_out, v_in, v_recv, row - 1, prev_home)

    def fold_with(into, recv, target):
        target[...] = jnp.zeros_like(target)
        for cc in range(n_col):
            part = pl.ds(cc, n_col - cc)

            @pl.when(col == cc)
            def _():
                remote(into.at[part], into.at[part], f_send, recv, (row, cc)).wait_recv()

        for cc in range(n_col):

            @pl.when(col <= cc)
            def _():
                target[...] += lax.dot_general(
                    inv_ref[:, cc * piece:(cc + 1) * piece],
                    into[cc].astype(jnp.bfloat16),
                    NT,
                    preferred_element_type=jnp.float32,
                )

    def long_step(q, cond):
        j = q * n_col + col

        @pl.when((j < long_count) & cond)
        def _():
            near = row - j <= near_of(j)

            @pl.when(near)
            def _():
                for s in range(n_col):
                    part = y_in.at[q, s, :, tail_of(s)]
                    remote(part, part, y_send.at[0], y_recv.at[q, s], (j, col)).wait_recv()
                y = y_in[q, 0]
                for s in range(1, n_col):
                    y = y + y_in[q, s]
                y_full[...] = y

            @pl.when(jnp.logical_not(near))
            def _():
                remote(y_in.at[q, 0], y_in.at[q, 0], y_send.at[0], y_recv.at[q, 0], (j, col)).wait_recv()
                y_full[...] = y_in[q, 0]

            y = y_full[...].astype(jnp.bfloat16)

            @pl.when(takes & (j == theirs))
            def _():
                wl_out[...] = jnp.dot(y, d_tile[...], preferred_element_type=jnp.float32)
                @pl.when(jnp.logical_not(is_ahead))
                def _():
                    for s in range(n_col):
                        remote(wl_out, wl_in, wl_send, wl_recv, (row - 1, s)).start()

                @pl.when(is_end | is_ahead)
                def _():
                    for peer in peers:
                        remote(wl_out, wl_in, wp_send, wl_recv, (row, peer)).start()
                    wl_in[...] = wl_out[...]

            @pl.when(takes_whole & (j == whole))
            def _():
                w2_out[...] = jnp.dot(y, d_tile[...], preferred_element_type=jnp.float32)
                for s in range(n_col):
                    remote(w2_out, w2_in, pd_send, p_recv.at[whole], (row - 1, s)).start()
                for peer in peers:
                    remote(w2_out, w2_in, du_send, x_recv, (row, peer)).start()
                w2_in[...] = w2_out[...]

            inner = jnp.dot(y, vt_ref[q], preferred_element_type=jnp.float32)
            keep = lax.broadcasted_iota(jnp.int32, (nrhs, rank_max), 1) < rank_ref[q]
            inner = jnp.where(keep, inner, 0.0).astype(jnp.bfloat16)
            p = jnp.dot(inner, u_ref[q], preferred_element_type=jnp.float32)
            for s in range(n_col):
                p_out[q, s] = p[:, s * piece:(s + 1) * piece]
            for peer in peers:
                remote(p_out.at[q, peer], p_in.at[j], p_send.at[q], p_recv.at[j], (row, peer)).start()
            p_in[j] = p_out[q, col]

    def products():
        fold_with(v_in, v_recv, fold)
        factor = fold[...].astype(jnp.bfloat16)
        shared_wait(u_in, u_recv, prev_home)
        shared_wait(l_in, k_recv, mine_home)
        a_out[0] = jnp.dot(u_in[...].astype(jnp.bfloat16), factor, preferred_element_type=jnp.float32)
        a_out[1] = jnp.dot(l_in[...].astype(jnp.bfloat16), factor, preferred_element_type=jnp.float32)
        shared_wait(l2_in, du_recv, whole_home)
        a_out[2] = jnp.dot(l2_in[...].astype(jnp.bfloat16), factor, preferred_element_type=jnp.float32)
        for k in range(3):
            for s in range(n_col):
                remote(a_out.at[k], a_in.at[k, col], a_send, a_recv, (row + 1, s)).start()

    @pl.when(relays_late)
    def _():
        products()
        relay(v_out, v_in, v_recv, row - 1, prev_home)

    @pl.when(takes | takes_whole)
    def _():
        remote(d_in, d_in, d_send, d_recv, (row - 1, col)).wait_recv()
        d_tile[...] = d_in[...].T.astype(jnp.bfloat16)

    @pl.when(is_end & (col != far_home))
    def _():
        relay(x_out, x_in, x_recv, row - 2, far_home)

    for q in range(per_col):
        long_step(q, jnp.logical_not(is_ahead & (q * n_col + col == row - 2)))

    def send_w(out, into, send, recv, i):
        for s in range(n_col):
            remote(out, into.at[col], send, recv, (i, s)).start()

    def wait_w(into, send, recv, i):
        remote(into, into, send, recv, (i, 0)).wait_recv()
        total = into[0]
        for s in range(1, n_col):
            total = total + into[s]
        return total

    def borrowed_y(c):
        tail = tail_of(c)
        slot = (ahead - 1) // n_col
        home = (ahead - 1) % n_col
        return remote(hy_out.at[:, tail], y_in.at[slot, c, :, tail], y_send.at[0], y_recv.at[slot, c], (end, home))

    @pl.when(is_ahead)
    def _():
        back = (row - 1, col)
        by_col(lambda c: remote(hv_in.at[:, tail_of(c)], hv_in.at[:, tail_of(c)], wl_send, wx_recv, back).wait_recv())
        by_col(lambda c: hv_tile.__setitem__((slice(None), tail_of(c)), hv_in[:, tail_of(c)].astype(jnp.bfloat16)))
        remote(hl_in, hl_in, a_send, k_recv, back).wait_recv()
        remote(hu_in, hu_in, we_send, a_recv, back).wait_recv()
        remote(hf_in, hf_in, wx_send, we_recv, back).wait_recv()
        remote(hb_in, hb_in, wp_send, t_recv, back).wait_recv()
        l_part = hl_in[...].astype(jnp.bfloat16)
        u_part = hu_in[...].astype(jnp.bfloat16)
        factor = hf_in[...].astype(jnp.bfloat16)

        @pl.when(answers > 0)
        def _():
            pl.semaphore_wait(ready, answers)

        @pl.when(jnp.logical_not(takes))
        def _():
            remote(wl_in, wl_in, wp_send, wl_recv, (row, their_home)).wait_recv()

        part = hb_in[...] - jnp.dot(wl_in[...].astype(jnp.bfloat16), l_part, preferred_element_type=jnp.float32)
        inner = wait_w(hw_in, w_send, du_recv, row - 2)
        part -= jnp.dot(inner.astype(jnp.bfloat16), u_part, preferred_element_type=jnp.float32)
        part = part.astype(jnp.bfloat16)
        hw_out[...] = jnp.dot(part, factor, preferred_element_type=jnp.float32)
        for peer in peers:
            remote(hw_out, w_in.at[col], a_send, w_recv, (row, peer)).start()
        w_in[col] = hw_out[...]

        def borrowed_part(c):
            tail = tail_of(c)
            hy_out[:, tail] = jnp.dot(part, hv_tile[:, tail], preferred_element_type=jnp.float32)
            borrowed_y(c).start()

        by_col(borrowed_part)
        hz_out[...] = part.astype(jnp.float32)
        remote(hz_out, hz_in, pd_send, du_recv, back).start()

    for q in range(per_col):
        long_step(q, is_ahead & (q * n_col + col == row - 2))

    pl.when(is_even_end & jnp.logical_not(relays_late))(products)

    @pl.when(feeds & jnp.logical_not(is_even_end))
    def _():
        fold_with(v_in, v_recv, fold)

        @pl.when(lent)
        def _():
            lend(fold, hf_in, wx_send, we_recv).start()

    @pl.when(gives & crosses & jnp.logical_not(is_even_end))
    def _():
        share(u_out, u_in, u_recv)

    @pl.when(hands & jnp.logical_not(early_l))
    def _():
        share(l_out, l_in, k_recv)

    @pl.when(gives_far)
    def _():
        spread_late(x_out, x_in, x_recv, row - 2, far_home)
        share(t_out, t_in, t_recv)

    @pl.when(is_ahead)
    def _():
        fold_with(x_in, x_recv, fold_x)

    @pl.when(is_end)
    def _():
        remote(a_in, a_in, a_send, a_recv, (row - 1, 0)).wait_recv()
        for k in range(3):
            total = a_in[k, 0]
            for s in range(1, n_col):
                total = total + a_in[k, s]
            a_sum[k] = total.astype(jnp.bfloat16)

    def gather_p(j, acc):
        home = lax.rem(j, n_col)

        @pl.when(home != col)
        def _():
            remote(p_in.at[j], p_in.at[j], p_send.at[0], p_recv.at[j], (row, home)).wait_recv()

        return acc - p_in[j]

    base[...] = lax.fori_loop(0, long_count, gather_p, base[...])

    @pl.when(lent)
    def _():
        hb_out[...] = base[...]
        lend(hb_out, hb_in, wp_send, t_recv).start()
        shared_wait(l_in, k_recv, mine_home)
        lend(l_in, hl_in, a_send, k_recv).start()
        shared_wait(u_in, u_recv, prev_home)
        lend(u_in, hu_in, we_send, a_recv).start()
        remote(hz_in, hz_in, pd_send, du_recv, (row + 1, col)).wait_recv()
        base[...] = hz_in[...]

    @pl.when(is_even_end)
    def _():
        w_out[...] = jnp.dot(base[...].astype(jnp.bfloat16), fold[...].astype(jnp.bfloat16), preferred_element_type=jnp.float32)
        send_w(w_out, w_in, w_send, w_recv, row + 1)

    @pl.when(handed & jnp.logical_not(lent))
    def _():
        @pl.when(jnp.logical_not(is_even_end))
        def _():
            shared_wait(l_in, k_recv, mine_home)

        l_part = l_in[...].astype(jnp.bfloat16)

        @pl.when(is_even_end)
        def _():
            remote(w2_in, w2_in, pd_send, p_recv.at[whole], (row + 1, whole_home)).wait_recv()
            base[...] -= jnp.dot(
                w2_in[...].astype(jnp.bfloat16), l2_in[...].astype(jnp.bfloat16), preferred_element_type=jnp.float32
            )

        remote(wl_in, wl_in, wl_send, wl_recv, (row + 1, mine_home)).wait_recv()
        base[...] -= jnp.dot(wl_in[...].astype(jnp.bfloat16), l_part, preferred_element_type=jnp.float32)

    @pl.when(is_ahead)
    def _():
        shared_wait(u_in, u_recv, prev_home)
        u_part = u_in[...].astype(jnp.bfloat16)
        part = w_in.at[others]
        remote(part, part, a_send, w_recv, (row, peers[0])).wait_recv()
        inner = w_in[0]
        for s in range(1, n_col):
            inner = inner + w_in[s]
        base[...] -= jnp.dot(inner.astype(jnp.bfloat16), u_part, preferred_element_type=jnp.float32)

    @pl.when(short & jnp.logical_not(is_end | is_ahead | lent))
    def _():
        @pl.when(jnp.logical_not(is_even_end))
        def _():
            shared_wait(u_in, u_recv, prev_home)

        u_part = u_in[...].astype(jnp.bfloat16)
        inner = wait_w(w_in, w_send, w_recv, row - 1)
        base[...] -= jnp.dot(inner.astype(jnp.bfloat16), u_part, preferred_element_type=jnp.float32)

    @pl.when(is_end)
    def _():
        shared_wait(u_in, u_recv, prev_home)
        shared_wait(t_in, t_recv, far_home)
        u_part = u_in[...].astype(jnp.bfloat16)
        t_part = t_in[...].astype(jnp.bfloat16)

        @pl.when(jnp.logical_not(takes))
        def _():
            remote(wl_in, wl_in, wp_send, wl_recv, (row, their_home)).wait_recv()

        @pl.when(jnp.logical_not(takes_whole))
        def _():
            remote(w2_in, w2_in, du_send, x_recv, (row, whole_home)).wait_recv()

        inner = wait_w(w_in, w_send, w_recv, row - 1)
        inner -= jnp.dot(w2_in[...].astype(jnp.bfloat16), a_sum[2], preferred_element_type=jnp.float32)
        inner -= jnp.dot(wl_in[...].astype(jnp.bfloat16), a_sum[1], preferred_element_type=jnp.float32)
        late = wait_w(wx_in, wx_send, wx_recv, row - 2)
        base[...] -= jnp.dot(late.astype(jnp.bfloat16), t_part, preferred_element_type=jnp.float32)
        late = wait_w(we_in, we_send, we_recv, row - 2)
        inner -= jnp.dot(late.astype(jnp.bfloat16), a_sum[0], preferred_element_type=jnp.float32)
        base[...] -= jnp.dot(inner.astype(jnp.bfloat16), u_part, preferred_element_type=jnp.float32)

    reduced = base[...].astype(jnp.bfloat16)

    @pl.when(jnp.logical_not(even | is_ahead) & (answers > 0))
    def _():
        pl.semaphore_wait(ready, answers)

    @pl.when(feeds & jnp.logical_not(is_even_end | lent))
    def _():
        w_out[...] = jnp.dot(reduced, fold[...].astype(jnp.bfloat16), preferred_element_type=jnp.float32)

        @pl.when(is_ahead)
        def _():
            send_w(w_out, w_in, w_send, w_recv, row + 1)
            send_w(w_out, we_in, we_send, we_recv, row + 2)
            wx_out[...] = jnp.dot(reduced, fold_x[...].astype(jnp.bfloat16), preferred_element_type=jnp.float32)
            send_w(wx_out, wx_in, wx_send, wx_recv, row + 2)

        @pl.when(before)
        def _():
            send_w(w_out, hw_in, w_send, du_recv, row + 2)

        @pl.when(jnp.logical_not(before | is_ahead))
        def _():
            send_w(w_out, w_in, w_send, w_recv, row + 1)

    def own_part(c):
        tail = tail_of(c)
        y_row[c, :, tail] = jnp.dot(reduced, inv_ref[:, tail], preferred_element_type=jnp.float32)

    by_col(own_part)

    def near_copy(i, c):
        tail = tail_of(c)
        return remote(
            y_row.at[c, :, tail], y_in.at[own_slot, c, :, tail], y_send.at[lax.rem(i - row - 1, y_sends)], y_recv.at[own_slot, c], (i, own_home)
        )

    def send_y(i, carry):
        @pl.when((row < longs_of(i)) & jnp.logical_not(lent))
        def _():
            by_col(lambda c: near_copy(i, c).start())

        return carry

    def own_copy(c, peer):
        part = y_row.at[c, :, tail_of(c)]
        return remote(part, part, o_send, o_recv.at[c], (row, peer))

    first = row == 0
    lax.fori_loop(row + 1, jnp.where(first, 2, near_end), send_y, 0)
    for peer in peers:
        by_col(lambda c: own_copy(c, peer).start())

    @pl.when(first)
    def _():
        log_part()
        pl.semaphore_wait(ready, answers)
        lax.fori_loop(2, near_end, send_y, 0)

    remote(logs.at[others], logs.at[others], l_send, l_recv, (row, peers[0])).wait()
    log_sum = logs[0]
    for s in range(1, n_col):
        log_sum = log_sum + logs[s]
    log_term = log_sum * (1.0 / width) - 0.5 * math.log(2.0 * math.pi)

    def left_y(i, carry):
        @pl.when((row < longs_of(i)) & jnp.logical_not(lent))
        def _():
            by_col(lambda c: near_copy(i, c).wait_send())

        return carry

    lax.fori_loop(row + 1, near_end, left_y, 0)

    @pl.when(feeds & jnp.logical_not(lent))
    def _():
        remote(w_in, w_in, w_send, w_recv, (row + 1, 0)).wait_send()

    @pl.when(lent)
    def _():
        by_col(lambda c: lend_inverse(c).wait_send())
        lend(fold, hf_in, wx_send, we_recv).wait_send()
        lend(hb_out, hb_in, wp_send, t_recv).wait_send()
        lend(l_in, hl_in, a_send, k_recv).wait_send()
        lend(u_in, hu_in, we_send, a_recv).wait_send()

    @pl.when(is_ahead)
    def _():
        part = w_in.at[others]
        remote(part, part, a_send, w_recv, (row, peers[0])).wait_send()
        by_col(lambda c: borrowed_y(c).wait_send())
        remote(hz_out, hz_in, pd_send, du_recv, (row - 1, col)).wait_send()
        remote(w_in, w_in, we_send, we_recv, (row + 2, 0)).wait_send()
        remote(w_in, w_in, wx_send, wx_recv, (row + 2, 0)).wait_send()

    @pl.when(is_even_end)
    def _():
        remote(a_in, a_in, a_send, a_recv, (row + 1, 0)).wait_send()

    @pl.when(takes)
    def _():
        @pl.when(jnp.logical_not(is_ahead))
        def _():
            remote(w_in, w_in, wl_send, wl_recv, (row - 1, 0)).wait_send()

        @pl.when(is_end | is_ahead)
        def _():
            remote(w_in.at[others], w_in.at[others], wp_send, wl_recv, (row, peers[0])).wait_send()

    @pl.when(hands)
    def _():
        remote(d_out, d_in, d_send, d_recv, (row + 1, col)).wait_send()
        share_done(l_out)

    @pl.when(hands_whole)
    def _():
        remote(d_out, d_in, d_send, d_recv, (row + 1, col)).wait_send()
        share_done(l_out)

    @pl.when(takes_whole)
    def _():
        remote(w_in, w_in, pd_send, p_recv.at[0], (row - 1, 0)).wait_send()
        remote(w_in.at[others], w_in.at[others], du_send, x_recv, (row, peers[0])).wait_send()

    @pl.when(gives)
    def _():
        spread_done(v_out, prev_home, crosses)
        share_done(u_out)

    @pl.when(gives_far)
    def _():
        spread_done(x_out, far_home, jnp.bool_(True))
        share_done(t_out)

    @pl.when(crosses & (col != prev_home))
    def _():
        relay_done(v_out, prev_home)

    @pl.when(is_end & (col != far_home))
    def _():
        relay_done(x_out, far_home)

    for q in range(per_col):

        @pl.when(q * n_col + col < long_count)
        def _():
            part = p_out.at[q, others]
            remote(part, part, p_send.at[q], p_recv.at[0], (row, peers[0])).wait_send()

    for s in range(n_col):

        @pl.when(col != s)
        def _():
            own_copy(s, peers[0]).wait_recv()

    y = y_row[0]
    for s in range(1, n_col):
        y = y + y_row[s]
    y_all[...] = y

    def far_copy(i):
        return remote(y_all, y_in.at[own_slot, 0], y_send.at[lax.rem(i - row - 1, y_sends)], y_recv.at[own_slot, 0], (i, col))

    def send_far(i, carry):
        far_copy(i).start()
        return carry

    lax.fori_loop(jnp.where(relays, near_end, n_row), n_row, send_far, 0)
    white_ref[0, 0] = y
    quadratic = jnp.sum(y * y, axis=1, keepdims=True) * (1.0 / width)
    lik = -0.5 * quadratic + log_term
    r_id = lax.broadcasted_iota(jnp.int32, (nrhs, 128), 0)
    c_id = lax.broadcasted_iota(jnp.int32, (nrhs, 128), 1)
    flat = jnp.sum(jnp.where(r_id == c_id, lik, 0.0), axis=0, keepdims=True)
    lik_ref[0] = flat[:, :nrhs]

    def left_far(i, carry):
        far_copy(i).wait_send()
        return carry

    lax.fori_loop(jnp.where(relays, near_end, n_row), n_row, left_far, 0)

    def own_left(c):
        part = y_row.at[others, :, tail_of(c)]
        remote(part, part, o_send, o_recv.at[c], (row, peers[0])).wait_send()

    by_col(own_left)


def local(n_row, n_col, right_side, inverse_t, u_factor, v_factor, ranks):
    nrhs, width = right_side.shape[2:]
    per_col, _, rank_max = u_factor.shape[2:5]
    piece = width // n_col
    vmem = pl.BlockSpec(memory_space=pltpu.VMEM)
    hbm = pl.BlockSpec(memory_space=pl.ANY)
    dma = pltpu.SemaphoreType.DMA

    def f32(*shape):
        return pltpu.VMEM(shape, jnp.float32)

    def bf16(*shape):
        return pltpu.VMEM(shape, jnp.bfloat16)

    tile_set = [
        f32(n_col, rank_max, piece),
        f32(n_col, rank_max, piece),
        f32(n_col, rank_max, piece),
        f32(rank_max, piece),
        f32(piece, rank_max),
        f32(nrhs, rank_max),
        f32(n_col, nrhs, rank_max),
    ]
    return pl.pallas_call(
        functools.partial(kernel, n_row, n_col),
        out_shape=(
            pltpu.VMEM((1, 1, nrhs, width), jnp.float32),
            pltpu.VMEM((1, 1, nrhs), jnp.float32),
        ),
        in_specs=[hbm, hbm, hbm, hbm, hbm],
        out_specs=(vmem, vmem),
        scratch_shapes=[
            f32(nrhs, width),
            bf16(piece, width),
            bf16(per_col, rank_max, width),
            bf16(per_col, rank_max, width),
            pltpu.SMEM((per_col,), jnp.int32),
            f32(per_col, n_col, nrhs, width),
            f32(per_col, n_col, nrhs, piece),
            f32(n_row, nrhs, piece),
            f32(n_col, nrhs, width),
            f32(n_col, 1, 128),
            f32(nrhs, piece),
            f32(nrhs, width),
            f32(nrhs, width),
            *tile_set,
            *tile_set,
            f32(rank_max, width),
            f32(rank_max, width),
            bf16(width, rank_max),
            bf16(per_col, width, rank_max),
            f32(rank_max, piece),
            f32(nrhs, rank_max),
            f32(nrhs, rank_max),
            f32(n_col, rank_max, piece),
            f32(rank_max, piece),
            f32(nrhs, rank_max),
            f32(nrhs, rank_max),
            f32(n_col, nrhs, rank_max),
            f32(3, rank_max, rank_max),
            f32(3, n_col, rank_max, rank_max),
            bf16(3, rank_max, rank_max),
            f32(rank_max, piece),
            f32(rank_max, piece),
            f32(piece, rank_max),
            f32(piece, width),
            f32(piece, width),
            bf16(piece, width),
            f32(nrhs, piece),
            f32(nrhs, piece),
            f32(nrhs, piece),
            f32(nrhs, piece),
            f32(nrhs, rank_max),
            f32(n_col, nrhs, rank_max),
            f32(nrhs, width),
            dma((5,)),
            dma((max(NEAR + 1, n_row - NEAR - 1),)),
            dma((per_col, n_col)),
            dma((per_col,)),
            dma((n_row - 3,)),
            dma, dma((n_col,)), dma, dma,
            dma((n_col,)),
            dma, dma, dma, dma, dma,
            dma((n_col,)),
            dma, dma,
            pltpu.SemaphoreType.REGULAR,
            dma, dma, dma, dma, dma, dma, dma, dma,
            dma, dma, dma,
            dma, dma, dma, dma, dma, dma,
        ],
        compiler_params=pltpu.CompilerParams(collective_id=0, has_side_effects=True),
        name="forward_solve",
    )(right_side, inverse_t, u_factor, v_factor, ranks.reshape(per_col))


def solution(mesh):
    placed = (
        P(None, "row", None, None),
        P(None, "row", "col", None),
        P(None, "row", None, "col", None, None),
        P(None, "row", None, "col", None, None),
        P(None, "row", None, "col"),
    )
    return jax.shard_map(
        functools.partial(local, mesh.shape["row"], mesh.shape["col"]),
        mesh=mesh,
        in_specs=placed,
        out_specs=(P(None, "row", None, None), P(None, "row", None)),
        check_vma=False,
    )
```

```python
import functools
import math

import jax
import jax.numpy as jnp
from jax import lax
from jax.experimental import pallas as pl
from jax.experimental.pallas import tpu as pltpu
from jax.sharding import PartitionSpec as P

MESH = pl.DeviceIdType.MESH
NT = (((1,), (1,)), ((), ()))
FIRST_SHORT = 3
NEAR = 3


def remote(src, dst, send_sem, recv_sem, device):
    return pltpu.make_async_remote_copy(
        src_ref=src,
        dst_ref=dst,
        send_sem=send_sem,
        recv_sem=recv_sem,
        device_id=device,
        device_id_type=MESH,
    )


def kernel(
    n_row, n_col,
    rhs_hbm, inv_hbm, u_hbm, v_hbm, rank_hbm,
    white_ref, lik_ref,
    rhs_ref, inv_ref, u_ref, v_ref, rank_ref,
    y_in, p_out, p_in, y_row, logs, base, y_full, y_all, tally,
    v_out, v_in, u_out, u_in, fold, w_out, w_in,
    x_out, x_in, t_out, t_in, fold_x, wx_out, wx_in,
    d_out, d_in, d_tile, vt_ref, l2_in, w2_out, w2_in, l_out, l_in, wl_out, wl_in, we_in,
    a_out, a_in, a_sum,
    hl_in, hu_in, hf_in, hv_out, hv_in, hv_tile, hb_out, hb_in, hz_out, hz_in, hw_out, hw_in, hy_out,
    in_sem, y_send, y_recv, p_send, p_recv, o_send, o_recv, l_send, l_recv,
    v_send, v_recv, u_send, u_recv, w_send, w_recv, m_recv, f_send, e_send, ready, ready_far, pass_send,
    x_recv, t_recv, k_recv, d_send, d_recv, du_recv, wl_send, wl_recv, wp_send,
    we_send, we_recv, wx_send, wx_recv, a_send, a_recv,
):
    row = lax.axis_index("row")
    col = lax.axis_index("col")
    per_col, rank_max, width = u_ref.shape
    nrhs = rhs_ref.shape[0]
    piece = width // n_col
    half = n_col // 2
    y_sends = y_send.shape[0]
    some = half
    peers = [lax.rem(col + k, n_col) for k in range(1, n_col)]
    others = pl.ds(0, n_col - 1)
    own_slot = row // n_col
    own_home = lax.rem(row, n_col)
    end = n_row - 1
    even_end = n_row - 2
    ahead = n_row - 3

    def longs_of(i):
        count = jnp.where(i >= FIRST_SHORT, i - 1, i)
        handed = (lax.rem(i, 2) == 0) & (i >= 2)
        return count - jnp.where(handed, 1, 0) - jnp.where(i >= even_end, 1, 0)

    def near_of(i):
        return jnp.where(i == 0, 1, NEAR + jnp.where(i >= 2, 1, 0))

    copies = [
        pltpu.make_async_copy(v_hbm.at[0, 0, :, 0], v_ref, in_sem.at[0]),
        pltpu.make_async_copy(u_hbm.at[0, 0, :, 0], u_ref, in_sem.at[1]),
        None,
        pltpu.make_async_copy(rhs_hbm.at[0, 0], rhs_ref, in_sem.at[3]),
        pltpu.make_async_copy(rank_hbm, rank_ref, in_sem.at[4]),
    ]
    @pl.when(lax.axis_index("row") > 0)
    def _():
        copies[0].start()
        copies[1].start()

    def tail_of(c):
        start = c * piece // 128 * 128
        return pl.ds(start, width - start)

    def inverse_copy(c):
        return pltpu.make_async_copy(inv_hbm.at[0, 0, :, tail_of(c)], inv_ref.at[:, tail_of(c)], in_sem.at[2])

    def by_col(act):
        for c in range(n_col):
            pl.when(col == c)(functools.partial(act, c))

    by_col(lambda c: inverse_copy(c).start())
    for copy in copies[3:]:
        copy.start()
    barrier = pltpu.get_barrier_semaphore()

    def signal(sem, i, s):
        pl.semaphore_signal(sem, inc=1, device_id=(i, s), device_id_type=MESH)

    for peer in peers:
        signal(barrier, row, peer)

    def set_base():
        for cc in range(n_col):

            @pl.when(col == cc)
            def _():
                base[...] = rhs_ref[:, cc * piece:(cc + 1) * piece]

    def own_part(c, reduced):
        tail = tail_of(c)
        y_row[c, :, tail] = jnp.dot(reduced, inv_ref[:, tail], preferred_element_type=jnp.float32)

    def near_copy(i, c):
        tail = tail_of(c)
        sem = y_send.at[lax.rem(i - row - 1, y_sends)]
        return remote(y_row.at[c, :, tail], y_in.at[own_slot, c, :, tail], sem, y_recv.at[own_slot], (i, own_home))

    first = row == 0

    @pl.when(first)
    def _():
        for s in range(n_col):
            signal(barrier, 1, s)
        copies[3].wait()
        by_col(lambda c: inverse_copy(c).wait())
        set_base()
        reduced = base[...].astype(jnp.bfloat16)
        by_col(lambda c: own_part(c, reduced))
        pl.semaphore_wait(barrier, 2 * n_col - 1)
        by_col(lambda c: near_copy(1, c).start())

    for s in range(1, n_col):
        start = s * piece // 128 * 128
        if start:
            y_row[s, :, :start] = jnp.zeros((nrhs, start), jnp.float32)
            for q in range(per_col):
                y_in[q, s, :, :start] = jnp.zeros((nrhs, start), jnp.float32)

    even = lax.rem(row, 2) == 0
    short = row >= FIRST_SHORT
    feeds = (row + 1 >= FIRST_SHORT) & (row < end)
    is_end = row == end
    is_even_end = row == even_end
    is_ahead = row == ahead
    lent = row == ahead - 1
    before = row == ahead - 2
    long_count = longs_of(row)
    near_end = jnp.minimum(row + near_of(row) + 1, n_row)
    relays = (col == own_home) & (row > 0)
    passes = (row == 1) & (col == 0)

    def row_of(i, cond, act):
        @pl.when(cond)
        def _():
            for s in range(n_col):
                act(i, s)

        return jnp.where(cond, n_col, 0)

    def above(act):
        yield row + 1, row_of(row + 1, (row > 0) & (row < end), act)
        for d in range(2, NEAR + 2):
            wide = (is_ahead | before) if d == 2 else jnp.bool_(False)
            one = (row + d < n_row) & (d <= near_of(row)) & jnp.logical_not(wide)

            @pl.when(one)
            def _():
                act(row + d, own_home)

            yield row + d, jnp.where(one, 1, 0)
            if d == 2:
                yield row + d, row_of(row + d, wide, act)

    def below(act, act_far=None):
        row_of(row - 1, row > 0, act)
        count = jnp.where(row > 0, n_col, 0)
        for d in range(2, NEAR + 2):
            fed = (row >= d) & (d <= near_of(row - d)) & (lax.rem(jnp.maximum(row - d, 0), n_col) == col)
            if d == 2:
                fed = fed | is_end | is_ahead
            count += row_of(row - d, fed, act)
        for q in range(per_col):
            j = q * n_col + col
            far = j < row - near_of(j)

            source = jnp.where(j == 0, 1, j)
            soon = (j == 0) & (row <= 3)

            @pl.when(far & soon)
            def _():
                act(source, col)

            @pl.when(far & jnp.logical_not(soon))
            def _():
                (act_far or act)(source, col)

            count += jnp.where(far, 1, 0)
        return count

    def at_once(low, high):
        return (low == 0) & (high == 1)

    greeted = jnp.int32(n_col - 1)
    answers = jnp.int32(0)
    for i, count in above(lambda i, s: signal(barrier, i, s)):
        answers += count

    def greet_far(i, count):
        signal(barrier, i, col)
        return count + 1

    far_answers = lax.fori_loop(jnp.where(relays, near_end, n_row), n_row, greet_far, jnp.int32(0))
    far_answers = lax.fori_loop(jnp.where(passes, 4, n_row), n_row, greet_far, far_answers)
    answers = lax.fori_loop(jnp.where(passes, 2, n_row), jnp.where(passes, 4, n_row), greet_far, answers)

    def greet_quick(i, s):
        @pl.when(at_once(i, row))
        def _():
            signal(barrier, i, s)

    def answer(i, s):
        @pl.when(jnp.logical_not(at_once(i, row)))
        def _():
            signal(ready, i, s)

    greeted += below(greet_quick)

    prev = jnp.maximum(row - 1, 0)
    prev_slot = prev // n_col
    prev_home = lax.rem(prev, n_col)
    gives = short & (col == prev_home)
    crosses = short & even
    far_slot = ahead // n_col
    far_home = ahead % n_col
    gives_far = is_end & (col == far_home)
    handed = even & (row >= 2)
    mine = jnp.where(handed, long_count + jnp.where(is_even_end, 1, 0), 0)
    mine_slot = mine // n_col
    mine_home = lax.rem(mine, n_col)
    hands = handed & (col == mine_home)
    taken = (row >= 3) & jnp.logical_not(even)
    theirs = jnp.where(taken, longs_of(prev) + jnp.where(is_end, 1, 0), 0)
    their_home = lax.rem(theirs, n_col)
    takes = taken & (col == their_home)
    whole = even_end - 3
    whole_slot = whole // n_col
    whole_home = whole % n_col
    hands_whole = is_even_end & (col == whole_home)
    takes_whole = is_end & (col == whole_home)

    def masked_u(slot):
        keep = lax.broadcasted_iota(jnp.int32, (rank_max, width), 0) < rank_ref[slot]
        return jnp.where(keep, u_ref[slot].astype(jnp.float32), 0.0)

    def cut(tile, into):
        for s in range(n_col):
            into[s] = tile[:, s * piece:(s + 1) * piece]

    @pl.when(row > 0)
    def _():
        copies[0].wait()
        copies[1].wait()

    copies[4].wait()

    @pl.when(hands)
    def _():
        d_out[...] = v_ref[mine_slot].astype(jnp.float32)
        cut(masked_u(mine_slot), l_out)

    @pl.when(hands_whole)
    def _():
        d_out[...] = v_ref[whole_slot].astype(jnp.float32)
        cut(masked_u(whole_slot), l_out)

    @pl.when(gives)
    def _():
        cut(v_ref[prev_slot].astype(jnp.float32), v_out)
        cut(masked_u(prev_slot), u_out)

    @pl.when(gives_far)
    def _():
        cut(v_ref[far_slot].astype(jnp.float32), x_out)
        cut(masked_u(far_slot), t_out)

    @pl.when(row > 0)
    def _():
        pl.semaphore_wait(barrier, greeted)

    below(answer, lambda i, s: signal(ready_far, i, s))

    def by_way(home, s, cc):
        across = n_col - 1 - home
        return (home != s) & jnp.where(across < home, (across != s) | (cc < s + some), (s > home) | (cc < s + half))

    def is_late(home, s, cc):
        across = n_col - 1 - home
        return (across == s) & (across < home) & (cc >= s + some)

    def split_row(home):
        return n_col - 1 - home < home

    def is_split(home, s):
        across = n_col - 1 - home
        return (across == s) & (across < home)

    def joined(home, s):
        across = n_col - 1 - home
        return (across > home) & (across == s)

    def spread(out, into, recv, target, home, cross):
        for s in range(n_col):
            for cc in range(s, min(s + some, n_col)):

                @pl.when(cross & is_split(home, s))
                def _():
                    remote(out.at[cc], out.at[cc], v_send.at[s], m_recv.at[cc], (row, s)).start()

        for s in range(n_col):
            if s > 0:

                @pl.when(cross & joined(home, s - 1))
                def _():
                    remote(out.at[s - 1], out.at[s - 1], v_send.at[s], m_recv.at[s - 1], (row, s)).start()

            for cc in range(s, n_col):
                gone = cross & (joined(home, s) | is_split(home, s))
                way = cross & by_way(home, s, cc)
                later = cross & is_late(home, s, cc)

                @pl.when(way & jnp.logical_not(gone))
                def _():
                    remote(out.at[cc], out.at[cc], v_send.at[s], m_recv.at[cc], (row, s)).start()

                @pl.when(jnp.logical_not(way | later | gone))
                def _():
                    remote(out.at[cc], into.at[cc], v_send.at[s], recv.at[cc], (target, s)).start()

    def spread_late(out, into, recv, target, home):
        for s in range(n_col):

            @pl.when(split_row(home) & (n_col - home == s))
            def _():
                part = pl.ds(s, n_col - s)
                remote(out.at[part], out.at[part], v_send.at[s], m_recv.at[0], (row, s)).wait_send()

        for s in range(n_col):
            for cc in range(min(s + some, n_col), n_col):

                @pl.when(is_late(home, s, cc))
                def _():
                    remote(out.at[cc], into.at[cc], v_send.at[s], recv.at[cc], (target, s)).start()

    def spread_done(out, home, cross):
        for s in range(n_col):
            part = pl.ds(s, n_col - s)
            gone = cross & joined(home, s)
            gone = gone | (cross & split_row(home) & (n_col - home == s))
            more = (cross & joined(home, s - 1)) if s > 0 else jnp.bool_(False)

            @pl.when(jnp.logical_not(gone | more))
            def _():
                remote(out.at[part], out.at[part], v_send.at[s], m_recv.at[0], (row, s)).wait_send()

            if s > 0:
                part_more = pl.ds(s - 1, n_col - s + 1)

                @pl.when(more)
                def _():
                    remote(out.at[part_more], out.at[part_more], v_send.at[s], m_recv.at[0], (row, s)).wait_send()

    def relay(out, into, recv, target, home):
        across = n_col - 1 - home
        more = joined(home, col - 1)
        first = jnp.where(more, col - 1, col)
        part = jnp.where(across < home, across == col, col < home)
        share_of = jnp.where(across < home, some, half)
        stop = jnp.where(part, jnp.minimum(col + share_of, n_col), n_col)
        stop = jnp.where(joined(home, col), col + 1, stop)

        def forward(cc, carry):
            remote(out.at[cc], out.at[cc], v_send.at[0], m_recv.at[cc], (row, home)).wait_recv()

            @pl.when(cc >= col)
            def _():
                remote(out.at[cc], into.at[cc], f_send, recv.at[cc], (target, col)).start()

            @pl.when(more & (cc == across))
            def _():
                remote(out.at[cc], out.at[cc], e_send, m_recv.at[cc], (row, across)).start()

            @pl.when(more & (cc > across))
            def _():
                remote(out.at[cc], into.at[cc], e_send, recv.at[cc], (target, across)).start()

            return carry

        lax.fori_loop(first, stop, forward, 0)

    def relay_done(out, home):
        across = n_col - 1 - home
        for cc in range(n_col):
            here = col == cc
            half_way = jnp.where(across < home, across == cc, cc < home)

            @pl.when(here & joined(home, cc))
            def _():
                remote(out.at[cc], out.at[cc], f_send, v_recv.at[0], (row, home)).wait_send()

            @pl.when(here & jnp.logical_not(half_way | joined(home, cc)))
            def _():
                part = pl.ds(cc, n_col - cc)
                remote(out.at[part], out.at[part], f_send, v_recv.at[0], (row, home)).wait_send()

            for count, cond in ((some, across < home), (half, across > home)):
                few = pl.ds(cc, min(count, n_col - cc))

                @pl.when(here & half_way & cond)
                def _():
                    remote(out.at[few], out.at[few], f_send, v_recv.at[0], (row, home)).wait_send()

            if cc > 0:

                @pl.when((col == cc) & joined(home, cc - 1))
                def _():
                    part = pl.ds(cc - 1, n_col - cc + 1)
                    remote(out.at[part], out.at[part], e_send, v_recv.at[0], (row, home)).wait_send()

    def share(out, into, recv):
        for k in range(n_col):
            peer = lax.rem(2 * n_col - 1 - col + k, n_col)

            @pl.when(peer != col)
            def _():
                remote(out.at[peer], into, u_send, recv, (row, peer)).start()

        into[...] = out[col]

    def share_done(out):
        remote(out.at[others], out.at[others], u_send, u_recv, (row, peers[0])).wait_send()

    def shared_wait(into, recv, home):
        @pl.when(col != home)
        def _():
            remote(into, into, u_send, recv, (row, home)).wait_recv()

    early_l = (row < FIRST_SHORT) | is_even_end

    opposite = n_col - 1 - col

    @pl.when(hands)
    def _():
        for peer in peers:

            @pl.when(early_l | (peer != opposite))
            def _():
                remote(l_out.at[peer], l_in, u_send, k_recv, (row, peer)).start()

        l_in[...] = l_out[col]

    @pl.when(hands_whole)
    def _():
        share(l_out, l2_in, du_recv)

    @pl.when(gives)
    def _():
        spread(v_out, v_in, v_recv, row - 1, prev_home, crosses)

    @pl.when(gives & (is_even_end | jnp.logical_not(even)))
    def _():
        share(u_out, u_in, u_recv)

    @pl.when(gives_far)
    def _():
        spread(x_out, x_in, x_recv, row - 2, far_home, jnp.bool_(True))

    @pl.when((handed) & (answers > 0))
    def _():
        pl.semaphore_wait(ready, answers)

    @pl.when(hands | hands_whole)
    def _():
        remote(d_out, d_in, d_send, d_recv, (row + 1, col)).start()

    relays_late = is_even_end & joined(prev_home, col)

    @pl.when(crosses & (col != prev_home) & jnp.logical_not(relays_late))
    def _():
        relay(v_out, v_in, v_recv, row - 1, prev_home)

    @pl.when(row > 0)
    def _():
        by_col(lambda c: inverse_copy(c).wait())
        copies[3].wait()


    def lend(src, dst, send, recv):
        return remote(src, dst, send, recv, (row + 1, col))

    def lend_inverse(c):
        return lend(hv_out.at[:, tail_of(c)], hv_in.at[:, tail_of(c)], wl_send, wx_recv)

    def lend_tail(c):
        hv_out[:, tail_of(c)] = inv_ref[:, tail_of(c)].astype(jnp.float32)
        lend_inverse(c).start()

    pl.when(lent)(functools.partial(by_col, lend_tail))

    pl.when(row > 0)(set_base)

    def log_part():
        for cc in range(n_col):

            @pl.when(col == cc)
            def _():
                block = inv_ref[:, cc * piece:(cc + 1) * piece].astype(jnp.float32)
                r_id = lax.broadcasted_iota(jnp.int32, (piece, piece), 0)
                c_id = lax.broadcasted_iota(jnp.int32, (piece, piece), 1)
                diagonal = jnp.sum(jnp.where(r_id == c_id, block, 0.0), axis=0, keepdims=True)
                total = jnp.sum(jnp.log(diagonal), axis=1, keepdims=True)
                logs[cc] = jnp.broadcast_to(total, (1, 128))

        for peer in peers:
            remote(logs.at[col], logs.at[col], l_send, l_recv, (row, peer)).start()

    pl.when(row > 0)(log_part)

    for q in range(per_col):

        @pl.when(q * n_col + col < long_count)
        def _():
            vt_ref[q] = v_ref[q].astype(jnp.float32).T.astype(jnp.bfloat16)

    @pl.when(gives & crosses)
    def _():
        spread_late(v_out, v_in, v_recv, row - 1, prev_home)

    @pl.when(gives & crosses & jnp.logical_not(is_even_end))
    def _():
        share(u_out, u_in, u_recv)

    @pl.when(hands & jnp.logical_not(early_l))
    def _():
        remote(l_out.at[opposite], l_in, u_send, k_recv, (row, opposite)).start()

    def fold_with(into, recv, target):
        target[...] = jnp.zeros_like(target)
        for cc in range(n_col):

            @pl.when(col <= cc)
            def _():
                remote(into.at[cc], into.at[cc], f_send, recv.at[cc], (row, cc)).wait_recv()
                target[...] += lax.dot_general(
                    inv_ref[:, cc * piece:(cc + 1) * piece],
                    into[cc].astype(jnp.bfloat16),
                    NT,
                    preferred_element_type=jnp.float32,
                )

    def long_step(q, cond):
        j = q * n_col + col

        @pl.when((j < long_count) & cond)
        def _():
            near = row - j <= near_of(j)

            @pl.when(near)
            def _():
                remote(tally, tally, y_send.at[0], y_recv.at[q], (j, col)).wait_recv()
                y = y_in[q, 0]
                for s in range(1, n_col):
                    y = y + y_in[q, s]
                y_full[...] = y

            @pl.when(jnp.logical_not(near))
            def _():
                remote(y_in.at[q, 0], y_in.at[q, 0], y_send.at[0], y_recv.at[q], (j, col)).wait_recv()
                y_full[...] = y_in[q, 0]

            y = y_full[...].astype(jnp.bfloat16)

            @pl.when(takes & (j == theirs))
            def _():
                wl_out[...] = jnp.dot(y, d_tile[...], preferred_element_type=jnp.float32)
                @pl.when(jnp.logical_not(is_ahead))
                def _():
                    for s in range(n_col):
                        remote(wl_out, wl_in, wl_send, wl_recv, (row - 1, s)).start()

                @pl.when(is_end | is_ahead)
                def _():
                    for peer in peers:
                        remote(wl_out, wl_in, wp_send, wl_recv, (row, peer)).start()
                    wl_in[...] = wl_out[...]

            @pl.when(takes_whole & (j == whole))
            def _():
                w2_out[...] = jnp.dot(y, d_tile[...], preferred_element_type=jnp.float32)
                for s in range(n_col):
                    remote(w2_out, w2_in, wl_send, p_recv.at[whole], (row - 1, s)).start()
                for peer in peers:
                    remote(w2_out, w2_in, wp_send, x_recv.at[0], (row, peer)).start()
                w2_in[...] = w2_out[...]

            inner = jnp.dot(y, vt_ref[q], preferred_element_type=jnp.float32)
            keep = lax.broadcasted_iota(jnp.int32, (nrhs, rank_max), 1) < rank_ref[q]
            inner = jnp.where(keep, inner, 0.0).astype(jnp.bfloat16)
            p = jnp.dot(inner, u_ref[q], preferred_element_type=jnp.float32)
            for s in range(n_col):
                p_out[q, s] = p[:, s * piece:(s + 1) * piece]
            for peer in peers:
                remote(p_out.at[q, peer], p_in.at[j], p_send.at[q], p_recv.at[j], (row, peer)).start()
            p_in[j] = p_out[q, col]

    def products():
        fold_with(v_in, v_recv, fold)
        factor = fold[...].astype(jnp.bfloat16)
        shared_wait(u_in, u_recv, prev_home)
        shared_wait(l_in, k_recv, mine_home)
        a_out[0] = jnp.dot(u_in[...].astype(jnp.bfloat16), factor, preferred_element_type=jnp.float32)
        a_out[1] = jnp.dot(l_in[...].astype(jnp.bfloat16), factor, preferred_element_type=jnp.float32)
        shared_wait(l2_in, du_recv, whole_home)
        a_out[2] = jnp.dot(l2_in[...].astype(jnp.bfloat16), factor, preferred_element_type=jnp.float32)
        for k in range(3):
            for s in range(n_col):
                remote(a_out.at[k], a_in.at[k, col], a_send, a_recv, (row + 1, s)).start()

    @pl.when(relays_late)
    def _():
        products()
        relay(v_out, v_in, v_recv, row - 1, prev_home)

    @pl.when(takes | takes_whole)
    def _():
        remote(d_in, d_in, d_send, d_recv, (row - 1, col)).wait_recv()
        d_tile[...] = d_in[...].T.astype(jnp.bfloat16)

    @pl.when(is_end & (col != far_home))
    def _():
        relay(x_out, x_in, x_recv, row - 2, far_home)

    for q in range(per_col):
        long_step(q, jnp.logical_not(is_ahead & (q * n_col + col == row - 2)))

    def pass_on(i, carry):
        remote(y_full, y_in.at[0, 0], pass_send, y_recv.at[0], (i, 0)).start()
        return carry

    @pl.when(passes)
    def _():
        pl.semaphore_wait(ready, answers)
        lax.fori_loop(2, 4, pass_on, 0)

    def send_w(out, into, send, recv, i):
        for s in range(n_col):
            remote(out, into.at[col], send, recv, (i, s)).start()

    def wait_w(into, send, recv, i):
        remote(into, into, send, recv, (i, 0)).wait_recv()
        total = into[0]
        for s in range(1, n_col):
            total = total + into[s]
        return total

    def borrowed_y(c):
        tail = tail_of(c)
        slot = (ahead - 1) // n_col
        home = (ahead - 1) % n_col
        return remote(hy_out.at[:, tail], y_in.at[slot, c, :, tail], y_send.at[0], y_recv.at[slot], (end, home))

    @pl.when(is_ahead)
    def _():
        back = (row - 1, col)
        by_col(lambda c: remote(hv_in.at[:, tail_of(c)], hv_in.at[:, tail_of(c)], wl_send, wx_recv, back).wait_recv())
        by_col(lambda c: hv_tile.__setitem__((slice(None), tail_of(c)), hv_in[:, tail_of(c)].astype(jnp.bfloat16)))
        remote(hl_in, hl_in, a_send, k_recv, back).wait_recv()
        remote(hu_in, hu_in, we_send, a_recv, back).wait_recv()
        remote(hf_in, hf_in, wx_send, we_recv, back).wait_recv()
        remote(hb_in, hb_in, wp_send, t_recv, back).wait_recv()
        l_part = hl_in[...].astype(jnp.bfloat16)
        u_part = hu_in[...].astype(jnp.bfloat16)
        factor = hf_in[...].astype(jnp.bfloat16)

        @pl.when(answers > 0)
        def _():
            pl.semaphore_wait(ready, answers)

        @pl.when(jnp.logical_not(takes))
        def _():
            remote(wl_in, wl_in, wp_send, wl_recv, (row, their_home)).wait_recv()

        part = hb_in[...] - jnp.dot(wl_in[...].astype(jnp.bfloat16), l_part, preferred_element_type=jnp.float32)
        inner = wait_w(hw_in, w_send, du_recv, row - 2)
        part -= jnp.dot(inner.astype(jnp.bfloat16), u_part, preferred_element_type=jnp.float32)
        part = part.astype(jnp.bfloat16)
        hw_out[...] = jnp.dot(part, factor, preferred_element_type=jnp.float32)
        for peer in peers:
            remote(hw_out, w_in.at[col], a_send, w_recv, (row, peer)).start()
        w_in[col] = hw_out[...]

        def borrowed_part(c):
            tail = tail_of(c)
            hy_out[:, tail] = jnp.dot(part, hv_tile[:, tail], preferred_element_type=jnp.float32)
            borrowed_y(c).start()

        by_col(borrowed_part)
        hz_out[...] = part.astype(jnp.float32)
        remote(hz_out, hz_in, wl_send, du_recv, back).start()

    for q in range(per_col):
        long_step(q, is_ahead & (q * n_col + col == row - 2))

    pl.when(is_even_end & jnp.logical_not(relays_late))(products)

    @pl.when(feeds & jnp.logical_not(is_even_end))
    def _():
        fold_with(v_in, v_recv, fold)

        @pl.when(lent)
        def _():
            lend(fold, hf_in, wx_send, we_recv).start()

    @pl.when(gives_far)
    def _():
        spread_late(x_out, x_in, x_recv, row - 2, far_home)
        share(t_out, t_in, t_recv)

    @pl.when(is_ahead)
    def _():
        fold_with(x_in, x_recv, fold_x)

    @pl.when(is_end)
    def _():
        remote(a_in, a_in, a_send, a_recv, (row - 1, 0)).wait_recv()
        for k in range(3):
            total = a_in[k, 0]
            for s in range(1, n_col):
                total = total + a_in[k, s]
            a_sum[k] = total.astype(jnp.bfloat16)

    def gather_p(j, acc):
        home = lax.rem(j, n_col)

        @pl.when(home != col)
        def _():
            remote(p_in.at[j], p_in.at[j], p_send.at[0], p_recv.at[j], (row, home)).wait_recv()

        return acc - p_in[j]

    base[...] = lax.fori_loop(0, long_count, gather_p, base[...])

    @pl.when(lent)
    def _():
        hb_out[...] = base[...]
        lend(hb_out, hb_in, wp_send, t_recv).start()
        shared_wait(l_in, k_recv, mine_home)
        lend(l_in, hl_in, a_send, k_recv).start()
        shared_wait(u_in, u_recv, prev_home)
        lend(u_in, hu_in, we_send, a_recv).start()
        remote(hz_in, hz_in, wl_send, du_recv, (row + 1, col)).wait_recv()
        base[...] = hz_in[...]

    @pl.when(is_even_end)
    def _():
        w_out[...] = jnp.dot(base[...].astype(jnp.bfloat16), fold[...].astype(jnp.bfloat16), preferred_element_type=jnp.float32)
        send_w(w_out, w_in, w_send, w_recv, row + 1)

    @pl.when(handed & jnp.logical_not(lent))
    def _():
        @pl.when(jnp.logical_not(is_even_end))
        def _():
            shared_wait(l_in, k_recv, mine_home)

        l_part = l_in[...].astype(jnp.bfloat16)

        @pl.when(is_even_end)
        def _():
            remote(w2_in, w2_in, wl_send, p_recv.at[whole], (row + 1, whole_home)).wait_recv()
            base[...] -= jnp.dot(
                w2_in[...].astype(jnp.bfloat16), l2_in[...].astype(jnp.bfloat16), preferred_element_type=jnp.float32
            )

        remote(wl_in, wl_in, wl_send, wl_recv, (row + 1, mine_home)).wait_recv()
        base[...] -= jnp.dot(wl_in[...].astype(jnp.bfloat16), l_part, preferred_element_type=jnp.float32)

    @pl.when(is_ahead)
    def _():
        shared_wait(u_in, u_recv, prev_home)
        u_part = u_in[...].astype(jnp.bfloat16)
        part = w_in.at[others]
        remote(part, part, a_send, w_recv, (row, peers[0])).wait_recv()
        inner = w_in[0]
        for s in range(1, n_col):
            inner = inner + w_in[s]
        base[...] -= jnp.dot(inner.astype(jnp.bfloat16), u_part, preferred_element_type=jnp.float32)

    @pl.when(short & jnp.logical_not(is_end | is_ahead | lent))
    def _():
        @pl.when(jnp.logical_not(is_even_end))
        def _():
            shared_wait(u_in, u_recv, prev_home)

        u_part = u_in[...].astype(jnp.bfloat16)
        inner = wait_w(w_in, w_send, w_recv, row - 1)
        base[...] -= jnp.dot(inner.astype(jnp.bfloat16), u_part, preferred_element_type=jnp.float32)

    @pl.when(is_end)
    def _():
        shared_wait(u_in, u_recv, prev_home)
        shared_wait(t_in, t_recv, far_home)
        u_part = u_in[...].astype(jnp.bfloat16)
        t_part = t_in[...].astype(jnp.bfloat16)

        @pl.when(jnp.logical_not(takes))
        def _():
            remote(wl_in, wl_in, wp_send, wl_recv, (row, their_home)).wait_recv()

        @pl.when(jnp.logical_not(takes_whole))
        def _():
            remote(w2_in, w2_in, wp_send, x_recv.at[0], (row, whole_home)).wait_recv()

        inner = wait_w(w_in, w_send, w_recv, row - 1)
        inner -= jnp.dot(w2_in[...].astype(jnp.bfloat16), a_sum[2], preferred_element_type=jnp.float32)
        inner -= jnp.dot(wl_in[...].astype(jnp.bfloat16), a_sum[1], preferred_element_type=jnp.float32)
        late = wait_w(wx_in, wx_send, wx_recv, row - 2)
        base[...] -= jnp.dot(late.astype(jnp.bfloat16), t_part, preferred_element_type=jnp.float32)
        late = wait_w(we_in, we_send, we_recv, row - 2)
        inner -= jnp.dot(late.astype(jnp.bfloat16), a_sum[0], preferred_element_type=jnp.float32)
        base[...] -= jnp.dot(inner.astype(jnp.bfloat16), u_part, preferred_element_type=jnp.float32)

    reduced = base[...].astype(jnp.bfloat16)

    @pl.when(jnp.logical_not(even | is_ahead | passes) & (answers > 0))
    def _():
        pl.semaphore_wait(ready, answers)

    @pl.when(feeds & jnp.logical_not(is_even_end | lent))
    def _():
        w_out[...] = jnp.dot(reduced, fold[...].astype(jnp.bfloat16), preferred_element_type=jnp.float32)

        @pl.when(is_ahead)
        def _():
            send_w(w_out, w_in, w_send, w_recv, row + 1)
            send_w(w_out, we_in, we_send, we_recv, row + 2)
            wx_out[...] = jnp.dot(reduced, fold_x[...].astype(jnp.bfloat16), preferred_element_type=jnp.float32)
            send_w(wx_out, wx_in, wx_send, wx_recv, row + 2)

        @pl.when(before)
        def _():
            send_w(w_out, hw_in, w_send, du_recv, row + 2)

        @pl.when(jnp.logical_not(before | is_ahead))
        def _():
            send_w(w_out, w_in, w_send, w_recv, row + 1)

    @pl.when(row > 0)
    def _():
        by_col(lambda c: own_part(c, reduced))

    def send_y(i, carry):
        @pl.when((row < longs_of(i)) & jnp.logical_not(lent))
        def _():
            by_col(lambda c: near_copy(i, c).start())

        return carry

    def own_copy(c, peer):
        part = y_row.at[c, :, tail_of(c)]
        return remote(part, part, o_send, o_recv, (row, peer))

    lax.fori_loop(row + 1, jnp.where(first, 0, near_end), send_y, 0)
    for peer in peers:
        by_col(lambda c: own_copy(c, peer).start())

    @pl.when(first)
    def _():
        log_part()

    remote(logs.at[others], logs.at[others], l_send, l_recv, (row, peers[0])).wait()
    log_sum = logs[0]
    for s in range(1, n_col):
        log_sum = log_sum + logs[s]
    log_term = log_sum * (1.0 / width) - 0.5 * math.log(2.0 * math.pi)

    def left_y(i, carry):
        @pl.when((row < longs_of(i)) & jnp.logical_not(lent))
        def _():
            by_col(lambda c: near_copy(i, c).wait_send())

        return carry

    lax.fori_loop(row + 1, near_end, left_y, 0)

    @pl.when(feeds & jnp.logical_not(lent))
    def _():
        remote(w_in, w_in, w_send, w_recv, (row + 1, 0)).wait_send()

    @pl.when(lent)
    def _():
        by_col(lambda c: lend_inverse(c).wait_send())
        lend(fold, hf_in, wx_send, we_recv).wait_send()
        lend(hb_out, hb_in, wp_send, t_recv).wait_send()
        lend(l_in, hl_in, a_send, k_recv).wait_send()
        lend(u_in, hu_in, we_send, a_recv).wait_send()

    @pl.when(is_ahead)
    def _():
        part = w_in.at[others]
        remote(part, part, a_send, w_recv, (row, peers[0])).wait_send()
        by_col(lambda c: borrowed_y(c).wait_send())
        remote(hz_out, hz_in, wl_send, du_recv, (row - 1, col)).wait_send()
        remote(w_in, w_in, we_send, we_recv, (row + 2, 0)).wait_send()
        remote(w_in, w_in, wx_send, wx_recv, (row + 2, 0)).wait_send()

    @pl.when(is_even_end)
    def _():
        remote(a_in, a_in, a_send, a_recv, (row + 1, 0)).wait_send()

    @pl.when(takes)
    def _():
        @pl.when(jnp.logical_not(is_ahead))
        def _():
            remote(w_in, w_in, wl_send, wl_recv, (row - 1, 0)).wait_send()

        @pl.when(is_end | is_ahead)
        def _():
            remote(w_in.at[others], w_in.at[others], wp_send, wl_recv, (row, peers[0])).wait_send()

    @pl.when(hands)
    def _():
        remote(d_out, d_in, d_send, d_recv, (row + 1, col)).wait_send()
        share_done(l_out)

    @pl.when(hands_whole)
    def _():
        remote(d_out, d_in, d_send, d_recv, (row + 1, col)).wait_send()
        share_done(l_out)

    @pl.when(takes_whole)
    def _():
        remote(w_in, w_in, wl_send, p_recv.at[0], (row - 1, 0)).wait_send()
        remote(w_in.at[others], w_in.at[others], wp_send, x_recv.at[0], (row, peers[0])).wait_send()

    @pl.when(gives)
    def _():
        spread_done(v_out, prev_home, crosses)
        share_done(u_out)

    @pl.when(gives_far)
    def _():
        spread_done(x_out, far_home, jnp.bool_(True))
        share_done(t_out)

    @pl.when(crosses & (col != prev_home))
    def _():
        relay_done(v_out, prev_home)

    @pl.when(is_end & (col != far_home))
    def _():
        relay_done(x_out, far_home)

    for q in range(per_col):

        @pl.when(q * n_col + col < long_count)
        def _():
            part = p_out.at[q, others]
            remote(part, part, p_send.at[q], p_recv.at[0], (row, peers[0])).wait_send()

    def wait_others(c):
        part = tally.at[pl.ds(0, tally.shape[0] - tail_of(c).size // 128)]
        remote(part, part, o_send, o_recv, (row, peers[0])).wait_recv()

    by_col(wait_others)
    y = y_row[0]
    for s in range(1, n_col):
        y = y + y_row[s]
    y_all[...] = y

    def far_copy(i):
        return remote(y_all, y_in.at[own_slot, 0], y_send.at[lax.rem(i - row - 1, y_sends)], y_recv.at[own_slot], (i, col))

    def send_far(i, carry):
        far_copy(i).start()
        return carry

    @pl.when(far_answers > 0)
    def _():
        pl.semaphore_wait(ready_far, far_answers)

    @pl.when(passes)
    def _():
        lax.fori_loop(4, n_row, pass_on, 0)
        part = y_in.at[:, pl.ds(0, (n_row - 2) // per_col)]
        remote(part, part, pass_send, y_recv.at[0], (2, 0)).wait_send()

    lax.fori_loop(jnp.where(relays, near_end, n_row), n_row, send_far, 0)
    white_ref[0, 0] = y
    quadratic = jnp.sum(y * y, axis=1, keepdims=True) * (1.0 / width)
    lik = -0.5 * quadratic + log_term
    r_id = lax.broadcasted_iota(jnp.int32, (nrhs, 128), 0)
    c_id = lax.broadcasted_iota(jnp.int32, (nrhs, 128), 1)
    flat = jnp.sum(jnp.where(r_id == c_id, lik, 0.0), axis=0, keepdims=True)
    lik_ref[0] = flat[:, :nrhs]

    def left_far(i, carry):
        far_copy(i).wait_send()
        return carry

    lax.fori_loop(jnp.where(relays, near_end, n_row), n_row, left_far, 0)

    def own_left(c):
        part = y_row.at[others, :, tail_of(c)]
        remote(part, part, o_send, o_recv, (row, peers[0])).wait_send()

    by_col(own_left)


def local(n_row, n_col, right_side, inverse_t, u_factor, v_factor, ranks):
    nrhs, width = right_side.shape[2:]
    per_col, _, rank_max = u_factor.shape[2:5]
    piece = width // n_col
    vmem = pl.BlockSpec(memory_space=pltpu.VMEM)
    hbm = pl.BlockSpec(memory_space=pl.ANY)
    dma = pltpu.SemaphoreType.DMA

    def f32(*shape):
        return pltpu.VMEM(shape, jnp.float32)

    def bf16(*shape):
        return pltpu.VMEM(shape, jnp.bfloat16)

    units = sum((width - c * piece // 128 * 128) // 128 for c in range(n_col))
    tile_set = [
        f32(n_col, rank_max, piece),
        f32(n_col, rank_max, piece),
        f32(n_col, rank_max, piece),
        f32(rank_max, piece),
        f32(piece, rank_max),
        f32(nrhs, rank_max),
        f32(n_col, nrhs, rank_max),
    ]
    return pl.pallas_call(
        functools.partial(kernel, n_row, n_col),
        out_shape=(
            pltpu.VMEM((1, 1, nrhs, width), jnp.float32),
            pltpu.VMEM((1, 1, nrhs), jnp.float32),
        ),
        in_specs=[hbm, hbm, hbm, hbm, hbm],
        out_specs=(vmem, vmem),
        scratch_shapes=[
            f32(nrhs, width),
            bf16(piece, width),
            bf16(per_col, rank_max, width),
            bf16(per_col, rank_max, width),
            pltpu.SMEM((per_col,), jnp.int32),
            f32(per_col, n_col, nrhs, width),
            f32(per_col, n_col, nrhs, piece),
            f32(n_row, nrhs, piece),
            f32(n_col, nrhs, width),
            f32(n_col, 1, 128),
            f32(nrhs, piece),
            f32(nrhs, width),
            f32(nrhs, width),
            f32(units, nrhs, 128),
            *tile_set,
            *tile_set,
            f32(rank_max, width),
            f32(rank_max, width),
            bf16(width, rank_max),
            bf16(per_col, width, rank_max),
            f32(rank_max, piece),
            f32(nrhs, rank_max),
            f32(nrhs, rank_max),
            f32(n_col, rank_max, piece),
            f32(rank_max, piece),
            f32(nrhs, rank_max),
            f32(nrhs, rank_max),
            f32(n_col, nrhs, rank_max),
            f32(3, rank_max, rank_max),
            f32(3, n_col, rank_max, rank_max),
            bf16(3, rank_max, rank_max),
            f32(rank_max, piece),
            f32(rank_max, piece),
            f32(piece, rank_max),
            f32(piece, width),
            f32(piece, width),
            bf16(piece, width),
            f32(nrhs, piece),
            f32(nrhs, piece),
            f32(nrhs, piece),
            f32(nrhs, piece),
            f32(nrhs, rank_max),
            f32(n_col, nrhs, rank_max),
            f32(nrhs, width),
            dma((5,)),
            dma((max(NEAR + 1, n_row - NEAR - 1),)),
            dma((per_col,)),
            dma((per_col,)),
            dma((n_row - 3,)),
            dma, dma, dma, dma,
            dma((n_col,)),
            dma((n_col,)),
            dma, dma, dma, dma,
            dma((n_col,)),
            dma, dma,
            pltpu.SemaphoreType.REGULAR,
            pltpu.SemaphoreType.REGULAR,
            dma,
            dma((n_col,)),
            dma, dma, dma, dma, dma,
            dma, dma, dma, dma, dma, dma, dma, dma, dma,
        ],
        compiler_params=pltpu.CompilerParams(collective_id=0, has_side_effects=True),
        name="forward_solve",
    )(right_side, inverse_t, u_factor, v_factor, ranks.reshape(per_col))


def solution(mesh):
    placed = (
        P(None, "row", None, None),
        P(None, "row", "col", None),
        P(None, "row", None, "col", None, None),
        P(None, "row", None, "col", None, None),
        P(None, "row", None, "col"),
    )
    return jax.shard_map(
        functools.partial(local, mesh.shape["row"], mesh.shape["col"]),
        mesh=mesh,
        in_specs=placed,
        out_specs=(P(None, "row", None, None), P(None, "row", None)),
        check_vma=False,
    )
```

```python
import functools
import math

import jax
import jax.numpy as jnp
from jax import lax
from jax.experimental import pallas as pl
from jax.experimental.pallas import tpu as pltpu
from jax.sharding import PartitionSpec as P

MESH = pl.DeviceIdType.MESH
NT = (((1,), (1,)), ((), ()))
FIRST_SHORT = 3
NEAR = 3


def remote(src, dst, send_sem, recv_sem, device):
    return pltpu.make_async_remote_copy(
        src_ref=src,
        dst_ref=dst,
        send_sem=send_sem,
        recv_sem=recv_sem,
        device_id=device,
        device_id_type=MESH,
    )


def kernel(
    n_row, n_col,
    rhs_hbm, inv_hbm, u_hbm, v_hbm, rank_hbm,
    white_ref, lik_ref,
    rhs_ref, inv_ref, u_ref, v_ref, rank_ref,
    y_in, p_out, p_in, y_row, logs, base, y_full, y_all, tally,
    v_out, v_in, u_out, u_in, fold, w_out, w_in,
    x_out, x_in, t_out, t_in, fold_x, wx_out, wx_in,
    d_out, d_in, d_tile, vt_ref, l2_in, w2_out, w2_in, l_out, l_in, wl_out, wl_in, we_in,
    a_out, a_in, a_sum,
    hl_in, hu_in, hf_in, hv_out, hv_in, hv_tile, hb_out, hb_in, hz_out, hz_in, hw_out, hw_in, hy_out,
    in_sem, y_send, y_recv, p_send, p_recv, o_send, o_recv, l_send, l_recv,
    v_send, v_recv, u_send, u_recv, w_send, w_recv, m_recv, f_send, e_send, ready, ready_far, pass_send,
    t_recv, k_recv, d_send, d_recv, du_recv, wl_send, wl_recv, wp_send,
    we_send, we_recv, wx_send, wm_recv, a_send, a_recv,
):
    row = lax.axis_index("row")
    col = lax.axis_index("col")
    per_col, rank_max, width = u_ref.shape
    nrhs = rhs_ref.shape[0]
    piece = width // n_col
    half = n_col // 2
    y_sends = y_send.shape[0]
    some = half
    peers = [lax.rem(col + k, n_col) for k in range(1, n_col)]
    others = pl.ds(0, n_col - 1)
    own_slot = row // n_col
    own_home = lax.rem(row, n_col)
    end = n_row - 1
    even_end = n_row - 2
    ahead = n_row - 3

    def longs_of(i):
        count = jnp.where(i >= FIRST_SHORT, i - 1, i)
        handed = (lax.rem(i, 2) == 0) & (i >= 2)
        return count - jnp.where(handed, 1, 0) - jnp.where(i >= even_end, 1, 0)

    def near_of(i):
        return jnp.where(i == 0, 1, NEAR + jnp.where(i >= 2, 1, 0))

    copies = [
        pltpu.make_async_copy(v_hbm.at[0, 0, :, 0], v_ref, in_sem.at[0]),
        pltpu.make_async_copy(u_hbm.at[0, 0, :, 0], u_ref, in_sem.at[1]),
        None,
        pltpu.make_async_copy(rhs_hbm.at[0, 0], rhs_ref, in_sem.at[3]),
        pltpu.make_async_copy(rank_hbm, rank_ref, in_sem.at[4]),
    ]
    @pl.when(lax.axis_index("row") > 0)
    def _():
        copies[0].start()
        copies[1].start()

    def tail_of(c):
        start = c * piece // 128 * 128
        return pl.ds(start, width - start)

    def inverse_copy(c):
        return pltpu.make_async_copy(inv_hbm.at[0, 0, :, tail_of(c)], inv_ref.at[:, tail_of(c)], in_sem.at[2])

    def by_col(act):
        for c in range(n_col):
            pl.when(col == c)(functools.partial(act, c))

    by_col(lambda c: inverse_copy(c).start())
    for copy in copies[3:]:
        copy.start()
    barrier = pltpu.get_barrier_semaphore()

    def signal(sem, i, s):
        pl.semaphore_signal(sem, inc=1, device_id=(i, s), device_id_type=MESH)

    for peer in peers:
        signal(barrier, row, peer)

    def set_base():
        for cc in range(n_col):

            @pl.when(col == cc)
            def _():
                base[...] = rhs_ref[:, cc * piece:(cc + 1) * piece]

    def own_part(c, reduced):
        tail = tail_of(c)
        y_row[c, :, tail] = jnp.dot(reduced, inv_ref[:, tail], preferred_element_type=jnp.float32)

    def near_copy(i, c):
        tail = tail_of(c)
        sem = y_send.at[lax.rem(i - row - 1, y_sends)]
        return remote(y_row.at[c, :, tail], y_in.at[own_slot, c, :, tail], sem, y_recv.at[own_slot], (i, own_home))

    first = row == 0

    @pl.when(first)
    def _():
        for s in range(n_col):
            signal(barrier, 1, s)
        copies[3].wait()
        by_col(lambda c: inverse_copy(c).wait())
        set_base()
        reduced = base[...].astype(jnp.bfloat16)
        by_col(lambda c: own_part(c, reduced))
        pl.semaphore_wait(barrier, 2 * n_col - 1)
        by_col(lambda c: near_copy(1, c).start())

    for s in range(1, n_col):
        start = s * piece // 128 * 128
        if start:
            y_row[s, :, :start] = jnp.zeros((nrhs, start), jnp.float32)
            for q in range(per_col):
                y_in[q, s, :, :start] = jnp.zeros((nrhs, start), jnp.float32)

    even = lax.rem(row, 2) == 0
    short = row >= FIRST_SHORT
    feeds = (row + 1 >= FIRST_SHORT) & (row < end)
    is_end = row == end
    is_even_end = row == even_end
    is_ahead = row == ahead
    lent = row == ahead - 1
    before = row == ahead - 2
    long_count = longs_of(row)
    near_end = jnp.minimum(row + near_of(row) + 1, n_row)
    relays = (col == own_home) & (row > 0)
    passes = (row == 1) & (col == 0)

    def row_of(i, cond, act):
        @pl.when(cond)
        def _():
            for s in range(n_col):
                act(i, s)

        return jnp.where(cond, n_col, 0)

    def above(act):
        yield row + 1, row_of(row + 1, (row > 0) & (row < end), act)
        for d in range(2, NEAR + 2):
            wide = (is_ahead | before) if d == 2 else jnp.bool_(False)
            one = (row + d < n_row) & (d <= near_of(row)) & jnp.logical_not(wide)

            @pl.when(one)
            def _():
                act(row + d, own_home)

            yield row + d, jnp.where(one, 1, 0)
            if d == 2:
                yield row + d, row_of(row + d, wide, act)

    def below(act, act_far=None):
        row_of(row - 1, row > 0, act)
        count = jnp.where(row > 0, n_col, 0)
        for d in range(2, NEAR + 2):
            fed = (row >= d) & (d <= near_of(row - d)) & (lax.rem(jnp.maximum(row - d, 0), n_col) == col)
            if d == 2:
                fed = fed | is_end | is_ahead
            count += row_of(row - d, fed, act)
        for q in range(per_col):
            j = q * n_col + col
            far = j < row - near_of(j)

            source = jnp.where(j == 0, 1, j)
            soon = (j == 0) & (row <= 3)

            @pl.when(far & soon)
            def _():
                act(source, col)

            @pl.when(far & jnp.logical_not(soon))
            def _():
                (act_far or act)(source, col)

            count += jnp.where(far, 1, 0)
        return count

    def at_once(low, high):
        return (low == 0) & (high == 1)

    greeted = jnp.int32(n_col - 1)
    answers = jnp.int32(0)
    for i, count in above(lambda i, s: signal(barrier, i, s)):
        answers += count

    def greet_far(i, count):
        signal(barrier, i, col)
        return count + 1

    far_answers = lax.fori_loop(jnp.where(relays, near_end, n_row), n_row, greet_far, jnp.int32(0))
    far_answers = lax.fori_loop(jnp.where(passes, 4, n_row), n_row, greet_far, far_answers)
    answers = lax.fori_loop(jnp.where(passes, 2, n_row), jnp.where(passes, 4, n_row), greet_far, answers)

    def greet_quick(i, s):
        @pl.when(at_once(i, row))
        def _():
            signal(barrier, i, s)

    def answer(i, s):
        @pl.when(jnp.logical_not(at_once(i, row)))
        def _():
            signal(ready, i, s)

    greeted += below(greet_quick)

    prev = jnp.maximum(row - 1, 0)
    prev_slot = prev // n_col
    prev_home = lax.rem(prev, n_col)
    gives = short & (col == prev_home)
    crosses = short & even
    far_slot = ahead // n_col
    far_home = ahead % n_col
    gives_far = is_end & (col == far_home)
    handed = even & (row >= 2)
    mine = jnp.where(handed, long_count + jnp.where(is_even_end, 1, 0), 0)
    mine_slot = mine // n_col
    mine_home = lax.rem(mine, n_col)
    hands = handed & (col == mine_home)
    taken = (row >= 3) & jnp.logical_not(even)
    theirs = jnp.where(taken, longs_of(prev) + jnp.where(is_end, 1, 0), 0)
    their_home = lax.rem(theirs, n_col)
    takes = taken & (col == their_home)
    whole = even_end - 3
    whole_slot = whole // n_col
    whole_home = whole % n_col
    hands_whole = is_even_end & (col == whole_home)
    takes_whole = is_end & (col == whole_home)

    def masked_u(slot):
        keep = lax.broadcasted_iota(jnp.int32, (rank_max, width), 0) < rank_ref[slot]
        return jnp.where(keep, u_ref[slot].astype(jnp.float32), 0.0)

    def cut(tile, into):
        for s in range(n_col):
            into[s] = tile[:, s * piece:(s + 1) * piece]

    @pl.when(row > 0)
    def _():
        copies[0].wait()
        copies[1].wait()

    copies[4].wait()

    @pl.when(hands)
    def _():
        d_out[...] = v_ref[mine_slot].astype(jnp.float32)
        cut(masked_u(mine_slot), l_out)

    @pl.when(hands_whole)
    def _():
        d_out[...] = v_ref[whole_slot].astype(jnp.float32)
        cut(masked_u(whole_slot), l_out)

    @pl.when(gives)
    def _():
        cut(v_ref[prev_slot].astype(jnp.float32), v_out)
        cut(masked_u(prev_slot), u_out)

    @pl.when(gives_far)
    def _():
        cut(v_ref[far_slot].astype(jnp.float32), x_out)
        cut(masked_u(far_slot), t_out)

    @pl.when(row > 0)
    def _():
        pl.semaphore_wait(barrier, greeted)

    below(answer, lambda i, s: signal(ready_far, i, s))

    def by_way(home, s, cc):
        across = n_col - 1 - home
        return (home != s) & jnp.where(
            across < home,
            jnp.where(across == s, cc < s + some, (home != s + 1) | (cc == s)),
            (s > home) | (cc < s + half),
        )

    def is_late(home, s, cc):
        across = n_col - 1 - home
        return (across == s) & (across < home) & (cc >= s + some)

    def beside(home, s):
        return split_row(home) & (home == s + 1) & (n_col - 1 - home != s)

    def split_row(home):
        return n_col - 1 - home < home

    def is_split(home, s):
        across = n_col - 1 - home
        return (across == s) & (across < home)

    def joined(home, s):
        across = n_col - 1 - home
        return (across > home) & (across == s)

    def spread(out, into, recv, target, home, cross):
        for s in range(n_col):
            for cc in range(s, min(s + some, n_col)):

                @pl.when(cross & is_split(home, s))
                def _():
                    remote(out.at[cc], out.at[cc], v_send.at[s], m_recv.at[cc], (row, s)).start()

        for s in range(n_col):
            if s > 0:

                @pl.when(cross & joined(home, s - 1))
                def _():
                    remote(out.at[s - 1], out.at[s - 1], v_send.at[s], m_recv.at[s - 1], (row, s)).start()

            for cc in range(s, n_col):
                gone = cross & (joined(home, s) | is_split(home, s))
                way = cross & by_way(home, s, cc)
                later = cross & is_late(home, s, cc)

                @pl.when(way & jnp.logical_not(gone))
                def _():
                    remote(out.at[cc], out.at[cc], v_send.at[s], m_recv.at[cc], (row, s)).start()

                @pl.when(jnp.logical_not(way | later | gone))
                def _():
                    remote(out.at[cc], into.at[cc], v_send.at[s], recv.at[cc], (target, s)).start()

    def spread_late(out, into, recv, target, home):
        for s in range(n_col):

            @pl.when(split_row(home) & (n_col - home == s))
            def _():
                part = pl.ds(s, n_col - s)
                remote(out.at[part], out.at[part], v_send.at[s], m_recv.at[0], (row, s)).wait_send()

        for s in range(n_col):
            for cc in range(min(s + some, n_col), n_col):

                @pl.when(is_late(home, s, cc))
                def _():
                    remote(out.at[cc], into.at[cc], v_send.at[s], recv.at[cc], (target, s)).start()

    def spread_done(out, home, cross):
        for s in range(n_col):
            part = pl.ds(s, n_col - s)
            gone = cross & joined(home, s)
            gone = gone | (cross & split_row(home) & (n_col - home == s))
            more = (cross & joined(home, s - 1)) if s > 0 else jnp.bool_(False)

            @pl.when(jnp.logical_not(gone | more))
            def _():
                remote(out.at[part], out.at[part], v_send.at[s], m_recv.at[0], (row, s)).wait_send()

            if s > 0:
                part_more = pl.ds(s - 1, n_col - s + 1)

                @pl.when(more)
                def _():
                    remote(out.at[part_more], out.at[part_more], v_send.at[s], m_recv.at[0], (row, s)).wait_send()

    def relay(out, into, recv, target, home):
        across = n_col - 1 - home
        more = joined(home, col - 1)
        first = jnp.where(more, col - 1, col)
        part = jnp.where(across < home, across == col, col < home)
        share_of = jnp.where(across < home, some, half)
        stop = jnp.where(part, jnp.minimum(col + share_of, n_col), n_col)
        stop = jnp.where(joined(home, col) | beside(home, col), col + 1, stop)

        def forward(cc, carry):
            remote(out.at[cc], out.at[cc], v_send.at[0], m_recv.at[cc], (row, home)).wait_recv()

            @pl.when(cc >= col)
            def _():
                remote(out.at[cc], into.at[cc], f_send, recv.at[cc], (target, col)).start()

            @pl.when(more & (cc == across))
            def _():
                remote(out.at[cc], out.at[cc], e_send, m_recv.at[cc], (row, across)).start()

            @pl.when(more & (cc > across))
            def _():
                remote(out.at[cc], into.at[cc], e_send, recv.at[cc], (target, across)).start()

            return carry

        lax.fori_loop(first, stop, forward, 0)

    def relay_done(out, home):
        across = n_col - 1 - home
        for cc in range(n_col):
            here = col == cc
            half_way = jnp.where(across < home, across == cc, cc < home)

            @pl.when(here & (joined(home, cc) | beside(home, cc)))
            def _():
                remote(out.at[cc], out.at[cc], f_send, v_recv.at[0], (row, home)).wait_send()

            @pl.when(here & jnp.logical_not(half_way | joined(home, cc) | beside(home, cc)))
            def _():
                part = pl.ds(cc, n_col - cc)
                remote(out.at[part], out.at[part], f_send, v_recv.at[0], (row, home)).wait_send()

            for count, cond in ((some, across < home), (half, across > home)):
                few = pl.ds(cc, min(count, n_col - cc))

                @pl.when(here & half_way & cond)
                def _():
                    remote(out.at[few], out.at[few], f_send, v_recv.at[0], (row, home)).wait_send()

            if cc > 0:

                @pl.when((col == cc) & joined(home, cc - 1))
                def _():
                    part = pl.ds(cc - 1, n_col - cc + 1)
                    remote(out.at[part], out.at[part], e_send, v_recv.at[0], (row, home)).wait_send()

    def share(out, into, recv):
        for k in range(n_col):
            peer = lax.rem(2 * n_col - 1 - col + k, n_col)

            @pl.when(peer != col)
            def _():
                remote(out.at[peer], into, u_send, recv, (row, peer)).start()

        into[...] = out[col]

    def share_done(out):
        remote(out.at[others], out.at[others], u_send, u_recv, (row, peers[0])).wait_send()

    def shared_wait(into, recv, home):
        @pl.when(col != home)
        def _():
            remote(into, into, u_send, recv, (row, home)).wait_recv()

    early_l = (row < FIRST_SHORT) | is_even_end

    opposite = n_col - 1 - col

    @pl.when(hands)
    def _():
        for peer in peers:

            @pl.when(early_l | (peer != opposite))
            def _():
                remote(l_out.at[peer], l_in, u_send, k_recv, (row, peer)).start()

        l_in[...] = l_out[col]

    @pl.when(hands_whole)
    def _():
        share(l_out, l2_in, du_recv)

    @pl.when(gives)
    def _():
        spread(v_out, v_in, v_recv, row - 1, prev_home, crosses)

    @pl.when(gives & (is_even_end | jnp.logical_not(even)))
    def _():
        share(u_out, u_in, u_recv)

    @pl.when(gives_far)
    def _():
        spread(x_out, x_in, m_recv, row - 2, far_home, jnp.bool_(True))

    @pl.when((handed) & (answers > 0))
    def _():
        pl.semaphore_wait(ready, answers)

    @pl.when(hands | hands_whole)
    def _():
        remote(d_out, d_in, d_send, d_recv, (row + 1, col)).start()

    relays_late = is_even_end & joined(prev_home, col)

    @pl.when(crosses & (col != prev_home) & jnp.logical_not(relays_late))
    def _():
        relay(v_out, v_in, v_recv, row - 1, prev_home)

    @pl.when(row > 0)
    def _():
        by_col(lambda c: inverse_copy(c).wait())
        copies[3].wait()


    def lend(src, dst, send, recv):
        return remote(src, dst, send, recv, (row + 1, col))

    def lend_inverse(c):
        return lend(hv_out.at[:, tail_of(c)], hv_in.at[:, tail_of(c)], wl_send, wm_recv)

    def lend_tail(c):
        hv_out[:, tail_of(c)] = inv_ref[:, tail_of(c)].astype(jnp.float32)
        lend_inverse(c).start()

    pl.when(lent)(functools.partial(by_col, lend_tail))

    pl.when(row > 0)(set_base)

    def log_part():
        for cc in range(n_col):

            @pl.when(col == cc)
            def _():
                block = inv_ref[:, cc * piece:(cc + 1) * piece].astype(jnp.float32)
                r_id = lax.broadcasted_iota(jnp.int32, (piece, piece), 0)
                c_id = lax.broadcasted_iota(jnp.int32, (piece, piece), 1)
                diagonal = jnp.sum(jnp.where(r_id == c_id, block, 0.0), axis=0, keepdims=True)
                total = jnp.sum(jnp.log(diagonal), axis=1, keepdims=True)
                logs[cc] = jnp.broadcast_to(total, (1, 128))

        for peer in peers:
            remote(logs.at[col], logs.at[col], l_send, l_recv, (row, peer)).start()

    pl.when(row > 0)(log_part)

    for q in range(per_col):

        @pl.when(q * n_col + col < long_count)
        def _():
            vt_ref[q] = v_ref[q].astype(jnp.float32).T.astype(jnp.bfloat16)

    @pl.when(gives & crosses)
    def _():
        spread_late(v_out, v_in, v_recv, row - 1, prev_home)

    @pl.when(gives & crosses & jnp.logical_not(is_even_end))
    def _():
        share(u_out, u_in, u_recv)

    @pl.when(hands & jnp.logical_not(early_l))
    def _():
        remote(l_out.at[opposite], l_in, u_send, k_recv, (row, opposite)).start()

    def fold_with(into, recv, target):
        target[...] = jnp.zeros_like(target)
        for cc in range(n_col):

            @pl.when(col <= cc)
            def _():
                remote(into.at[cc], into.at[cc], f_send, recv.at[cc], (row, cc)).wait_recv()
                target[...] += lax.dot_general(
                    inv_ref[:, cc * piece:(cc + 1) * piece],
                    into[cc].astype(jnp.bfloat16),
                    NT,
                    preferred_element_type=jnp.float32,
                )

    def long_step(q, cond):
        j = q * n_col + col

        @pl.when((j < long_count) & cond)
        def _():
            near = row - j <= near_of(j)

            @pl.when(near)
            def _():
                remote(tally, tally, y_send.at[0], y_recv.at[q], (j, col)).wait_recv()
                y = y_in[q, 0]
                for s in range(1, n_col):
                    y = y + y_in[q, s]
                y_full[...] = y

            @pl.when(jnp.logical_not(near))
            def _():
                remote(y_in.at[q, 0], y_in.at[q, 0], y_send.at[0], y_recv.at[q], (j, col)).wait_recv()
                y_full[...] = y_in[q, 0]

            y = y_full[...].astype(jnp.bfloat16)

            @pl.when(takes & (j == theirs))
            def _():
                wl_out[...] = jnp.dot(y, d_tile[...], preferred_element_type=jnp.float32)
                @pl.when(jnp.logical_not(is_ahead))
                def _():
                    for s in range(n_col):
                        remote(wl_out, wl_in, wl_send, wl_recv, (row - 1, s)).start()

                @pl.when(is_end | is_ahead)
                def _():
                    for peer in peers:
                        remote(wl_out, wl_in, wp_send, wl_recv, (row, peer)).start()
                    wl_in[...] = wl_out[...]

            @pl.when(takes_whole & (j == whole))
            def _():
                w2_out[...] = jnp.dot(y, d_tile[...], preferred_element_type=jnp.float32)
                for s in range(n_col):
                    remote(w2_out, w2_in, wl_send, p_recv.at[whole], (row - 1, s)).start()
                for peer in peers:
                    remote(w2_out, w2_in, wp_send, k_recv, (row, peer)).start()
                w2_in[...] = w2_out[...]

            inner = jnp.dot(y, vt_ref[q], preferred_element_type=jnp.float32)
            keep = lax.broadcasted_iota(jnp.int32, (nrhs, rank_max), 1) < rank_ref[q]
            inner = jnp.where(keep, inner, 0.0).astype(jnp.bfloat16)
            p = jnp.dot(inner, u_ref[q], preferred_element_type=jnp.float32)
            for s in range(n_col):
                p_out[q, s] = p[:, s * piece:(s + 1) * piece]
            for peer in peers:
                remote(p_out.at[q, peer], p_in.at[j], p_send.at[q], p_recv.at[j], (row, peer)).start()
            p_in[j] = p_out[q, col]

    def products():
        fold_with(v_in, v_recv, fold)
        factor = fold[...].astype(jnp.bfloat16)
        shared_wait(u_in, u_recv, prev_home)
        shared_wait(l_in, k_recv, mine_home)
        a_out[0] = jnp.dot(u_in[...].astype(jnp.bfloat16), factor, preferred_element_type=jnp.float32)
        a_out[1] = jnp.dot(l_in[...].astype(jnp.bfloat16), factor, preferred_element_type=jnp.float32)
        shared_wait(l2_in, du_recv, whole_home)
        a_out[2] = jnp.dot(l2_in[...].astype(jnp.bfloat16), factor, preferred_element_type=jnp.float32)
        for k in range(3):
            for s in range(n_col):
                remote(a_out.at[k], a_in.at[k, col], a_send, a_recv, (row + 1, s)).start()

    @pl.when(relays_late)
    def _():
        products()
        relay(v_out, v_in, v_recv, row - 1, prev_home)

    @pl.when(takes | takes_whole)
    def _():
        remote(d_in, d_in, d_send, d_recv, (row - 1, col)).wait_recv()
        d_tile[...] = d_in[...].T.astype(jnp.bfloat16)

    @pl.when(is_end & (col != far_home))
    def _():
        relay(x_out, x_in, m_recv, row - 2, far_home)

    for q in range(per_col):
        long_step(q, jnp.logical_not(is_ahead & (q * n_col + col == row - 2)))

    def pass_on(i, carry):
        remote(y_full, y_in.at[0, 0], pass_send, y_recv.at[0], (i, 0)).start()
        return carry

    @pl.when(passes)
    def _():
        pl.semaphore_wait(ready, answers)
        lax.fori_loop(2, 4, pass_on, 0)

    def send_w(out, into, send, recv, i):
        for s in range(n_col):
            remote(out, into.at[col], send, recv, (i, s)).start()

    def wait_w(into, send, recv, i):
        remote(into, into, send, recv, (i, 0)).wait_recv()
        total = into[0]
        for s in range(1, n_col):
            total = total + into[s]
        return total

    def borrowed_y(c):
        tail = tail_of(c)
        slot = (ahead - 1) // n_col
        home = (ahead - 1) % n_col
        return remote(hy_out.at[:, tail], y_in.at[slot, c, :, tail], y_send.at[0], y_recv.at[slot], (end, home))

    @pl.when(is_ahead)
    def _():
        back = (row - 1, col)
        by_col(lambda c: remote(hv_in.at[:, tail_of(c)], hv_in.at[:, tail_of(c)], wl_send, wm_recv, back).wait_recv())
        by_col(lambda c: hv_tile.__setitem__((slice(None), tail_of(c)), hv_in[:, tail_of(c)].astype(jnp.bfloat16)))
        remote(hl_in, hl_in, a_send, k_recv, back).wait_recv()
        remote(hu_in, hu_in, we_send, a_recv, back).wait_recv()
        remote(hf_in, hf_in, wx_send, we_recv, back).wait_recv()
        remote(hb_in, hb_in, wp_send, t_recv, back).wait_recv()
        l_part = hl_in[...].astype(jnp.bfloat16)
        u_part = hu_in[...].astype(jnp.bfloat16)
        factor = hf_in[...].astype(jnp.bfloat16)

        @pl.when(answers > 0)
        def _():
            pl.semaphore_wait(ready, answers)

        @pl.when(jnp.logical_not(takes))
        def _():
            remote(wl_in, wl_in, wp_send, wl_recv, (row, their_home)).wait_recv()

        part = hb_in[...] - jnp.dot(wl_in[...].astype(jnp.bfloat16), l_part, preferred_element_type=jnp.float32)
        inner = wait_w(hw_in, w_send, du_recv, row - 2)
        part -= jnp.dot(inner.astype(jnp.bfloat16), u_part, preferred_element_type=jnp.float32)
        part = part.astype(jnp.bfloat16)
        def borrowed_part(c):
            tail = tail_of(c)
            hy_out[:, tail] = jnp.dot(part, hv_tile[:, tail], preferred_element_type=jnp.float32)
            borrowed_y(c).start()

        by_col(borrowed_part)
        hw_out[...] = jnp.dot(part, factor, preferred_element_type=jnp.float32)
        for peer in peers:
            remote(hw_out, w_in.at[col], a_send, w_recv, (row, peer)).start()
        w_in[col] = hw_out[...]

        hz_out[...] = part.astype(jnp.float32)
        remote(hz_out, hz_in, wl_send, du_recv, back).start()

    for q in range(per_col):
        long_step(q, is_ahead & (q * n_col + col == row - 2))

    pl.when(is_even_end & jnp.logical_not(relays_late))(products)

    @pl.when(feeds & jnp.logical_not(is_even_end))
    def _():
        fold_with(v_in, v_recv, fold)

        @pl.when(lent)
        def _():
            lend(fold, hf_in, wx_send, we_recv).start()

    @pl.when(gives_far)
    def _():
        spread_late(x_out, x_in, m_recv, row - 2, far_home)
        share(t_out, t_in, t_recv)

    @pl.when(is_ahead)
    def _():
        fold_with(x_in, m_recv, fold_x)

    @pl.when(is_end)
    def _():
        remote(a_in, a_in, a_send, a_recv, (row - 1, 0)).wait_recv()
        for k in range(3):
            total = a_in[k, 0]
            for s in range(1, n_col):
                total = total + a_in[k, s]
            a_sum[k] = total.astype(jnp.bfloat16)

    def gather_p(j, acc):
        home = lax.rem(j, n_col)

        @pl.when(home != col)
        def _():
            remote(p_in.at[j], p_in.at[j], p_send.at[0], p_recv.at[j], (row, home)).wait_recv()

        return acc - p_in[j]

    base[...] = lax.fori_loop(0, long_count, gather_p, base[...])

    @pl.when(lent)
    def _():
        hb_out[...] = base[...]
        lend(hb_out, hb_in, wp_send, t_recv).start()
        shared_wait(l_in, k_recv, mine_home)
        lend(l_in, hl_in, a_send, k_recv).start()
        shared_wait(u_in, u_recv, prev_home)
        lend(u_in, hu_in, we_send, a_recv).start()
        remote(hz_in, hz_in, wl_send, du_recv, (row + 1, col)).wait_recv()
        base[...] = hz_in[...]

    @pl.when(is_even_end)
    def _():
        w_out[...] = jnp.dot(base[...].astype(jnp.bfloat16), fold[...].astype(jnp.bfloat16), preferred_element_type=jnp.float32)
        send_w(w_out, w_in, w_send, w_recv, row + 1)

    @pl.when(handed & jnp.logical_not(lent))
    def _():
        @pl.when(jnp.logical_not(is_even_end))
        def _():
            shared_wait(l_in, k_recv, mine_home)

        l_part = l_in[...].astype(jnp.bfloat16)

        @pl.when(is_even_end)
        def _():
            remote(w2_in, w2_in, wl_send, p_recv.at[whole], (row + 1, whole_home)).wait_recv()
            base[...] -= jnp.dot(
                w2_in[...].astype(jnp.bfloat16), l2_in[...].astype(jnp.bfloat16), preferred_element_type=jnp.float32
            )

        remote(wl_in, wl_in, wl_send, wl_recv, (row + 1, mine_home)).wait_recv()
        base[...] -= jnp.dot(wl_in[...].astype(jnp.bfloat16), l_part, preferred_element_type=jnp.float32)

    @pl.when(is_ahead)
    def _():
        shared_wait(u_in, u_recv, prev_home)
        u_part = u_in[...].astype(jnp.bfloat16)
        part = w_in.at[others]
        remote(part, part, a_send, w_recv, (row, peers[0])).wait_recv()
        inner = w_in[0]
        for s in range(1, n_col):
            inner = inner + w_in[s]
        base[...] -= jnp.dot(inner.astype(jnp.bfloat16), u_part, preferred_element_type=jnp.float32)

    @pl.when(short & jnp.logical_not(is_end | is_ahead | lent))
    def _():
        @pl.when(jnp.logical_not(is_even_end))
        def _():
            shared_wait(u_in, u_recv, prev_home)

        u_part = u_in[...].astype(jnp.bfloat16)
        inner = wait_w(w_in, w_send, w_recv, row - 1)
        base[...] -= jnp.dot(inner.astype(jnp.bfloat16), u_part, preferred_element_type=jnp.float32)

    @pl.when(is_end)
    def _():
        shared_wait(u_in, u_recv, prev_home)
        shared_wait(t_in, t_recv, far_home)
        u_part = u_in[...].astype(jnp.bfloat16)
        t_part = t_in[...].astype(jnp.bfloat16)

        @pl.when(jnp.logical_not(takes))
        def _():
            remote(wl_in, wl_in, wp_send, wl_recv, (row, their_home)).wait_recv()

        @pl.when(jnp.logical_not(takes_whole))
        def _():
            remote(w2_in, w2_in, wp_send, k_recv, (row, whole_home)).wait_recv()

        inner = wait_w(w_in, w_send, w_recv, row - 1)
        inner -= jnp.dot(w2_in[...].astype(jnp.bfloat16), a_sum[2], preferred_element_type=jnp.float32)
        inner -= jnp.dot(wl_in[...].astype(jnp.bfloat16), a_sum[1], preferred_element_type=jnp.float32)
        late = wait_w(wx_in, wx_send, wm_recv, row - 2)
        base[...] -= jnp.dot(late.astype(jnp.bfloat16), t_part, preferred_element_type=jnp.float32)
        late = wait_w(we_in, we_send, we_recv, row - 2)
        inner -= jnp.dot(late.astype(jnp.bfloat16), a_sum[0], preferred_element_type=jnp.float32)
        base[...] -= jnp.dot(inner.astype(jnp.bfloat16), u_part, preferred_element_type=jnp.float32)

    reduced = base[...].astype(jnp.bfloat16)

    @pl.when(jnp.logical_not(even | is_ahead | passes) & (answers > 0))
    def _():
        pl.semaphore_wait(ready, answers)

    @pl.when(feeds & jnp.logical_not(is_even_end | lent))
    def _():
        w_out[...] = jnp.dot(reduced, fold[...].astype(jnp.bfloat16), preferred_element_type=jnp.float32)

        @pl.when(is_ahead)
        def _():
            send_w(w_out, w_in, w_send, w_recv, row + 1)
            send_w(w_out, we_in, we_send, we_recv, row + 2)
            wx_out[...] = jnp.dot(reduced, fold_x[...].astype(jnp.bfloat16), preferred_element_type=jnp.float32)
            send_w(wx_out, wx_in, wx_send, wm_recv, row + 2)

        @pl.when(before)
        def _():
            send_w(w_out, hw_in, w_send, du_recv, row + 2)

        @pl.when(jnp.logical_not(before | is_ahead))
        def _():
            send_w(w_out, w_in, w_send, w_recv, row + 1)

    @pl.when(row > 0)
    def _():
        by_col(lambda c: own_part(c, reduced))

    def send_y(i, carry):
        @pl.when((row < longs_of(i)) & jnp.logical_not(lent))
        def _():
            by_col(lambda c: near_copy(i, c).start())

        return carry

    def own_copy(c, peer):
        part = y_row.at[c, :, tail_of(c)]
        return remote(part, part, o_send, o_recv, (row, peer))

    lax.fori_loop(row + 1, jnp.where(first, 0, near_end), send_y, 0)
    for peer in peers:
        by_col(lambda c: own_copy(c, peer).start())

    @pl.when(first)
    def _():
        log_part()

    remote(logs.at[others], logs.at[others], l_send, l_recv, (row, peers[0])).wait()
    log_sum = logs[0]
    for s in range(1, n_col):
        log_sum = log_sum + logs[s]
    log_term = log_sum * (1.0 / width) - 0.5 * math.log(2.0 * math.pi)

    def left_y(i, carry):
        @pl.when((row < longs_of(i)) & jnp.logical_not(lent))
        def _():
            by_col(lambda c: near_copy(i, c).wait_send())

        return carry

    lax.fori_loop(row + 1, near_end, left_y, 0)

    @pl.when(feeds & jnp.logical_not(lent))
    def _():
        remote(w_in, w_in, w_send, w_recv, (row + 1, 0)).wait_send()

    @pl.when(lent)
    def _():
        by_col(lambda c: lend_inverse(c).wait_send())
        lend(fold, hf_in, wx_send, we_recv).wait_send()
        lend(hb_out, hb_in, wp_send, t_recv).wait_send()
        lend(l_in, hl_in, a_send, k_recv).wait_send()
        lend(u_in, hu_in, we_send, a_recv).wait_send()

    @pl.when(is_ahead)
    def _():
        part = w_in.at[others]
        remote(part, part, a_send, w_recv, (row, peers[0])).wait_send()
        by_col(lambda c: borrowed_y(c).wait_send())
        remote(hz_out, hz_in, wl_send, du_recv, (row - 1, col)).wait_send()
        remote(w_in, w_in, we_send, we_recv, (row + 2, 0)).wait_send()
        remote(w_in, w_in, wx_send, wm_recv, (row + 2, 0)).wait_send()

    @pl.when(is_even_end)
    def _():
        remote(a_in, a_in, a_send, a_recv, (row + 1, 0)).wait_send()

    @pl.when(takes)
    def _():
        @pl.when(jnp.logical_not(is_ahead))
        def _():
            remote(w_in, w_in, wl_send, wl_recv, (row - 1, 0)).wait_send()

        @pl.when(is_end | is_ahead)
        def _():
            remote(w_in.at[others], w_in.at[others], wp_send, wl_recv, (row, peers[0])).wait_send()

    @pl.when(hands)
    def _():
        remote(d_out, d_in, d_send, d_recv, (row + 1, col)).wait_send()
        share_done(l_out)

    @pl.when(hands_whole)
    def _():
        remote(d_out, d_in, d_send, d_recv, (row + 1, col)).wait_send()
        share_done(l_out)

    @pl.when(takes_whole)
    def _():
        remote(w_in, w_in, wl_send, p_recv.at[0], (row - 1, 0)).wait_send()
        remote(w_in.at[others], w_in.at[others], wp_send, k_recv, (row, peers[0])).wait_send()

    @pl.when(gives)
    def _():
        spread_done(v_out, prev_home, crosses)
        share_done(u_out)

    @pl.when(gives_far)
    def _():
        spread_done(x_out, far_home, jnp.bool_(True))
        share_done(t_out)

    @pl.when(crosses & (col != prev_home))
    def _():
        relay_done(v_out, prev_home)

    @pl.when(is_end & (col != far_home))
    def _():
        relay_done(x_out, far_home)

    for q in range(per_col):

        @pl.when(q * n_col + col < long_count)
        def _():
            part = p_out.at[q, others]
            remote(part, part, p_send.at[q], p_recv.at[0], (row, peers[0])).wait_send()

    def wait_others(c):
        part = tally.at[pl.ds(0, tally.shape[0] - tail_of(c).size // 128)]
        remote(part, part, o_send, o_recv, (row, peers[0])).wait_recv()

    by_col(wait_others)
    y = y_row[0]
    for s in range(1, n_col):
        y = y + y_row[s]
    y_all[...] = y

    def far_copy(i):
        return remote(y_all, y_in.at[own_slot, 0], y_send.at[lax.rem(i - row - 1, y_sends)], y_recv.at[own_slot], (i, col))

    def send_far(i, carry):
        far_copy(i).start()
        return carry

    @pl.when(far_answers > 0)
    def _():
        pl.semaphore_wait(ready_far, far_answers)

    @pl.when(passes)
    def _():
        lax.fori_loop(4, n_row, pass_on, 0)
        part = y_in.at[:, pl.ds(0, (n_row - 2) // per_col)]
        remote(part, part, pass_send, y_recv.at[0], (2, 0)).wait_send()

    lax.fori_loop(jnp.where(relays, near_end, n_row), n_row, send_far, 0)
    white_ref[0, 0] = y
    quadratic = jnp.sum(y * y, axis=1, keepdims=True) * (1.0 / width)
    lik = -0.5 * quadratic + log_term
    r_id = lax.broadcasted_iota(jnp.int32, (nrhs, 128), 0)
    c_id = lax.broadcasted_iota(jnp.int32, (nrhs, 128), 1)
    flat = jnp.sum(jnp.where(r_id == c_id, lik, 0.0), axis=0, keepdims=True)
    lik_ref[0] = flat[:, :nrhs]

    def left_far(i, carry):
        far_copy(i).wait_send()
        return carry

    lax.fori_loop(jnp.where(relays, near_end, n_row), n_row, left_far, 0)

    def own_left(c):
        part = y_row.at[others, :, tail_of(c)]
        remote(part, part, o_send, o_recv, (row, peers[0])).wait_send()

    by_col(own_left)


def local(n_row, n_col, right_side, inverse_t, u_factor, v_factor, ranks):
    nrhs, width = right_side.shape[2:]
    per_col, _, rank_max = u_factor.shape[2:5]
    piece = width // n_col
    vmem = pl.BlockSpec(memory_space=pltpu.VMEM)
    hbm = pl.BlockSpec(memory_space=pl.ANY)
    dma = pltpu.SemaphoreType.DMA

    def f32(*shape):
        return pltpu.VMEM(shape, jnp.float32)

    def bf16(*shape):
        return pltpu.VMEM(shape, jnp.bfloat16)

    units = sum((width - c * piece // 128 * 128) // 128 for c in range(n_col))
    tile_set = [
        f32(n_col, rank_max, piece),
        f32(n_col, rank_max, piece),
        f32(n_col, rank_max, piece),
        f32(rank_max, piece),
        f32(piece, rank_max),
        f32(nrhs, rank_max),
        f32(n_col, nrhs, rank_max),
    ]
    return pl.pallas_call(
        functools.partial(kernel, n_row, n_col),
        out_shape=(
            pltpu.VMEM((1, 1, nrhs, width), jnp.float32),
            pltpu.VMEM((1, 1, nrhs), jnp.float32),
        ),
        in_specs=[hbm, hbm, hbm, hbm, hbm],
        out_specs=(vmem, vmem),
        scratch_shapes=[
            f32(nrhs, width),
            bf16(piece, width),
            bf16(per_col, rank_max, width),
            bf16(per_col, rank_max, width),
            pltpu.SMEM((per_col,), jnp.int32),
            f32(per_col, n_col, nrhs, width),
            f32(per_col, n_col, nrhs, piece),
            f32(n_row, nrhs, piece),
            f32(n_col, nrhs, width),
            f32(n_col, 1, 128),
            f32(nrhs, piece),
            f32(nrhs, width),
            f32(nrhs, width),
            f32(units, nrhs, 128),
            *tile_set,
            *tile_set,
            f32(rank_max, width),
            f32(rank_max, width),
            bf16(width, rank_max),
            bf16(per_col, width, rank_max),
            f32(rank_max, piece),
            f32(nrhs, rank_max),
            f32(nrhs, rank_max),
            f32(n_col, rank_max, piece),
            f32(rank_max, piece),
            f32(nrhs, rank_max),
            f32(nrhs, rank_max),
            f32(n_col, nrhs, rank_max),
            f32(3, rank_max, rank_max),
            f32(3, n_col, rank_max, rank_max),
            bf16(3, rank_max, rank_max),
            f32(rank_max, piece),
            f32(rank_max, piece),
            f32(piece, rank_max),
            f32(piece, width),
            f32(piece, width),
            bf16(piece, width),
            f32(nrhs, piece),
            f32(nrhs, piece),
            f32(nrhs, piece),
            f32(nrhs, piece),
            f32(nrhs, rank_max),
            f32(n_col, nrhs, rank_max),
            f32(nrhs, width),
            dma((5,)),
            dma((max(NEAR + 1, n_row - NEAR - 1),)),
            dma((per_col,)),
            dma((per_col,)),
            dma((n_row - 3,)),
            dma, dma, dma, dma,
            dma((n_col,)),
            dma((n_col,)),
            dma, dma, dma, dma,
            dma((n_col,)),
            dma, dma,
            pltpu.SemaphoreType.REGULAR,
            pltpu.SemaphoreType.REGULAR,
            dma,
            dma, dma, dma, dma, dma,
            dma, dma, dma, dma, dma, dma, dma, dma, dma,
        ],
        compiler_params=pltpu.CompilerParams(collective_id=0, has_side_effects=True),
        name="forward_solve",
    )(right_side, inverse_t, u_factor, v_factor, ranks.reshape(per_col))


def solution(mesh):
    placed = (
        P(None, "row", None, None),
        P(None, "row", "col", None),
        P(None, "row", None, "col", None, None),
        P(None, "row", None, "col", None, None),
        P(None, "row", None, "col"),
    )
    return jax.shard_map(
        functools.partial(local, mesh.shape["row"], mesh.shape["col"]),
        mesh=mesh,
        in_specs=placed,
        out_specs=(P(None, "row", None, None), P(None, "row", None)),
        check_vma=False,
    )
```

```python
import functools
import math

import jax
import jax.numpy as jnp
from jax import lax
from jax.experimental import pallas as pl
from jax.experimental.pallas import tpu as pltpu
from jax.sharding import PartitionSpec as P

MESH = pl.DeviceIdType.MESH
NT = (((1,), (1,)), ((), ()))
FIRST_SHORT = 3
NEAR = 3


def remote(src, dst, send_sem, recv_sem, device):
    return pltpu.make_async_remote_copy(
        src_ref=src,
        dst_ref=dst,
        send_sem=send_sem,
        recv_sem=recv_sem,
        device_id=device,
        device_id_type=MESH,
    )


def kernel(
    n_row, n_col,
    rhs_hbm, inv_hbm, u_hbm, v_hbm, rank_hbm,
    white_ref, lik_ref,
    rhs_ref, inv_ref, u_ref, v_ref, rank_ref,
    y_in, p_out, p_in, y_row, logs, base, y_full, y_all, tally,
    v_out, v_in, u_out, u_in, fold, w_out, w_in,
    x_out, x_in, t_out, t_in, fold_x, wx_out, wx_in,
    d_out, d_in, d_tile, vt_ref, l2_in, w2_out, w2_in, l_out, l_in, wl_out, wl_in, we_in,
    a_out, a_in, a_sum,
    hl_in, hu_in, hf_in, hv_out, hv_in, hv_tile, hb_out, hb_in, hz_out, hz_in, hw_out, hw_in, hy_out,
    in_sem, y_send, y_recv, p_send, p_recv, o_send, o_recv, l_send, l_recv,
    v_send, v_recv, u_send, u_recv, w_send, w_recv, m_recv, f_send, e_send, ready, ready_far, pass_send,
    t_recv, k_recv, d_send, d_recv, du_recv, wl_send, wl_recv, wp_send,
    we_send, we_recv, wx_send, wx_recv, a_send, a_recv,
):
    row = lax.axis_index("row")
    col = lax.axis_index("col")
    per_col, rank_max, width = u_ref.shape
    nrhs = rhs_ref.shape[0]
    piece = width // n_col
    half = n_col // 2
    y_sends = y_send.shape[0]
    some = half
    peers = [lax.rem(col + k, n_col) for k in range(1, n_col)]
    others = pl.ds(0, n_col - 1)
    own_slot = row // n_col
    own_home = lax.rem(row, n_col)
    end = n_row - 1
    even_end = n_row - 2
    ahead = n_row - 3

    def longs_of(i):
        count = jnp.where(i >= FIRST_SHORT, i - 1, i)
        handed = (lax.rem(i, 2) == 0) & (i >= 2)
        return count - jnp.where(handed, 1, 0) - jnp.where(i >= even_end, 1, 0)

    def near_of(i):
        return jnp.where(i == 0, 1, NEAR + jnp.where(i >= 2, 1, 0))

    copies = [
        pltpu.make_async_copy(v_hbm.at[0, 0, :, 0], v_ref, in_sem.at[0]),
        pltpu.make_async_copy(u_hbm.at[0, 0, :, 0], u_ref, in_sem.at[1]),
        None,
        pltpu.make_async_copy(rhs_hbm.at[0, 0], rhs_ref, in_sem.at[3]),
        pltpu.make_async_copy(rank_hbm, rank_ref, in_sem.at[4]),
    ]
    @pl.when(lax.axis_index("row") > 0)
    def _():
        copies[0].start()
        copies[1].start()

    def tail_of(c):
        start = c * piece // 128 * 128
        return pl.ds(start, width - start)

    def inverse_copy(c):
        return pltpu.make_async_copy(inv_hbm.at[0, 0, :, tail_of(c)], inv_ref.at[:, tail_of(c)], in_sem.at[2])

    def by_col(act):
        for c in range(n_col):
            pl.when(col == c)(functools.partial(act, c))

    by_col(lambda c: inverse_copy(c).start())
    for copy in copies[3:]:
        copy.start()
    barrier = pltpu.get_barrier_semaphore()

    def signal(sem, i, s):
        pl.semaphore_signal(sem, inc=1, device_id=(i, s), device_id_type=MESH)

    for peer in peers:
        signal(barrier, row, peer)

    def set_base():
        for cc in range(n_col):

            @pl.when(col == cc)
            def _():
                base[...] = rhs_ref[:, cc * piece:(cc + 1) * piece]

    def own_part(c, reduced):
        tail = tail_of(c)
        y_row[c, :, tail] = jnp.dot(reduced, inv_ref[:, tail], preferred_element_type=jnp.float32)

    def near_copy(i, c):
        tail = tail_of(c)
        sem = y_send.at[lax.rem(i - row - 1, y_sends)]
        return remote(y_row.at[c, :, tail], y_in.at[own_slot, c, :, tail], sem, y_recv.at[own_slot], (i, own_home))

    first = row == 0

    @pl.when(first)
    def _():
        for s in range(n_col):
            signal(barrier, 1, s)
        copies[3].wait()
        by_col(lambda c: inverse_copy(c).wait())
        set_base()
        reduced = base[...].astype(jnp.bfloat16)
        by_col(lambda c: own_part(c, reduced))
        pl.semaphore_wait(barrier, 2 * n_col - 1)
        by_col(lambda c: near_copy(1, c).start())

    for s in range(1, n_col):
        start = s * piece // 128 * 128
        if start:
            y_row[s, :, :start] = jnp.zeros((nrhs, start), jnp.float32)
            for q in range(per_col):
                y_in[q, s, :, :start] = jnp.zeros((nrhs, start), jnp.float32)

    even = lax.rem(row, 2) == 0
    short = row >= FIRST_SHORT
    feeds = (row + 1 >= FIRST_SHORT) & (row < end)
    is_end = row == end
    is_even_end = row == even_end
    is_ahead = row == ahead
    lent = row == ahead - 1
    before = row == ahead - 2
    long_count = longs_of(row)
    near_end = jnp.minimum(row + near_of(row) + 1, n_row)
    relays = (col == own_home) & (row > 0)
    passes = (row == 1) & (col == 0)

    def row_of(i, cond, act):
        @pl.when(cond)
        def _():
            for s in range(n_col):
                act(i, s)

        return jnp.where(cond, n_col, 0)

    def above(act):
        yield row + 1, row_of(row + 1, (row > 0) & (row < end), act)
        for d in range(2, NEAR + 2):
            wide = (is_ahead | before) if d == 2 else jnp.bool_(False)
            one = (row + d < n_row) & (d <= near_of(row)) & jnp.logical_not(wide)

            @pl.when(one)
            def _():
                act(row + d, own_home)

            yield row + d, jnp.where(one, 1, 0)
            if d == 2:
                yield row + d, row_of(row + d, wide, act)

    def below(act, act_far=None):
        row_of(row - 1, row > 0, act)
        count = jnp.where(row > 0, n_col, 0)
        for d in range(2, NEAR + 2):
            fed = (row >= d) & (d <= near_of(row - d)) & (lax.rem(jnp.maximum(row - d, 0), n_col) == col)
            if d == 2:
                fed = fed | is_end | is_ahead
            count += row_of(row - d, fed, act)
        for q in range(per_col):
            j = q * n_col + col
            far = j < row - near_of(j)

            source = jnp.where(j == 0, 1, j)
            soon = (j == 0) & (row <= 3)

            @pl.when(far & soon)
            def _():
                act(source, col)

            @pl.when(far & jnp.logical_not(soon))
            def _():
                (act_far or act)(source, col)

            count += jnp.where(far, 1, 0)
        return count

    def at_once(low, high):
        return (low == 0) & (high == 1)

    greeted = jnp.int32(n_col - 1)
    answers = jnp.int32(0)
    for i, count in above(lambda i, s: signal(barrier, i, s)):
        answers += count

    def greet_far(i, count):
        signal(barrier, i, col)
        return count + 1

    far_answers = lax.fori_loop(jnp.where(relays, near_end, n_row), n_row, greet_far, jnp.int32(0))
    far_answers = lax.fori_loop(jnp.where(passes, 4, n_row), n_row, greet_far, far_answers)
    answers = lax.fori_loop(jnp.where(passes, 2, n_row), jnp.where(passes, 4, n_row), greet_far, answers)

    def greet_quick(i, s):
        @pl.when(at_once(i, row))
        def _():
            signal(barrier, i, s)

    def answer(i, s):
        @pl.when(jnp.logical_not(at_once(i, row)))
        def _():
            signal(ready, i, s)

    greeted += below(greet_quick)

    prev = jnp.maximum(row - 1, 0)
    prev_slot = prev // n_col
    prev_home = lax.rem(prev, n_col)
    gives = short & (col == prev_home)
    crosses = short & even
    far_slot = ahead // n_col
    far_home = ahead % n_col
    gives_far = is_end & (col == far_home)
    handed = even & (row >= 2)
    mine = jnp.where(handed, long_count + jnp.where(is_even_end, 1, 0), 0)
    mine_slot = mine // n_col
    mine_home = lax.rem(mine, n_col)
    hands = handed & (col == mine_home)
    taken = (row >= 3) & jnp.logical_not(even)
    theirs = jnp.where(taken, longs_of(prev) + jnp.where(is_end, 1, 0), 0)
    their_home = lax.rem(theirs, n_col)
    takes = taken & (col == their_home)
    whole = even_end - 3
    whole_slot = whole // n_col
    whole_home = whole % n_col
    hands_whole = is_even_end & (col == whole_home)
    takes_whole = is_end & (col == whole_home)

    def masked_u(slot):
        keep = lax.broadcasted_iota(jnp.int32, (rank_max, width), 0) < rank_ref[slot]
        return jnp.where(keep, u_ref[slot].astype(jnp.float32), 0.0)

    def cut(tile, into):
        for s in range(n_col):
            into[s] = tile[:, s * piece:(s + 1) * piece]

    @pl.when(row > 0)
    def _():
        copies[0].wait()
        copies[1].wait()

    copies[4].wait()

    @pl.when(hands)
    def _():
        d_out[...] = v_ref[mine_slot].astype(jnp.float32)
        cut(masked_u(mine_slot), l_out)

    @pl.when(hands_whole)
    def _():
        d_out[...] = v_ref[whole_slot].astype(jnp.float32)
        cut(masked_u(whole_slot), l_out)

    @pl.when(gives)
    def _():
        cut(v_ref[prev_slot].astype(jnp.float32), v_out)
        cut(masked_u(prev_slot), u_out)

    @pl.when(gives_far)
    def _():
        cut(v_ref[far_slot].astype(jnp.float32), x_out)
        cut(masked_u(far_slot), t_out)

    @pl.when(row > 0)
    def _():
        pl.semaphore_wait(barrier, greeted)

    below(answer, lambda i, s: signal(ready_far, i, s))

    def by_way(home, s, cc):
        across = n_col - 1 - home
        return (home != s) & jnp.where(
            across < home,
            jnp.where(across == s, cc < s + some, (home != s + 1) | (cc == s)),
            (s > home) | (cc < s + half),
        )

    def is_late(home, s, cc):
        across = n_col - 1 - home
        return (across == s) & (across < home) & (cc >= s + some)

    def beside(home, s):
        return split_row(home) & (home == s + 1) & (n_col - 1 - home != s)

    def split_row(home):
        return n_col - 1 - home < home

    def is_split(home, s):
        across = n_col - 1 - home
        return (across == s) & (across < home)

    def joined(home, s):
        across = n_col - 1 - home
        return (across > home) & (across == s)

    def spread(out, into, recv, target, home, cross):
        for s in range(n_col):
            for cc in range(s, min(s + some, n_col)):

                @pl.when(cross & is_split(home, s))
                def _():
                    remote(out.at[cc], out.at[cc], v_send.at[s], m_recv.at[cc], (row, s)).start()

        for s in range(n_col):
            if s > 0:

                @pl.when(cross & joined(home, s - 1))
                def _():
                    remote(out.at[s - 1], out.at[s - 1], v_send.at[s], m_recv.at[s - 1], (row, s)).start()

            for cc in range(s, n_col):
                gone = cross & (joined(home, s) | is_split(home, s))
                way = cross & by_way(home, s, cc)
                later = cross & is_late(home, s, cc)

                @pl.when(way & jnp.logical_not(gone))
                def _():
                    remote(out.at[cc], out.at[cc], v_send.at[s], m_recv.at[cc], (row, s)).start()

                @pl.when(jnp.logical_not(way | later | gone))
                def _():
                    remote(out.at[cc], into.at[cc], v_send.at[s], recv.at[cc], (target, s)).start()

    def spread_late(out, into, recv, target, home):
        for s in range(n_col):

            @pl.when(split_row(home) & (n_col - home == s))
            def _():
                part = pl.ds(s, n_col - s)
                remote(out.at[part], out.at[part], v_send.at[s], m_recv.at[0], (row, s)).wait_send()

        for s in range(n_col):
            for cc in range(min(s + some, n_col), n_col):

                @pl.when(is_late(home, s, cc))
                def _():
                    remote(out.at[cc], into.at[cc], v_send.at[s], recv.at[cc], (target, s)).start()

    def spread_done(out, home, cross):
        for s in range(n_col):
            part = pl.ds(s, n_col - s)
            gone = cross & joined(home, s)
            gone = gone | (cross & split_row(home) & (n_col - home == s))
            more = (cross & joined(home, s - 1)) if s > 0 else jnp.bool_(False)

            @pl.when(jnp.logical_not(gone | more))
            def _():
                remote(out.at[part], out.at[part], v_send.at[s], m_recv.at[0], (row, s)).wait_send()

            if s > 0:
                part_more = pl.ds(s - 1, n_col - s + 1)

                @pl.when(more)
                def _():
                    remote(out.at[part_more], out.at[part_more], v_send.at[s], m_recv.at[0], (row, s)).wait_send()

    def relay(out, into, recv, target, home):
        across = n_col - 1 - home
        more = joined(home, col - 1)
        first = jnp.where(more, col - 1, col)
        part = jnp.where(across < home, across == col, col < home)
        share_of = jnp.where(across < home, some, half)
        stop = jnp.where(part, jnp.minimum(col + share_of, n_col), n_col)
        stop = jnp.where(joined(home, col) | beside(home, col), col + 1, stop)

        def forward(cc, carry):
            remote(out.at[cc], out.at[cc], v_send.at[0], m_recv.at[cc], (row, home)).wait_recv()

            @pl.when(cc >= col)
            def _():
                remote(out.at[cc], into.at[cc], f_send, recv.at[cc], (target, col)).start()

            @pl.when(more & (cc == across))
            def _():
                remote(out.at[cc], out.at[cc], e_send, m_recv.at[cc], (row, across)).start()

            @pl.when(more & (cc > across))
            def _():
                remote(out.at[cc], into.at[cc], e_send, recv.at[cc], (target, across)).start()

            return carry

        lax.fori_loop(first, stop, forward, 0)

    def relay_done(out, home):
        across = n_col - 1 - home
        for cc in range(n_col):
            here = col == cc
            half_way = jnp.where(across < home, across == cc, cc < home)

            @pl.when(here & (joined(home, cc) | beside(home, cc)))
            def _():
                remote(out.at[cc], out.at[cc], f_send, v_recv.at[0], (row, home)).wait_send()

            @pl.when(here & jnp.logical_not(half_way | joined(home, cc) | beside(home, cc)))
            def _():
                part = pl.ds(cc, n_col - cc)
                remote(out.at[part], out.at[part], f_send, v_recv.at[0], (row, home)).wait_send()

            for count, cond in ((some, across < home), (half, across > home)):
                few = pl.ds(cc, min(count, n_col - cc))

                @pl.when(here & half_way & cond)
                def _():
                    remote(out.at[few], out.at[few], f_send, v_recv.at[0], (row, home)).wait_send()

            if cc > 0:

                @pl.when((col == cc) & joined(home, cc - 1))
                def _():
                    part = pl.ds(cc - 1, n_col - cc + 1)
                    remote(out.at[part], out.at[part], e_send, v_recv.at[0], (row, home)).wait_send()

    def share(out, into, recv):
        for k in range(n_col):
            peer = lax.rem(2 * n_col - 1 - col + k, n_col)

            @pl.when(peer != col)
            def _():
                remote(out.at[peer], into, u_send, recv, (row, peer)).start()

        into[...] = out[col]

    def share_done(out):
        remote(out.at[others], out.at[others], u_send, u_recv, (row, peers[0])).wait_send()

    def shared_wait(into, recv, home):
        @pl.when(col != home)
        def _():
            remote(into, into, u_send, recv, (row, home)).wait_recv()

    early_l = (row < FIRST_SHORT) | is_even_end

    opposite = n_col - 1 - col

    @pl.when(hands)
    def _():
        for peer in peers:

            @pl.when(early_l | (peer != opposite))
            def _():
                remote(l_out.at[peer], l_in, u_send, k_recv, (row, peer)).start()

        l_in[...] = l_out[col]

    @pl.when(hands_whole)
    def _():
        share(l_out, l2_in, du_recv)

    @pl.when(gives)
    def _():
        spread(v_out, v_in, v_recv, row - 1, prev_home, crosses)

    @pl.when(gives & (is_even_end | jnp.logical_not(even)))
    def _():
        share(u_out, u_in, u_recv)

    @pl.when(gives_far)
    def _():
        spread(x_out, x_in, m_recv, row - 2, far_home, jnp.bool_(True))

    @pl.when((handed) & (answers > 0))
    def _():
        pl.semaphore_wait(ready, answers)

    @pl.when(hands | hands_whole)
    def _():
        remote(d_out, d_in, d_send, d_recv, (row + 1, col)).start()

    relays_late = is_even_end & joined(prev_home, col)

    @pl.when(crosses & (col != prev_home) & jnp.logical_not(relays_late))
    def _():
        relay(v_out, v_in, v_recv, row - 1, prev_home)

    @pl.when(row > 0)
    def _():
        by_col(lambda c: inverse_copy(c).wait())
        copies[3].wait()


    def lend(src, dst, send, recv):
        return remote(src, dst, send, recv, (row + 1, col))

    def lend_inverse(c):
        return lend(hv_out.at[:, tail_of(c)], hv_in.at[:, tail_of(c)], wl_send, wx_recv)

    def lend_tail(c):
        hv_out[:, tail_of(c)] = inv_ref[:, tail_of(c)].astype(jnp.float32)
        lend_inverse(c).start()

    pl.when(lent)(functools.partial(by_col, lend_tail))

    pl.when(row > 0)(set_base)

    def log_part():
        for cc in range(n_col):

            @pl.when(col == cc)
            def _():
                block = inv_ref[:, cc * piece:(cc + 1) * piece].astype(jnp.float32)
                r_id = lax.broadcasted_iota(jnp.int32, (piece, piece), 0)
                c_id = lax.broadcasted_iota(jnp.int32, (piece, piece), 1)
                diagonal = jnp.sum(jnp.where(r_id == c_id, block, 0.0), axis=0, keepdims=True)
                total = jnp.sum(jnp.log(diagonal), axis=1, keepdims=True)
                logs[cc] = jnp.broadcast_to(total, (1, 128))

        for peer in peers:
            remote(logs.at[col], logs.at[col], l_send, l_recv, (row, peer)).start()

    pl.when(row > 0)(log_part)

    for q in range(per_col):

        @pl.when(q * n_col + col < long_count)
        def _():
            vt_ref[q] = v_ref[q].astype(jnp.float32).T.astype(jnp.bfloat16)

    @pl.when(gives & crosses)
    def _():
        spread_late(v_out, v_in, v_recv, row - 1, prev_home)

    @pl.when(gives & crosses & jnp.logical_not(is_even_end))
    def _():
        share(u_out, u_in, u_recv)

    @pl.when(hands & jnp.logical_not(early_l))
    def _():
        remote(l_out.at[opposite], l_in, u_send, k_recv, (row, opposite)).start()

    def fold_with(into, recv, target):
        target[...] = jnp.zeros_like(target)
        for cc in range(n_col):

            @pl.when(col <= cc)
            def _():
                remote(into.at[cc], into.at[cc], f_send, recv.at[cc], (row, cc)).wait_recv()
                target[...] += lax.dot_general(
                    inv_ref[:, cc * piece:(cc + 1) * piece],
                    into[cc].astype(jnp.bfloat16),
                    NT,
                    preferred_element_type=jnp.float32,
                )

    def long_step(q, cond):
        j = q * n_col + col

        @pl.when((j < long_count) & cond)
        def _():
            near = row - j <= near_of(j)

            @pl.when(near)
            def _():
                remote(tally, tally, y_send.at[0], y_recv.at[q], (j, col)).wait_recv()
                y = y_in[q, 0]
                for s in range(1, n_col):
                    y = y + y_in[q, s]
                y_full[...] = y

            @pl.when(jnp.logical_not(near))
            def _():
                remote(y_in.at[q, 0], y_in.at[q, 0], y_send.at[0], y_recv.at[q], (j, col)).wait_recv()
                y_full[...] = y_in[q, 0]

            y = y_full[...].astype(jnp.bfloat16)

            @pl.when(takes & (j == theirs))
            def _():
                wl_out[...] = jnp.dot(y, d_tile[...], preferred_element_type=jnp.float32)
                @pl.when(jnp.logical_not(is_ahead))
                def _():
                    for s in range(n_col):
                        remote(wl_out, wl_in, wl_send, wl_recv, (row - 1, s)).start()

                @pl.when(is_end | is_ahead)
                def _():
                    for peer in peers:
                        remote(wl_out, wl_in, wp_send, wl_recv, (row, peer)).start()
                    wl_in[...] = wl_out[...]

            @pl.when(takes_whole & (j == whole))
            def _():
                w2_out[...] = jnp.dot(y, d_tile[...], preferred_element_type=jnp.float32)
                for s in range(n_col):
                    remote(w2_out, w2_in, wl_send, p_recv.at[whole], (row - 1, s)).start()
                for peer in peers:
                    remote(w2_out, w2_in, wp_send, k_recv, (row, peer)).start()
                w2_in[...] = w2_out[...]

            inner = jnp.dot(y, vt_ref[q], preferred_element_type=jnp.float32)
            keep = lax.broadcasted_iota(jnp.int32, (nrhs, rank_max), 1) < rank_ref[q]
            inner = jnp.where(keep, inner, 0.0).astype(jnp.bfloat16)
            p = jnp.dot(inner, u_ref[q], preferred_element_type=jnp.float32)
            for s in range(n_col):
                p_out[q, s] = p[:, s * piece:(s + 1) * piece]
            for peer in peers:
                remote(p_out.at[q, peer], p_in.at[j], p_send.at[q], p_recv.at[j], (row, peer)).start()
            p_in[j] = p_out[q, col]

    def products():
        fold_with(v_in, v_recv, fold)
        factor = fold[...].astype(jnp.bfloat16)
        shared_wait(u_in, u_recv, prev_home)
        shared_wait(l_in, k_recv, mine_home)
        a_out[0] = jnp.dot(u_in[...].astype(jnp.bfloat16), factor, preferred_element_type=jnp.float32)
        a_out[1] = jnp.dot(l_in[...].astype(jnp.bfloat16), factor, preferred_element_type=jnp.float32)
        shared_wait(l2_in, du_recv, whole_home)
        a_out[2] = jnp.dot(l2_in[...].astype(jnp.bfloat16), factor, preferred_element_type=jnp.float32)
        for k in range(3):
            for s in range(n_col):
                remote(a_out.at[k], a_in.at[k, col], a_send, a_recv, (row + 1, s)).start()

    @pl.when(relays_late)
    def _():
        products()
        relay(v_out, v_in, v_recv, row - 1, prev_home)

    @pl.when(takes | takes_whole)
    def _():
        remote(d_in, d_in, d_send, d_recv, (row - 1, col)).wait_recv()
        d_tile[...] = d_in[...].T.astype(jnp.bfloat16)

    @pl.when(is_end & (col != far_home))
    def _():
        relay(x_out, x_in, m_recv, row - 2, far_home)

    for q in range(per_col):
        long_step(q, jnp.logical_not(is_ahead & (q * n_col + col == row - 2)))

    def pass_on(i, carry):
        remote(y_full, y_in.at[0, 0], pass_send, y_recv.at[0], (i, 0)).start()
        return carry

    @pl.when(passes)
    def _():
        pl.semaphore_wait(ready, answers)
        lax.fori_loop(2, 4, pass_on, 0)

    def send_w(out, into, send, recv, i):
        for s in range(n_col):
            remote(out, into.at[col], send, recv, (i, s)).start()

    def wait_w(into, send, recv, i):
        remote(into, into, send, recv, (i, 0)).wait_recv()
        total = into[0]
        for s in range(1, n_col):
            total = total + into[s]
        return total

    def borrowed_y(c):
        tail = tail_of(c)
        slot = (ahead - 1) // n_col
        home = (ahead - 1) % n_col
        return remote(hy_out.at[:, tail], y_in.at[slot, c, :, tail], y_send.at[0], y_recv.at[slot], (end, home))

    @pl.when(is_ahead)
    def _():
        back = (row - 1, col)
        by_col(lambda c: remote(hv_in.at[:, tail_of(c)], hv_in.at[:, tail_of(c)], wl_send, wx_recv, back).wait_recv())
        by_col(lambda c: hv_tile.__setitem__((slice(None), tail_of(c)), hv_in[:, tail_of(c)].astype(jnp.bfloat16)))
        remote(hl_in, hl_in, a_send, k_recv, back).wait_recv()
        remote(hu_in, hu_in, we_send, a_recv, back).wait_recv()
        remote(hf_in, hf_in, wx_send, we_recv, back).wait_recv()
        remote(hb_in, hb_in, wp_send, t_recv, back).wait_recv()
        l_part = hl_in[...].astype(jnp.bfloat16)
        u_part = hu_in[...].astype(jnp.bfloat16)
        factor = hf_in[...].astype(jnp.bfloat16)

        @pl.when(answers > 0)
        def _():
            pl.semaphore_wait(ready, answers)

        @pl.when(jnp.logical_not(takes))
        def _():
            remote(wl_in, wl_in, wp_send, wl_recv, (row, their_home)).wait_recv()

        part = hb_in[...] - jnp.dot(wl_in[...].astype(jnp.bfloat16), l_part, preferred_element_type=jnp.float32)
        inner = wait_w(hw_in, w_send, du_recv, row - 2)
        part -= jnp.dot(inner.astype(jnp.bfloat16), u_part, preferred_element_type=jnp.float32)
        part = part.astype(jnp.bfloat16)
        def borrowed_part(c):
            tail = tail_of(c)
            hy_out[:, tail] = jnp.dot(part, hv_tile[:, tail], preferred_element_type=jnp.float32)
            borrowed_y(c).start()

        by_col(borrowed_part)
        hw_out[...] = jnp.dot(part, factor, preferred_element_type=jnp.float32)
        for peer in peers:
            remote(hw_out, w_in.at[col], a_send, w_recv, (row, peer)).start()
        w_in[col] = hw_out[...]

        hz_out[...] = part.astype(jnp.float32)
        remote(hz_out, hz_in, wl_send, du_recv, back).start()

    for q in range(per_col):
        long_step(q, is_ahead & (q * n_col + col == row - 2))

    pl.when(is_even_end & jnp.logical_not(relays_late))(products)

    @pl.when(feeds & jnp.logical_not(is_even_end))
    def _():
        fold_with(v_in, v_recv, fold)

        @pl.when(lent)
        def _():
            lend(fold, hf_in, wx_send, we_recv).start()

    @pl.when(gives_far)
    def _():
        spread_late(x_out, x_in, m_recv, row - 2, far_home)
        share(t_out, t_in, t_recv)

    @pl.when(is_ahead)
    def _():
        fold_with(x_in, m_recv, fold_x)

    @pl.when(is_end)
    def _():
        remote(a_in, a_in, a_send, a_recv, (row - 1, 0)).wait_recv()
        for k in range(3):
            total = a_in[k, 0]
            for s in range(1, n_col):
                total = total + a_in[k, s]
            a_sum[k] = total.astype(jnp.bfloat16)

    def gather_p(j, acc):
        home = lax.rem(j, n_col)

        @pl.when(home != col)
        def _():
            remote(p_in.at[j], p_in.at[j], p_send.at[0], p_recv.at[j], (row, home)).wait_recv()

        return acc - p_in[j]

    base[...] = lax.fori_loop(0, long_count - jnp.where(is_ahead, 1, 0), gather_p, base[...])

    @pl.when(lent)
    def _():
        hb_out[...] = base[...]
        lend(hb_out, hb_in, wp_send, t_recv).start()
        shared_wait(l_in, k_recv, mine_home)
        lend(l_in, hl_in, a_send, k_recv).start()
        shared_wait(u_in, u_recv, prev_home)
        lend(u_in, hu_in, we_send, a_recv).start()
        remote(hz_in, hz_in, wl_send, du_recv, (row + 1, col)).wait_recv()
        base[...] = hz_in[...]

    @pl.when(is_even_end)
    def _():
        w_out[...] = jnp.dot(base[...].astype(jnp.bfloat16), fold[...].astype(jnp.bfloat16), preferred_element_type=jnp.float32)
        send_w(w_out, w_in, w_send, w_recv, row + 1)

    @pl.when(handed & jnp.logical_not(lent))
    def _():
        @pl.when(jnp.logical_not(is_even_end))
        def _():
            shared_wait(l_in, k_recv, mine_home)

        l_part = l_in[...].astype(jnp.bfloat16)

        @pl.when(is_even_end)
        def _():
            remote(w2_in, w2_in, wl_send, p_recv.at[whole], (row + 1, whole_home)).wait_recv()
            base[...] -= jnp.dot(
                w2_in[...].astype(jnp.bfloat16), l2_in[...].astype(jnp.bfloat16), preferred_element_type=jnp.float32
            )

        remote(wl_in, wl_in, wl_send, wl_recv, (row + 1, mine_home)).wait_recv()
        base[...] -= jnp.dot(wl_in[...].astype(jnp.bfloat16), l_part, preferred_element_type=jnp.float32)

    @pl.when(is_ahead)
    def _():
        shared_wait(u_in, u_recv, prev_home)
        u_part = u_in[...].astype(jnp.bfloat16)
        part = w_in.at[others]
        remote(part, part, a_send, w_recv, (row, peers[0])).wait_recv()
        inner = w_in[0]
        for s in range(1, n_col):
            inner = inner + w_in[s]
        part = base[...] - jnp.dot(inner.astype(jnp.bfloat16), u_part, preferred_element_type=jnp.float32)
        base[...] = gather_p(row - 2, part)

    @pl.when(short & jnp.logical_not(is_end | is_ahead | lent))
    def _():
        @pl.when(jnp.logical_not(is_even_end))
        def _():
            shared_wait(u_in, u_recv, prev_home)

        u_part = u_in[...].astype(jnp.bfloat16)
        inner = wait_w(w_in, w_send, w_recv, row - 1)
        base[...] -= jnp.dot(inner.astype(jnp.bfloat16), u_part, preferred_element_type=jnp.float32)

    @pl.when(is_end)
    def _():
        shared_wait(u_in, u_recv, prev_home)
        shared_wait(t_in, t_recv, far_home)
        u_part = u_in[...].astype(jnp.bfloat16)
        t_part = t_in[...].astype(jnp.bfloat16)
        carried = -jnp.dot(a_sum[0], u_part, preferred_element_type=jnp.float32)
        both = jnp.concatenate([carried.astype(jnp.bfloat16), t_part])

        @pl.when(jnp.logical_not(takes))
        def _():
            remote(wl_in, wl_in, wp_send, wl_recv, (row, their_home)).wait_recv()

        @pl.when(jnp.logical_not(takes_whole))
        def _():
            remote(w2_in, w2_in, wp_send, k_recv, (row, whole_home)).wait_recv()

        inner = wait_w(w_in, w_send, w_recv, row - 1)
        inner -= jnp.dot(w2_in[...].astype(jnp.bfloat16), a_sum[2], preferred_element_type=jnp.float32)
        inner -= jnp.dot(wl_in[...].astype(jnp.bfloat16), a_sum[1], preferred_element_type=jnp.float32)
        part = base[...] - jnp.dot(inner.astype(jnp.bfloat16), u_part, preferred_element_type=jnp.float32)
        late = [wait_w(we_in, we_send, we_recv, row - 2), wait_w(wx_in, wx_send, wx_recv, row - 2)]
        late = jnp.concatenate(late, axis=1).astype(jnp.bfloat16)
        base[...] = part - jnp.dot(late, both, preferred_element_type=jnp.float32)

    reduced = base[...].astype(jnp.bfloat16)

    @pl.when(jnp.logical_not(even | is_ahead | passes) & (answers > 0))
    def _():
        pl.semaphore_wait(ready, answers)

    @pl.when(feeds & jnp.logical_not(is_even_end | lent))
    def _():
        w_out[...] = jnp.dot(reduced, fold[...].astype(jnp.bfloat16), preferred_element_type=jnp.float32)

        @pl.when(is_ahead)
        def _():
            send_w(w_out, w_in, w_send, w_recv, row + 1)
            send_w(w_out, we_in, we_send, we_recv, row + 2)
            wx_out[...] = jnp.dot(reduced, fold_x[...].astype(jnp.bfloat16), preferred_element_type=jnp.float32)
            send_w(wx_out, wx_in, wx_send, wx_recv, row + 2)

        @pl.when(before)
        def _():
            send_w(w_out, hw_in, w_send, du_recv, row + 2)

        @pl.when(jnp.logical_not(before | is_ahead))
        def _():
            send_w(w_out, w_in, w_send, w_recv, row + 1)

    @pl.when(row > 0)
    def _():
        by_col(lambda c: own_part(c, reduced))

    def send_y(i, carry):
        @pl.when((row < longs_of(i)) & jnp.logical_not(lent))
        def _():
            by_col(lambda c: near_copy(i, c).start())

        return carry

    def own_copy(c, peer):
        part = y_row.at[c, :, tail_of(c)]
        return remote(part, part, o_send, o_recv, (row, peer))

    lax.fori_loop(row + 1, jnp.where(first, 0, near_end), send_y, 0)
    for peer in peers:
        by_col(lambda c: own_copy(c, peer).start())

    @pl.when(first)
    def _():
        log_part()

    remote(logs.at[others], logs.at[others], l_send, l_recv, (row, peers[0])).wait()
    log_sum = logs[0]
    for s in range(1, n_col):
        log_sum = log_sum + logs[s]
    log_term = log_sum * (1.0 / width) - 0.5 * math.log(2.0 * math.pi)

    def left_y(i, carry):
        @pl.when((row < longs_of(i)) & jnp.logical_not(lent))
        def _():
            by_col(lambda c: near_copy(i, c).wait_send())

        return carry

    lax.fori_loop(row + 1, near_end, left_y, 0)

    @pl.when(feeds & jnp.logical_not(lent))
    def _():
        remote(w_in, w_in, w_send, w_recv, (row + 1, 0)).wait_send()

    @pl.when(lent)
    def _():
        by_col(lambda c: lend_inverse(c).wait_send())
        lend(fold, hf_in, wx_send, we_recv).wait_send()
        lend(hb_out, hb_in, wp_send, t_recv).wait_send()
        lend(l_in, hl_in, a_send, k_recv).wait_send()
        lend(u_in, hu_in, we_send, a_recv).wait_send()

    @pl.when(is_ahead)
    def _():
        part = w_in.at[others]
        remote(part, part, a_send, w_recv, (row, peers[0])).wait_send()
        by_col(lambda c: borrowed_y(c).wait_send())
        remote(hz_out, hz_in, wl_send, du_recv, (row - 1, col)).wait_send()
        remote(w_in, w_in, we_send, we_recv, (row + 2, 0)).wait_send()
        remote(w_in, w_in, wx_send, wx_recv, (row + 2, 0)).wait_send()

    @pl.when(is_even_end)
    def _():
        remote(a_in, a_in, a_send, a_recv, (row + 1, 0)).wait_send()

    @pl.when(takes)
    def _():
        @pl.when(jnp.logical_not(is_ahead))
        def _():
            remote(w_in, w_in, wl_send, wl_recv, (row - 1, 0)).wait_send()

        @pl.when(is_end | is_ahead)
        def _():
            remote(w_in.at[others], w_in.at[others], wp_send, wl_recv, (row, peers[0])).wait_send()

    @pl.when(hands)
    def _():
        remote(d_out, d_in, d_send, d_recv, (row + 1, col)).wait_send()
        share_done(l_out)

    @pl.when(hands_whole)
    def _():
        remote(d_out, d_in, d_send, d_recv, (row + 1, col)).wait_send()
        share_done(l_out)

    @pl.when(takes_whole)
    def _():
        remote(w_in, w_in, wl_send, p_recv.at[0], (row - 1, 0)).wait_send()
        remote(w_in.at[others], w_in.at[others], wp_send, k_recv, (row, peers[0])).wait_send()

    @pl.when(gives)
    def _():
        spread_done(v_out, prev_home, crosses)
        share_done(u_out)

    @pl.when(gives_far)
    def _():
        spread_done(x_out, far_home, jnp.bool_(True))
        share_done(t_out)

    @pl.when(crosses & (col != prev_home))
    def _():
        relay_done(v_out, prev_home)

    @pl.when(is_end & (col != far_home))
    def _():
        relay_done(x_out, far_home)

    for q in range(per_col):

        @pl.when(q * n_col + col < long_count)
        def _():
            part = p_out.at[q, others]
            remote(part, part, p_send.at[q], p_recv.at[0], (row, peers[0])).wait_send()

    def wait_others(c):
        part = tally.at[pl.ds(0, tally.shape[0] - tail_of(c).size // 128)]
        remote(part, part, o_send, o_recv, (row, peers[0])).wait_recv()

    by_col(wait_others)
    y = y_row[0]
    for s in range(1, n_col):
        y = y + y_row[s]
    y_all[...] = y

    def far_copy(i):
        return remote(y_all, y_in.at[own_slot, 0], y_send.at[lax.rem(i - row - 1, y_sends)], y_recv.at[own_slot], (i, col))

    def send_far(i, carry):
        far_copy(i).start()
        return carry

    @pl.when(far_answers > 0)
    def _():
        pl.semaphore_wait(ready_far, far_answers)

    @pl.when(passes)
    def _():
        lax.fori_loop(4, n_row, pass_on, 0)
        part = y_in.at[:, pl.ds(0, (n_row - 2) // per_col)]
        remote(part, part, pass_send, y_recv.at[0], (2, 0)).wait_send()

    lax.fori_loop(jnp.where(relays, near_end, n_row), n_row, send_far, 0)
    white_ref[0, 0] = y
    quadratic = jnp.sum(y * y, axis=1, keepdims=True) * (1.0 / width)
    lik = -0.5 * quadratic + log_term
    r_id = lax.broadcasted_iota(jnp.int32, (nrhs, 128), 0)
    c_id = lax.broadcasted_iota(jnp.int32, (nrhs, 128), 1)
    flat = jnp.sum(jnp.where(r_id == c_id, lik, 0.0), axis=0, keepdims=True)
    lik_ref[0] = flat[:, :nrhs]

    def left_far(i, carry):
        far_copy(i).wait_send()
        return carry

    lax.fori_loop(jnp.where(relays, near_end, n_row), n_row, left_far, 0)

    def own_left(c):
        part = y_row.at[others, :, tail_of(c)]
        remote(part, part, o_send, o_recv, (row, peers[0])).wait_send()

    by_col(own_left)


def local(n_row, n_col, right_side, inverse_t, u_factor, v_factor, ranks):
    nrhs, width = right_side.shape[2:]
    per_col, _, rank_max = u_factor.shape[2:5]
    piece = width // n_col
    vmem = pl.BlockSpec(memory_space=pltpu.VMEM)
    hbm = pl.BlockSpec(memory_space=pl.ANY)
    dma = pltpu.SemaphoreType.DMA

    def f32(*shape):
        return pltpu.VMEM(shape, jnp.float32)

    def bf16(*shape):
        return pltpu.VMEM(shape, jnp.bfloat16)

    units = sum((width - c * piece // 128 * 128) // 128 for c in range(n_col))
    tile_set = [
        f32(n_col, rank_max, piece),
        f32(n_col, rank_max, piece),
        f32(n_col, rank_max, piece),
        f32(rank_max, piece),
        f32(piece, rank_max),
        f32(nrhs, rank_max),
        f32(n_col, nrhs, rank_max),
    ]
    return pl.pallas_call(
        functools.partial(kernel, n_row, n_col),
        out_shape=(
            pltpu.VMEM((1, 1, nrhs, width), jnp.float32),
            pltpu.VMEM((1, 1, nrhs), jnp.float32),
        ),
        in_specs=[hbm, hbm, hbm, hbm, hbm],
        out_specs=(vmem, vmem),
        scratch_shapes=[
            f32(nrhs, width),
            bf16(piece, width),
            bf16(per_col, rank_max, width),
            bf16(per_col, rank_max, width),
            pltpu.SMEM((per_col,), jnp.int32),
            f32(per_col, n_col, nrhs, width),
            f32(per_col, n_col, nrhs, piece),
            f32(n_row, nrhs, piece),
            f32(n_col, nrhs, width),
            f32(n_col, 1, 128),
            f32(nrhs, piece),
            f32(nrhs, width),
            f32(nrhs, width),
            f32(units, nrhs, 128),
            *tile_set,
            *tile_set,
            f32(rank_max, width),
            f32(rank_max, width),
            bf16(width, rank_max),
            bf16(per_col, width, rank_max),
            f32(rank_max, piece),
            f32(nrhs, rank_max),
            f32(nrhs, rank_max),
            f32(n_col, rank_max, piece),
            f32(rank_max, piece),
            f32(nrhs, rank_max),
            f32(nrhs, rank_max),
            f32(n_col, nrhs, rank_max),
            f32(3, rank_max, rank_max),
            f32(3, n_col, rank_max, rank_max),
            bf16(3, rank_max, rank_max),
            f32(rank_max, piece),
            f32(rank_max, piece),
            f32(piece, rank_max),
            f32(piece, width),
            f32(piece, width),
            bf16(piece, width),
            f32(nrhs, piece),
            f32(nrhs, piece),
            f32(nrhs, piece),
            f32(nrhs, piece),
            f32(nrhs, rank_max),
            f32(n_col, nrhs, rank_max),
            f32(nrhs, width),
            dma((5,)),
            dma((max(NEAR + 1, n_row - NEAR - 1),)),
            dma((per_col,)),
            dma((per_col,)),
            dma((n_row - 3,)),
            dma, dma, dma, dma,
            dma((n_col,)),
            dma((n_col,)),
            dma, dma, dma, dma,
            dma((n_col,)),
            dma, dma,
            pltpu.SemaphoreType.REGULAR,
            pltpu.SemaphoreType.REGULAR,
            dma,
            dma, dma, dma, dma, dma,
            dma, dma, dma, dma, dma, dma, dma, dma, dma,
        ],
        compiler_params=pltpu.CompilerParams(collective_id=0, has_side_effects=True),
        name="forward_solve",
    )(right_side, inverse_t, u_factor, v_factor, ranks.reshape(per_col))


def solution(mesh):
    placed = (
        P(None, "row", None, None),
        P(None, "row", "col", None),
        P(None, "row", None, "col", None, None),
        P(None, "row", None, "col", None, None),
        P(None, "row", None, "col"),
    )
    return jax.shard_map(
        functools.partial(local, mesh.shape["row"], mesh.shape["col"]),
        mesh=mesh,
        in_specs=placed,
        out_specs=(P(None, "row", None, None), P(None, "row", None)),
        check_vma=False,
    )
```

```python
import functools
import math

import jax
import jax.numpy as jnp
from jax import lax
from jax.experimental import pallas as pl
from jax.experimental.pallas import tpu as pltpu
from jax.sharding import PartitionSpec as P

MESH = pl.DeviceIdType.MESH
NT = (((1,), (1,)), ((), ()))
FIRST_SHORT = 3
NEAR = 3


def remote(src, dst, send_sem, recv_sem, device):
    return pltpu.make_async_remote_copy(
        src_ref=src,
        dst_ref=dst,
        send_sem=send_sem,
        recv_sem=recv_sem,
        device_id=device,
        device_id_type=MESH,
    )


def kernel(
    n_row, n_col,
    rhs_hbm, inv_hbm, u_hbm, v_hbm, rank_hbm,
    white_ref, lik_ref,
    rhs_ref, inv_ref, u_ref, v_ref, rank_ref,
    y_in, p_out, p_in, y_row, logs, base, y_full, y_all, tally,
    v_out, v_in, u_out, u_in, fold, w_out, w_in,
    x_out, x_in, t_out, t_in, fold_x, wx_out, wx_in,
    d_out, d_in, d_tile, vt_ref, l2_in, w2_out, w2_in, l_out, l_in, wl_out, wl_in, we_in,
    a_out, a_in, a_sum,
    hl_in, hu_in, hf_in, hv_out, hv_in, hv_tile, hb_out, hb_in, hz_out, hz_in, hw_out, hw_in, hy_out, fold_b, fold_xb,
    in_sem, y_send, y_recv, p_send, p_recv, o_send, o_recv, l_send, l_recv,
    v_send, v_recv, u_send, u_recv, w_send, w_recv, m_recv, f_send, e_send, ready, ready_far, pass_send,
    t_recv, k_recv, d_send, d_recv, du_recv, wl_send, wl_recv, wp_send,
    we_send, we_recv, wx_send, wx_recv, a_send, a_recv,
):
    row = lax.axis_index("row")
    col = lax.axis_index("col")
    per_col, rank_max, width = u_ref.shape
    nrhs = rhs_ref.shape[0]
    piece = width // n_col
    half = n_col // 2
    y_sends = y_send.shape[0]
    some = half
    peers = [lax.rem(col + k, n_col) for k in range(1, n_col)]
    others = pl.ds(0, n_col - 1)
    own_slot = row // n_col
    own_home = lax.rem(row, n_col)
    end = n_row - 1
    even_end = n_row - 2
    ahead = n_row - 3

    def longs_of(i):
        count = jnp.where(i >= FIRST_SHORT, i - 1, i)
        handed = (lax.rem(i, 2) == 0) & (i >= 2)
        return count - jnp.where(handed, 1, 0) - jnp.where(i >= even_end, 1, 0)

    def near_of(i):
        return jnp.where(i == 0, 1, NEAR + jnp.where(i >= 2, 1, 0))

    copies = [
        pltpu.make_async_copy(v_hbm.at[0, 0, :, 0], v_ref, in_sem.at[0]),
        pltpu.make_async_copy(u_hbm.at[0, 0, :, 0], u_ref, in_sem.at[1]),
        None,
        pltpu.make_async_copy(rhs_hbm.at[0, 0], rhs_ref, in_sem.at[3]),
        pltpu.make_async_copy(rank_hbm, rank_ref, in_sem.at[4]),
    ]
    @pl.when(lax.axis_index("row") > 0)
    def _():
        copies[0].start()
        copies[1].start()

    def tail_of(c):
        start = c * piece // 128 * 128
        return pl.ds(start, width - start)

    def inverse_copy(c):
        return pltpu.make_async_copy(inv_hbm.at[0, 0, :, tail_of(c)], inv_ref.at[:, tail_of(c)], in_sem.at[2])

    def by_col(act):
        for c in range(n_col):
            pl.when(col == c)(functools.partial(act, c))

    by_col(lambda c: inverse_copy(c).start())
    for copy in copies[3:]:
        copy.start()
    barrier = pltpu.get_barrier_semaphore()

    def signal(sem, i, s):
        pl.semaphore_signal(sem, inc=1, device_id=(i, s), device_id_type=MESH)

    for peer in peers:
        signal(barrier, row, peer)

    def set_base():
        for cc in range(n_col):

            @pl.when(col == cc)
            def _():
                base[...] = rhs_ref[:, cc * piece:(cc + 1) * piece]

    def own_part(c, reduced):
        tail = tail_of(c)
        y_row[c, :, tail] = jnp.dot(reduced, inv_ref[:, tail], preferred_element_type=jnp.float32)

    def near_copy(i, c):
        tail = tail_of(c)
        sem = y_send.at[lax.rem(i - row - 1, y_sends)]
        return remote(y_row.at[c, :, tail], y_in.at[own_slot, c, :, tail], sem, y_recv.at[own_slot], (i, own_home))

    first = row == 0

    @pl.when(first)
    def _():
        for s in range(n_col):
            signal(barrier, 1, s)
        copies[3].wait()
        by_col(lambda c: inverse_copy(c).wait())
        set_base()
        reduced = base[...].astype(jnp.bfloat16)
        by_col(lambda c: own_part(c, reduced))
        pl.semaphore_wait(barrier, 2 * n_col - 1)
        by_col(lambda c: near_copy(1, c).start())

    for s in range(1, n_col):
        start = s * piece // 128 * 128
        if start:
            y_row[s, :, :start] = jnp.zeros((nrhs, start), jnp.float32)
            for q in range(per_col):
                y_in[q, s, :, :start] = jnp.zeros((nrhs, start), jnp.float32)

    even = lax.rem(row, 2) == 0
    short = row >= FIRST_SHORT
    feeds = (row + 1 >= FIRST_SHORT) & (row < end)
    is_end = row == end
    is_even_end = row == even_end
    is_ahead = row == ahead
    lent = row == ahead - 1
    before = row == ahead - 2
    long_count = longs_of(row)
    near_end = jnp.minimum(row + near_of(row) + 1, n_row)
    relays = (col == own_home) & (row > 0)
    passes = (row == 1) & (col == 0)

    def row_of(i, cond, act):
        @pl.when(cond)
        def _():
            for s in range(n_col):
                act(i, s)

        return jnp.where(cond, n_col, 0)

    def above(act):
        yield row + 1, row_of(row + 1, (row > 0) & (row < end), act)
        for d in range(2, NEAR + 2):
            wide = (is_ahead | before) if d == 2 else jnp.bool_(False)
            one = (row + d < n_row) & (d <= near_of(row)) & jnp.logical_not(wide)

            @pl.when(one)
            def _():
                act(row + d, own_home)

            yield row + d, jnp.where(one, 1, 0)
            if d == 2:
                yield row + d, row_of(row + d, wide, act)

    def below(act, act_far=None):
        row_of(row - 1, row > 0, act)
        count = jnp.where(row > 0, n_col, 0)
        for d in range(2, NEAR + 2):
            fed = (row >= d) & (d <= near_of(row - d)) & (lax.rem(jnp.maximum(row - d, 0), n_col) == col)
            if d == 2:
                fed = fed | is_end | is_ahead
            count += row_of(row - d, fed, act)
        for q in range(per_col):
            j = q * n_col + col
            far = j < row - near_of(j)

            source = jnp.where(j == 0, 1, j)
            soon = (j == 0) & (row <= 3)

            @pl.when(far & soon)
            def _():
                act(source, col)

            @pl.when(far & jnp.logical_not(soon))
            def _():
                (act_far or act)(source, col)

            count += jnp.where(far, 1, 0)
        return count

    def at_once(low, high):
        return (low == 0) & (high == 1)

    greeted = jnp.int32(n_col - 1)
    answers = jnp.int32(0)
    for i, count in above(lambda i, s: signal(barrier, i, s)):
        answers += count

    def greet_far(i, count):
        signal(barrier, i, col)
        return count + 1

    far_answers = lax.fori_loop(jnp.where(relays, near_end, n_row), n_row, greet_far, jnp.int32(0))
    far_answers = lax.fori_loop(jnp.where(passes, 4, n_row), n_row, greet_far, far_answers)
    answers = lax.fori_loop(jnp.where(passes, 2, n_row), jnp.where(passes, 4, n_row), greet_far, answers)

    def greet_quick(i, s):
        @pl.when(at_once(i, row))
        def _():
            signal(barrier, i, s)

    def answer(i, s):
        @pl.when(jnp.logical_not(at_once(i, row)))
        def _():
            signal(ready, i, s)

    greeted += below(greet_quick)

    prev = jnp.maximum(row - 1, 0)
    prev_slot = prev // n_col
    prev_home = lax.rem(prev, n_col)
    gives = short & (col == prev_home)
    crosses = short & even
    far_slot = ahead // n_col
    far_home = ahead % n_col
    gives_far = is_end & (col == far_home)
    handed = even & (row >= 2)
    mine = jnp.where(handed, long_count + jnp.where(is_even_end, 1, 0), 0)
    mine_slot = mine // n_col
    mine_home = lax.rem(mine, n_col)
    hands = handed & (col == mine_home)
    taken = (row >= 3) & jnp.logical_not(even)
    theirs = jnp.where(taken, longs_of(prev) + jnp.where(is_end, 1, 0), 0)
    their_home = lax.rem(theirs, n_col)
    takes = taken & (col == their_home)
    whole = even_end - 3
    whole_slot = whole // n_col
    whole_home = whole % n_col
    hands_whole = is_even_end & (col == whole_home)
    takes_whole = is_end & (col == whole_home)

    def masked_u(slot):
        keep = lax.broadcasted_iota(jnp.int32, (rank_max, width), 0) < rank_ref[slot]
        return jnp.where(keep, u_ref[slot].astype(jnp.float32), 0.0)

    def cut(tile, into):
        for s in range(n_col):
            into[s] = tile[:, s * piece:(s + 1) * piece]

    @pl.when(row > 0)
    def _():
        copies[0].wait()
        copies[1].wait()

    copies[4].wait()

    @pl.when(hands)
    def _():
        d_out[...] = v_ref[mine_slot].astype(jnp.float32)
        cut(masked_u(mine_slot), l_out)

    @pl.when(hands_whole)
    def _():
        d_out[...] = v_ref[whole_slot].astype(jnp.float32)
        cut(masked_u(whole_slot), l_out)

    @pl.when(gives)
    def _():
        cut(v_ref[prev_slot].astype(jnp.float32), v_out)
        cut(masked_u(prev_slot), u_out)

    @pl.when(gives_far)
    def _():
        cut(v_ref[far_slot].astype(jnp.float32), x_out)
        cut(masked_u(far_slot), t_out)

    @pl.when(row > 0)
    def _():
        pl.semaphore_wait(barrier, greeted)

    below(answer, lambda i, s: signal(ready_far, i, s))

    def by_way(home, s, cc):
        across = n_col - 1 - home
        return (home != s) & jnp.where(
            across < home,
            jnp.where(across == s, cc < s + some, (home != s + 1) | (cc == s)),
            (s > home) | (cc < s + half),
        )

    def is_late(home, s, cc):
        across = n_col - 1 - home
        return (across == s) & (across < home) & (cc >= s + some)

    def beside(home, s):
        return split_row(home) & (home == s + 1) & (n_col - 1 - home != s)

    def split_row(home):
        return n_col - 1 - home < home

    def is_split(home, s):
        across = n_col - 1 - home
        return (across == s) & (across < home)

    def joined(home, s):
        across = n_col - 1 - home
        return (across > home) & (across == s)

    def spread(out, into, recv, target, home, cross):
        for s in range(n_col):
            for cc in range(s, min(s + some, n_col)):

                @pl.when(cross & is_split(home, s))
                def _():
                    remote(out.at[cc], out.at[cc], v_send.at[s], m_recv.at[cc], (row, s)).start()

        for s in range(n_col):
            if s > 0:

                @pl.when(cross & joined(home, s - 1))
                def _():
                    remote(out.at[s - 1], out.at[s - 1], v_send.at[s], m_recv.at[s - 1], (row, s)).start()

            for cc in range(s, n_col):
                gone = cross & (joined(home, s) | is_split(home, s))
                way = cross & by_way(home, s, cc)
                later = cross & is_late(home, s, cc)

                @pl.when(way & jnp.logical_not(gone))
                def _():
                    remote(out.at[cc], out.at[cc], v_send.at[s], m_recv.at[cc], (row, s)).start()

                @pl.when(jnp.logical_not(way | later | gone))
                def _():
                    remote(out.at[cc], into.at[cc], v_send.at[s], recv.at[cc], (target, s)).start()

    def spread_late(out, into, recv, target, home):
        for s in range(n_col):

            @pl.when(split_row(home) & (n_col - home == s))
            def _():
                part = pl.ds(s, n_col - s)
                remote(out.at[part], out.at[part], v_send.at[s], m_recv.at[0], (row, s)).wait_send()

        for s in range(n_col):
            for cc in range(min(s + some, n_col), n_col):

                @pl.when(is_late(home, s, cc))
                def _():
                    remote(out.at[cc], into.at[cc], v_send.at[s], recv.at[cc], (target, s)).start()

    def spread_done(out, home, cross):
        for s in range(n_col):
            part = pl.ds(s, n_col - s)
            gone = cross & joined(home, s)
            gone = gone | (cross & split_row(home) & (n_col - home == s))
            more = (cross & joined(home, s - 1)) if s > 0 else jnp.bool_(False)

            @pl.when(jnp.logical_not(gone | more))
            def _():
                remote(out.at[part], out.at[part], v_send.at[s], m_recv.at[0], (row, s)).wait_send()

            if s > 0:
                part_more = pl.ds(s - 1, n_col - s + 1)

                @pl.when(more)
                def _():
                    remote(out.at[part_more], out.at[part_more], v_send.at[s], m_recv.at[0], (row, s)).wait_send()

    def relay(out, into, recv, target, home):
        across = n_col - 1 - home
        more = joined(home, col - 1)
        first = jnp.where(more, col - 1, col)
        part = jnp.where(across < home, across == col, col < home)
        share_of = jnp.where(across < home, some, half)
        stop = jnp.where(part, jnp.minimum(col + share_of, n_col), n_col)
        stop = jnp.where(joined(home, col) | beside(home, col), col + 1, stop)

        def forward(cc, carry):
            remote(out.at[cc], out.at[cc], v_send.at[0], m_recv.at[cc], (row, home)).wait_recv()

            @pl.when(cc >= col)
            def _():
                remote(out.at[cc], into.at[cc], f_send, recv.at[cc], (target, col)).start()

            @pl.when(more & (cc == across))
            def _():
                remote(out.at[cc], out.at[cc], e_send, m_recv.at[cc], (row, across)).start()

            @pl.when(more & (cc > across))
            def _():
                remote(out.at[cc], into.at[cc], e_send, recv.at[cc], (target, across)).start()

            return carry

        lax.fori_loop(first, stop, forward, 0)

    def relay_done(out, home):
        across = n_col - 1 - home
        for cc in range(n_col):
            here = col == cc
            half_way = jnp.where(across < home, across == cc, cc < home)

            @pl.when(here & (joined(home, cc) | beside(home, cc)))
            def _():
                remote(out.at[cc], out.at[cc], f_send, v_recv.at[0], (row, home)).wait_send()

            @pl.when(here & jnp.logical_not(half_way | joined(home, cc) | beside(home, cc)))
            def _():
                part = pl.ds(cc, n_col - cc)
                remote(out.at[part], out.at[part], f_send, v_recv.at[0], (row, home)).wait_send()

            for count, cond in ((some, across < home), (half, across > home)):
                few = pl.ds(cc, min(count, n_col - cc))

                @pl.when(here & half_way & cond)
                def _():
                    remote(out.at[few], out.at[few], f_send, v_recv.at[0], (row, home)).wait_send()

            if cc > 0:

                @pl.when((col == cc) & joined(home, cc - 1))
                def _():
                    part = pl.ds(cc - 1, n_col - cc + 1)
                    remote(out.at[part], out.at[part], e_send, v_recv.at[0], (row, home)).wait_send()

    def share(out, into, recv):
        for k in range(n_col):
            peer = lax.rem(2 * n_col - 1 - col + k, n_col)

            @pl.when(peer != col)
            def _():
                remote(out.at[peer], into, u_send, recv, (row, peer)).start()

        into[...] = out[col]

    def share_done(out):
        remote(out.at[others], out.at[others], u_send, u_recv, (row, peers[0])).wait_send()

    def shared_wait(into, recv, home):
        @pl.when(col != home)
        def _():
            remote(into, into, u_send, recv, (row, home)).wait_recv()

    early_l = (row < FIRST_SHORT) | is_even_end

    opposite = n_col - 1 - col

    @pl.when(hands)
    def _():
        for peer in peers:

            @pl.when(early_l | (peer != opposite))
            def _():
                remote(l_out.at[peer], l_in, u_send, k_recv, (row, peer)).start()

        l_in[...] = l_out[col]

    @pl.when(hands_whole)
    def _():
        share(l_out, l2_in, du_recv)

    @pl.when(gives)
    def _():
        spread(v_out, v_in, v_recv, row - 1, prev_home, crosses)

    @pl.when(gives & (is_even_end | jnp.logical_not(even)))
    def _():
        share(u_out, u_in, u_recv)

    @pl.when(gives_far)
    def _():
        spread(x_out, x_in, m_recv, row - 2, far_home, jnp.bool_(True))

    @pl.when((handed) & (answers > 0))
    def _():
        pl.semaphore_wait(ready, answers)

    @pl.when(hands | hands_whole)
    def _():
        remote(d_out, d_in, d_send, d_recv, (row + 1, col)).start()

    relays_late = is_even_end & joined(prev_home, col)

    @pl.when(crosses & (col != prev_home) & jnp.logical_not(relays_late))
    def _():
        relay(v_out, v_in, v_recv, row - 1, prev_home)

    @pl.when(row > 0)
    def _():
        by_col(lambda c: inverse_copy(c).wait())
        copies[3].wait()


    def lend(src, dst, send, recv):
        return remote(src, dst, send, recv, (row + 1, col))

    def lend_inverse(c):
        return lend(hv_out.at[:, tail_of(c)], hv_in.at[:, tail_of(c)], wl_send, wx_recv)

    def lend_tail(c):
        hv_out[:, tail_of(c)] = inv_ref[:, tail_of(c)].astype(jnp.float32)
        lend_inverse(c).start()

    pl.when(lent)(functools.partial(by_col, lend_tail))

    pl.when(row > 0)(set_base)

    def log_part():
        for cc in range(n_col):

            @pl.when(col == cc)
            def _():
                block = inv_ref[:, cc * piece:(cc + 1) * piece].astype(jnp.float32)
                r_id = lax.broadcasted_iota(jnp.int32, (piece, piece), 0)
                c_id = lax.broadcasted_iota(jnp.int32, (piece, piece), 1)
                diagonal = jnp.sum(jnp.where(r_id == c_id, block, 0.0), axis=0, keepdims=True)
                total = jnp.sum(jnp.log(diagonal), axis=1, keepdims=True)
                logs[cc] = jnp.broadcast_to(total, (1, 128))

        for peer in peers:
            remote(logs.at[col], logs.at[col], l_send, l_recv, (row, peer)).start()

    pl.when(row > 0)(log_part)

    for q in range(per_col):

        @pl.when(q * n_col + col < long_count)
        def _():
            vt_ref[q] = v_ref[q].astype(jnp.float32).T.astype(jnp.bfloat16)

    @pl.when(gives & crosses)
    def _():
        spread_late(v_out, v_in, v_recv, row - 1, prev_home)

    @pl.when(gives & crosses & jnp.logical_not(is_even_end))
    def _():
        share(u_out, u_in, u_recv)

    @pl.when(hands & jnp.logical_not(early_l))
    def _():
        remote(l_out.at[opposite], l_in, u_send, k_recv, (row, opposite)).start()

    def fold_with(into, recv, target):
        target[...] = jnp.zeros_like(target)
        for cc in range(n_col):

            @pl.when(col <= cc)
            def _():
                remote(into.at[cc], into.at[cc], f_send, recv.at[cc], (row, cc)).wait_recv()
                target[...] += lax.dot_general(
                    inv_ref[:, cc * piece:(cc + 1) * piece],
                    into[cc].astype(jnp.bfloat16),
                    NT,
                    preferred_element_type=jnp.float32,
                )

    def long_step(q, cond):
        j = q * n_col + col

        @pl.when((j < long_count) & cond)
        def _():
            near = row - j <= near_of(j)

            @pl.when(near)
            def _():
                remote(tally, tally, y_send.at[0], y_recv.at[q], (j, col)).wait_recv()
                y = y_in[q, 0]
                for s in range(1, n_col):
                    y = y + y_in[q, s]
                y_full[...] = y

            @pl.when(jnp.logical_not(near))
            def _():
                remote(y_in.at[q, 0], y_in.at[q, 0], y_send.at[0], y_recv.at[q], (j, col)).wait_recv()
                y_full[...] = y_in[q, 0]

            y = y_full[...].astype(jnp.bfloat16)

            @pl.when(takes & (j == theirs))
            def _():
                wl_out[...] = jnp.dot(y, d_tile[...], preferred_element_type=jnp.float32)
                @pl.when(jnp.logical_not(is_ahead))
                def _():
                    for s in range(n_col):
                        remote(wl_out, wl_in, wl_send, wl_recv, (row - 1, s)).start()

                @pl.when(is_end | is_ahead)
                def _():
                    for peer in peers:
                        remote(wl_out, wl_in, wp_send, wl_recv, (row, peer)).start()
                    wl_in[...] = wl_out[...]

            @pl.when(takes_whole & (j == whole))
            def _():
                w2_out[...] = jnp.dot(y, d_tile[...], preferred_element_type=jnp.float32)
                for s in range(n_col):
                    remote(w2_out, w2_in, wl_send, p_recv.at[whole], (row - 1, s)).start()
                for peer in peers:
                    remote(w2_out, w2_in, wp_send, k_recv, (row, peer)).start()
                w2_in[...] = w2_out[...]

            inner = jnp.dot(y, vt_ref[q], preferred_element_type=jnp.float32)
            keep = lax.broadcasted_iota(jnp.int32, (nrhs, rank_max), 1) < rank_ref[q]
            inner = jnp.where(keep, inner, 0.0).astype(jnp.bfloat16)
            p = jnp.dot(inner, u_ref[q], preferred_element_type=jnp.float32)
            for s in range(n_col):
                p_out[q, s] = p[:, s * piece:(s + 1) * piece]
            for peer in peers:
                remote(p_out.at[q, peer], p_in.at[j], p_send.at[q], p_recv.at[j], (row, peer)).start()
            p_in[j] = p_out[q, col]

    def products():
        fold_with(v_in, v_recv, fold)
        factor = fold[...].astype(jnp.bfloat16)
        fold_b[...] = factor
        shared_wait(u_in, u_recv, prev_home)
        shared_wait(l_in, k_recv, mine_home)
        a_out[0] = jnp.dot(u_in[...].astype(jnp.bfloat16), factor, preferred_element_type=jnp.float32)
        a_out[1] = jnp.dot(l_in[...].astype(jnp.bfloat16), factor, preferred_element_type=jnp.float32)
        shared_wait(l2_in, du_recv, whole_home)
        a_out[2] = jnp.dot(l2_in[...].astype(jnp.bfloat16), factor, preferred_element_type=jnp.float32)
        for k in range(3):
            for s in range(n_col):
                remote(a_out.at[k], a_in.at[k, col], a_send, a_recv, (row + 1, s)).start()

    @pl.when(relays_late)
    def _():
        products()
        relay(v_out, v_in, v_recv, row - 1, prev_home)

    @pl.when(takes | takes_whole)
    def _():
        remote(d_in, d_in, d_send, d_recv, (row - 1, col)).wait_recv()
        d_tile[...] = d_in[...].T.astype(jnp.bfloat16)

    @pl.when(is_end & (col != far_home))
    def _():
        relay(x_out, x_in, m_recv, row - 2, far_home)

    for q in range(per_col):
        long_step(q, jnp.logical_not(is_ahead & (q * n_col + col == row - 2)))

    def pass_on(i, carry):
        remote(y_full, y_in.at[0, 0], pass_send, y_recv.at[0], (i, 0)).start()
        return carry

    @pl.when(passes)
    def _():
        pl.semaphore_wait(ready, answers)
        lax.fori_loop(2, 4, pass_on, 0)

    def send_w(out, into, send, recv, i):
        for s in range(n_col):
            remote(out, into.at[col], send, recv, (i, s)).start()

    def wait_w(into, send, recv, i):
        remote(into, into, send, recv, (i, 0)).wait_recv()
        total = into[0]
        for s in range(1, n_col):
            total = total + into[s]
        return total

    def borrowed_y(c):
        tail = tail_of(c)
        slot = (ahead - 1) // n_col
        home = (ahead - 1) % n_col
        return remote(hy_out.at[:, tail], y_in.at[slot, c, :, tail], y_send.at[0], y_recv.at[slot], (end, home))

    @pl.when(is_ahead)
    def _():
        back = (row - 1, col)
        by_col(lambda c: remote(hv_in.at[:, tail_of(c)], hv_in.at[:, tail_of(c)], wl_send, wx_recv, back).wait_recv())
        by_col(lambda c: hv_tile.__setitem__((slice(None), tail_of(c)), hv_in[:, tail_of(c)].astype(jnp.bfloat16)))
        remote(hl_in, hl_in, a_send, k_recv, back).wait_recv()
        remote(hu_in, hu_in, we_send, a_recv, back).wait_recv()
        remote(hf_in, hf_in, wx_send, we_recv, back).wait_recv()
        remote(hb_in, hb_in, wp_send, t_recv, back).wait_recv()
        l_part = hl_in[...].astype(jnp.bfloat16)
        u_part = hu_in[...].astype(jnp.bfloat16)
        factor = hf_in[...].astype(jnp.bfloat16)

        @pl.when(answers > 0)
        def _():
            pl.semaphore_wait(ready, answers)

        @pl.when(jnp.logical_not(takes))
        def _():
            remote(wl_in, wl_in, wp_send, wl_recv, (row, their_home)).wait_recv()

        part = hb_in[...] - jnp.dot(wl_in[...].astype(jnp.bfloat16), l_part, preferred_element_type=jnp.float32)
        inner = wait_w(hw_in, w_send, du_recv, row - 2)
        part -= jnp.dot(inner.astype(jnp.bfloat16), u_part, preferred_element_type=jnp.float32)
        part = part.astype(jnp.bfloat16)
        def borrowed_part(c):
            tail = tail_of(c)
            hy_out[:, tail] = jnp.dot(part, hv_tile[:, tail], preferred_element_type=jnp.float32)
            borrowed_y(c).start()

        by_col(borrowed_part)
        hw_out[...] = jnp.dot(part, factor, preferred_element_type=jnp.float32)
        for peer in peers:
            remote(hw_out, w_in.at[col], a_send, w_recv, (row, peer)).start()
        w_in[col] = hw_out[...]

        hz_out[...] = part.astype(jnp.float32)
        remote(hz_out, hz_in, wl_send, du_recv, back).start()

    for q in range(per_col):
        long_step(q, is_ahead & (q * n_col + col == row - 2))

    pl.when(is_even_end & jnp.logical_not(relays_late))(products)

    @pl.when(feeds & jnp.logical_not(is_even_end))
    def _():
        fold_with(v_in, v_recv, fold)
        fold_b[...] = fold[...].astype(jnp.bfloat16)

        @pl.when(lent)
        def _():
            lend(fold, hf_in, wx_send, we_recv).start()

    @pl.when(gives_far)
    def _():
        spread_late(x_out, x_in, m_recv, row - 2, far_home)
        share(t_out, t_in, t_recv)

    @pl.when(is_ahead)
    def _():
        fold_with(x_in, m_recv, fold_x)
        fold_xb[...] = fold_x[...].astype(jnp.bfloat16)

    @pl.when(is_end)
    def _():
        remote(a_in, a_in, a_send, a_recv, (row - 1, 0)).wait_recv()
        for k in range(3):
            total = a_in[k, 0]
            for s in range(1, n_col):
                total = total + a_in[k, s]
            a_sum[k] = total.astype(jnp.bfloat16)

    def gather_p(j, acc):
        home = lax.rem(j, n_col)

        @pl.when(home != col)
        def _():
            remote(p_in.at[j], p_in.at[j], p_send.at[0], p_recv.at[j], (row, home)).wait_recv()

        return acc - p_in[j]

    base[...] = lax.fori_loop(0, long_count - jnp.where(is_ahead, 1, 0), gather_p, base[...])

    @pl.when(lent)
    def _():
        hb_out[...] = base[...]
        lend(hb_out, hb_in, wp_send, t_recv).start()
        shared_wait(l_in, k_recv, mine_home)
        lend(l_in, hl_in, a_send, k_recv).start()
        shared_wait(u_in, u_recv, prev_home)
        lend(u_in, hu_in, we_send, a_recv).start()
        remote(hz_in, hz_in, wl_send, du_recv, (row + 1, col)).wait_recv()
        base[...] = hz_in[...]

    @pl.when(is_even_end)
    def _():
        w_out[...] = jnp.dot(base[...].astype(jnp.bfloat16), fold_b[...], preferred_element_type=jnp.float32)
        send_w(w_out, w_in, w_send, w_recv, row + 1)

    @pl.when(handed & jnp.logical_not(lent))
    def _():
        @pl.when(jnp.logical_not(is_even_end))
        def _():
            shared_wait(l_in, k_recv, mine_home)

        l_part = l_in[...].astype(jnp.bfloat16)

        @pl.when(is_even_end)
        def _():
            remote(w2_in, w2_in, wl_send, p_recv.at[whole], (row + 1, whole_home)).wait_recv()
            base[...] -= jnp.dot(
                w2_in[...].astype(jnp.bfloat16), l2_in[...].astype(jnp.bfloat16), preferred_element_type=jnp.float32
            )

        remote(wl_in, wl_in, wl_send, wl_recv, (row + 1, mine_home)).wait_recv()
        base[...] -= jnp.dot(wl_in[...].astype(jnp.bfloat16), l_part, preferred_element_type=jnp.float32)

    @pl.when(is_ahead)
    def _():
        shared_wait(u_in, u_recv, prev_home)
        u_part = u_in[...].astype(jnp.bfloat16)
        part = w_in.at[others]
        remote(part, part, a_send, w_recv, (row, peers[0])).wait_recv()
        inner = w_in[0]
        for s in range(1, n_col):
            inner = inner + w_in[s]
        part = base[...] - jnp.dot(inner.astype(jnp.bfloat16), u_part, preferred_element_type=jnp.float32)
        base[...] = gather_p(row - 2, part)

    @pl.when(short & jnp.logical_not(is_end | is_ahead | lent))
    def _():
        @pl.when(jnp.logical_not(is_even_end))
        def _():
            shared_wait(u_in, u_recv, prev_home)

        u_part = u_in[...].astype(jnp.bfloat16)
        inner = wait_w(w_in, w_send, w_recv, row - 1)
        base[...] -= jnp.dot(inner.astype(jnp.bfloat16), u_part, preferred_element_type=jnp.float32)

    @pl.when(is_end)
    def _():
        shared_wait(u_in, u_recv, prev_home)
        shared_wait(t_in, t_recv, far_home)
        u_part = u_in[...].astype(jnp.bfloat16)
        t_part = t_in[...].astype(jnp.bfloat16)
        carried = -jnp.dot(a_sum[0], u_part, preferred_element_type=jnp.float32)
        both = jnp.concatenate([carried.astype(jnp.bfloat16), t_part])

        @pl.when(jnp.logical_not(takes))
        def _():
            remote(wl_in, wl_in, wp_send, wl_recv, (row, their_home)).wait_recv()

        @pl.when(jnp.logical_not(takes_whole))
        def _():
            remote(w2_in, w2_in, wp_send, k_recv, (row, whole_home)).wait_recv()

        inner = wait_w(w_in, w_send, w_recv, row - 1)
        inner -= jnp.dot(w2_in[...].astype(jnp.bfloat16), a_sum[2], preferred_element_type=jnp.float32)
        inner -= jnp.dot(wl_in[...].astype(jnp.bfloat16), a_sum[1], preferred_element_type=jnp.float32)
        part = base[...] - jnp.dot(inner.astype(jnp.bfloat16), u_part, preferred_element_type=jnp.float32)
        late = [wait_w(we_in, we_send, we_recv, row - 2), wait_w(wx_in, wx_send, wx_recv, row - 2)]
        late = jnp.concatenate(late, axis=1).astype(jnp.bfloat16)
        base[...] = part - jnp.dot(late, both, preferred_element_type=jnp.float32)

    reduced = base[...].astype(jnp.bfloat16)

    @pl.when(jnp.logical_not(even | is_ahead | passes) & (answers > 0))
    def _():
        pl.semaphore_wait(ready, answers)

    @pl.when(feeds & jnp.logical_not(is_even_end | lent))
    def _():
        w_out[...] = jnp.dot(reduced, fold_b[...], preferred_element_type=jnp.float32)

        @pl.when(is_ahead)
        def _():
            send_w(w_out, w_in, w_send, w_recv, row + 1)
            send_w(w_out, we_in, we_send, we_recv, row + 2)
            wx_out[...] = jnp.dot(reduced, fold_xb[...], preferred_element_type=jnp.float32)
            send_w(wx_out, wx_in, wx_send, wx_recv, row + 2)

        @pl.when(before)
        def _():
            send_w(w_out, hw_in, w_send, du_recv, row + 2)

        @pl.when(jnp.logical_not(before | is_ahead))
        def _():
            send_w(w_out, w_in, w_send, w_recv, row + 1)

    @pl.when(row > 0)
    def _():
        by_col(lambda c: own_part(c, reduced))

    def send_y(i, carry):
        @pl.when((row < longs_of(i)) & jnp.logical_not(lent))
        def _():
            by_col(lambda c: near_copy(i, c).start())

        return carry

    def own_copy(c, peer):
        part = y_row.at[c, :, tail_of(c)]
        return remote(part, part, o_send, o_recv, (row, peer))

    lax.fori_loop(row + 1, jnp.where(first, 0, near_end), send_y, 0)
    for peer in peers:
        by_col(lambda c: own_copy(c, peer).start())

    @pl.when(first)
    def _():
        log_part()

    remote(logs.at[others], logs.at[others], l_send, l_recv, (row, peers[0])).wait()
    log_sum = logs[0]
    for s in range(1, n_col):
        log_sum = log_sum + logs[s]
    log_term = log_sum * (1.0 / width) - 0.5 * math.log(2.0 * math.pi)

    def left_y(i, carry):
        @pl.when((row < longs_of(i)) & jnp.logical_not(lent))
        def _():
            by_col(lambda c: near_copy(i, c).wait_send())

        return carry

    lax.fori_loop(row + 1, near_end, left_y, 0)

    @pl.when(feeds & jnp.logical_not(lent))
    def _():
        remote(w_in, w_in, w_send, w_recv, (row + 1, 0)).wait_send()

    @pl.when(lent)
    def _():
        by_col(lambda c: lend_inverse(c).wait_send())
        lend(fold, hf_in, wx_send, we_recv).wait_send()
        lend(hb_out, hb_in, wp_send, t_recv).wait_send()
        lend(l_in, hl_in, a_send, k_recv).wait_send()
        lend(u_in, hu_in, we_send, a_recv).wait_send()

    @pl.when(is_ahead)
    def _():
        part = w_in.at[others]
        remote(part, part, a_send, w_recv, (row, peers[0])).wait_send()
        by_col(lambda c: borrowed_y(c).wait_send())
        remote(hz_out, hz_in, wl_send, du_recv, (row - 1, col)).wait_send()
        remote(w_in, w_in, we_send, we_recv, (row + 2, 0)).wait_send()
        remote(w_in, w_in, wx_send, wx_recv, (row + 2, 0)).wait_send()

    @pl.when(is_even_end)
    def _():
        remote(a_in, a_in, a_send, a_recv, (row + 1, 0)).wait_send()

    @pl.when(takes)
    def _():
        @pl.when(jnp.logical_not(is_ahead))
        def _():
            remote(w_in, w_in, wl_send, wl_recv, (row - 1, 0)).wait_send()

        @pl.when(is_end | is_ahead)
        def _():
            remote(w_in.at[others], w_in.at[others], wp_send, wl_recv, (row, peers[0])).wait_send()

    @pl.when(hands)
    def _():
        remote(d_out, d_in, d_send, d_recv, (row + 1, col)).wait_send()
        share_done(l_out)

    @pl.when(hands_whole)
    def _():
        remote(d_out, d_in, d_send, d_recv, (row + 1, col)).wait_send()
        share_done(l_out)

    @pl.when(takes_whole)
    def _():
        remote(w_in, w_in, wl_send, p_recv.at[0], (row - 1, 0)).wait_send()
        remote(w_in.at[others], w_in.at[others], wp_send, k_recv, (row, peers[0])).wait_send()

    @pl.when(gives)
    def _():
        spread_done(v_out, prev_home, crosses)
        share_done(u_out)

    @pl.when(gives_far)
    def _():
        spread_done(x_out, far_home, jnp.bool_(True))
        share_done(t_out)

    @pl.when(crosses & (col != prev_home))
    def _():
        relay_done(v_out, prev_home)

    @pl.when(is_end & (col != far_home))
    def _():
        relay_done(x_out, far_home)

    for q in range(per_col):

        @pl.when(q * n_col + col < long_count)
        def _():
            part = p_out.at[q, others]
            remote(part, part, p_send.at[q], p_recv.at[0], (row, peers[0])).wait_send()

    def wait_others(c):
        part = tally.at[pl.ds(0, tally.shape[0] - tail_of(c).size // 128)]
        remote(part, part, o_send, o_recv, (row, peers[0])).wait_recv()

    by_col(wait_others)
    y = y_row[0]
    for s in range(1, n_col):
        y = y + y_row[s]
    y_all[...] = y

    def far_copy(i):
        return remote(y_all, y_in.at[own_slot, 0], y_send.at[lax.rem(i - row - 1, y_sends)], y_recv.at[own_slot], (i, col))

    def send_far(i, carry):
        far_copy(i).start()
        return carry

    @pl.when(far_answers > 0)
    def _():
        pl.semaphore_wait(ready_far, far_answers)

    @pl.when(passes)
    def _():
        lax.fori_loop(4, n_row, pass_on, 0)
        part = y_in.at[:, pl.ds(0, (n_row - 2) // per_col)]
        remote(part, part, pass_send, y_recv.at[0], (2, 0)).wait_send()

    lax.fori_loop(jnp.where(relays, near_end, n_row), n_row, send_far, 0)
    white_ref[0, 0] = y
    quadratic = jnp.sum(y * y, axis=1, keepdims=True) * (1.0 / width)
    lik = -0.5 * quadratic + log_term
    r_id = lax.broadcasted_iota(jnp.int32, (nrhs, 128), 0)
    c_id = lax.broadcasted_iota(jnp.int32, (nrhs, 128), 1)
    flat = jnp.sum(jnp.where(r_id == c_id, lik, 0.0), axis=0, keepdims=True)
    lik_ref[0] = flat[:, :nrhs]

    def left_far(i, carry):
        far_copy(i).wait_send()
        return carry

    lax.fori_loop(jnp.where(relays, near_end, n_row), n_row, left_far, 0)

    def own_left(c):
        part = y_row.at[others, :, tail_of(c)]
        remote(part, part, o_send, o_recv, (row, peers[0])).wait_send()

    by_col(own_left)


def local(n_row, n_col, right_side, inverse_t, u_factor, v_factor, ranks):
    nrhs, width = right_side.shape[2:]
    per_col, _, rank_max = u_factor.shape[2:5]
    piece = width // n_col
    vmem = pl.BlockSpec(memory_space=pltpu.VMEM)
    hbm = pl.BlockSpec(memory_space=pl.ANY)
    dma = pltpu.SemaphoreType.DMA

    def f32(*shape):
        return pltpu.VMEM(shape, jnp.float32)

    def bf16(*shape):
        return pltpu.VMEM(shape, jnp.bfloat16)

    units = sum((width - c * piece // 128 * 128) // 128 for c in range(n_col))
    tile_set = [
        f32(n_col, rank_max, piece),
        f32(n_col, rank_max, piece),
        f32(n_col, rank_max, piece),
        f32(rank_max, piece),
        f32(piece, rank_max),
        f32(nrhs, rank_max),
        f32(n_col, nrhs, rank_max),
    ]
    return pl.pallas_call(
        functools.partial(kernel, n_row, n_col),
        out_shape=(
            pltpu.VMEM((1, 1, nrhs, width), jnp.float32),
            pltpu.VMEM((1, 1, nrhs), jnp.float32),
        ),
        in_specs=[hbm, hbm, hbm, hbm, hbm],
        out_specs=(vmem, vmem),
        scratch_shapes=[
            f32(nrhs, width),
            bf16(piece, width),
            bf16(per_col, rank_max, width),
            bf16(per_col, rank_max, width),
            pltpu.SMEM((per_col,), jnp.int32),
            f32(per_col, n_col, nrhs, width),
            f32(per_col, n_col, nrhs, piece),
            f32(n_row, nrhs, piece),
            f32(n_col, nrhs, width),
            f32(n_col, 1, 128),
            f32(nrhs, piece),
            f32(nrhs, width),
            f32(nrhs, width),
            f32(units, nrhs, 128),
            *tile_set,
            *tile_set,
            f32(rank_max, width),
            f32(rank_max, width),
            bf16(width, rank_max),
            bf16(per_col, width, rank_max),
            f32(rank_max, piece),
            f32(nrhs, rank_max),
            f32(nrhs, rank_max),
            f32(n_col, rank_max, piece),
            f32(rank_max, piece),
            f32(nrhs, rank_max),
            f32(nrhs, rank_max),
            f32(n_col, nrhs, rank_max),
            f32(3, rank_max, rank_max),
            f32(3, n_col, rank_max, rank_max),
            bf16(3, rank_max, rank_max),
            f32(rank_max, piece),
            f32(rank_max, piece),
            f32(piece, rank_max),
            f32(piece, width),
            f32(piece, width),
            bf16(piece, width),
            f32(nrhs, piece),
            f32(nrhs, piece),
            f32(nrhs, piece),
            f32(nrhs, piece),
            f32(nrhs, rank_max),
            f32(n_col, nrhs, rank_max),
            f32(nrhs, width),
            bf16(piece, rank_max),
            bf16(piece, rank_max),
            dma((5,)),
            dma((max(NEAR + 1, n_row - NEAR - 1),)),
            dma((per_col,)),
            dma((per_col,)),
            dma((n_row - 3,)),
            dma, dma, dma, dma,
            dma((n_col,)),
            dma((n_col,)),
            dma, dma, dma, dma,
            dma((n_col,)),
            dma, dma,
            pltpu.SemaphoreType.REGULAR,
            pltpu.SemaphoreType.REGULAR,
            dma,
            dma, dma, dma, dma, dma,
            dma, dma, dma, dma, dma, dma, dma, dma, dma,
        ],
        compiler_params=pltpu.CompilerParams(collective_id=0, has_side_effects=True),
        name="forward_solve",
    )(right_side, inverse_t, u_factor, v_factor, ranks.reshape(per_col))


def solution(mesh):
    placed = (
        P(None, "row", None, None),
        P(None, "row", "col", None),
        P(None, "row", None, "col", None, None),
        P(None, "row", None, "col", None, None),
        P(None, "row", None, "col"),
    )
    return jax.shard_map(
        functools.partial(local, mesh.shape["row"], mesh.shape["col"]),
        mesh=mesh,
        in_specs=placed,
        out_specs=(P(None, "row", None, None), P(None, "row", None)),
        check_vma=False,
    )
```
